512 devices in a mesh: dp: 32 (over x, y), mx: 4 (over z_hi, core), my: 4 (over z_lo).
Axes of the slice: x: 4, y: 8, z: 8 (z_hi: 2, z_lo: 4; z = z_hi * 4 + z_lo), core: 2. Of those that a mesh axis runs over, the one named last changes fastest.
Arguments:
- mentor_final_states: bfloat16 [2048, 4608], P('dp'), may hold values from -12 to 12
- mentor_output_matrix: bfloat16 [4608, 4096], P(None, ('mx', 'my')), may hold values from -0.09375 to 0.09375
- learner_final_states: bfloat16 [2048, 3584], P('dp', 'mx'), may hold values from -12 to 12
- learner_output_matrix: bfloat16 [3584, 4096], P('mx', 'my'), may hold values from -0.09375 to 0.09375
- loss_mask: int32 [2048], P('dp'), may hold values 0 or 1
Outputs:
- mismatch_per_piece: float32 [2048], P('dp')
- mean_loss: float32 [], replicated
- student_grad: float32 [2048, 4096], P('dp', 'my')
The draws below stay inside these ranges and needn't reach their ends.
All inputs are finite; a program needn't handle non-finite values.
Results may differ from the reference program's by a relative error of at most 0.0003.
Values sent between devices are 32-bit elements.
A program may use at most 64 MiB of HBM per device.

```python
import jax
import jax.numpy as jnp

D_T = 4608
D_S = 3584
WORD_LEXICON = 4096
WINDOW_PIECES = 2048


def with_ends(array, key, least, high):
    dims = array.shape
    place = [jax.random.randint(jax.random.fold_in(key, axis), (), 0, dims[axis]) for axis in range(len(dims))]
    array = array.at[tuple(place)].set(least)
    longest = dims.index(max(dims))
    place[longest] = (place[longest] + 1) % dims[longest]
    return array.at[tuple(place)].set(high)


def steps_of(own_key, shape, pieces, smallest, largest):
    def one(dim, shards_of):
        draws = jax.random.uniform(jax.random.fold_in(jax.random.fold_in(own_key, 6), dim), (shards_of,), jnp.float32, smallest / len(pieces), largest / len(pieces))
        return jnp.repeat(jnp.exp(draws), shape[dim] // shards_of).reshape((-1,) + (1,) * (len(shape) - dim - 1))

    level = one(*pieces[0])
    for cut in pieces[1:]:
        level = level * one(*cut)
    return level


def bell_draw(own_key, extent, spread, limit, cuts=(), kind=jnp.bfloat16):
    result = spread * jax.random.normal(own_key, extent, jnp.float32)
    if cuts:
        result = result * steps_of(own_key, extent, cuts, -0.22, 0.18)
    return jnp.clip(result, -limit, limit).astype(kind)


def setup_inputs(seed: int = 0) -> dict:
    arg_keys = jax.random.split(jax.random.key(seed), 6)
    mentor_final_states = bell_draw(arg_keys[0], (WINDOW_PIECES, D_T), 2.0, 12.0, ((0, 32),))
    mentor_output_matrix = bell_draw(arg_keys[1], (D_T, WORD_LEXICON), D_T ** -0.5, 0.09375, ((1, 16),))
    learner_final_states = bell_draw(arg_keys[2], (WINDOW_PIECES, D_S), 2.0, 12.0, ((0, 32), (1, 4)))
    learner_output_matrix = bell_draw(arg_keys[3], (D_S, WORD_LEXICON), D_S ** -0.5, 0.09375, ((0, 4), (1, 4)))
    loss_mask = with_ends((jax.random.randint(arg_keys[4], (WINDOW_PIECES,), 0, 4) < 3).astype(jnp.int32), jax.random.fold_in(arg_keys[4], 1), 0, 1)
    return {"mentor_final_states": mentor_final_states, "mentor_output_matrix": mentor_output_matrix, "learner_final_states": learner_final_states, "learner_output_matrix": learner_output_matrix, "loss_mask": loss_mask}


SOFTENING_HEAT = 2.0


def log_softmax_rows(values):
    row_max = jnp.max(values, axis=1, keepdims=True)
    row_sum = jnp.sum(jnp.exp(values - row_max), axis=1, keepdims=True)
    return values - (row_max + jnp.log(row_sum))


def reference(mentor_final_states, mentor_output_matrix, learner_final_states, learner_output_matrix, loss_mask):
    mentor_softened_scores = jnp.dot(mentor_final_states, mentor_output_matrix, preferred_element_type=jnp.float32) / SOFTENING_HEAT
    learner_softened_scores = jnp.dot(learner_final_states, learner_output_matrix, preferred_element_type=jnp.float32) / SOFTENING_HEAT
    mentor_logarithmic_odds = log_softmax_rows(mentor_softened_scores)
    learner_logarithmic_odds = log_softmax_rows(learner_softened_scores)
    mentor_likelihoods = jnp.exp(mentor_logarithmic_odds)
    mismatch_per_piece = SOFTENING_HEAT * SOFTENING_HEAT * jnp.sum(mentor_likelihoods * (mentor_logarithmic_odds - learner_logarithmic_odds), axis=1)
    piece_importance = loss_mask.astype(jnp.float32)
    usable_count = jnp.sum(piece_importance)
    mean_loss = jnp.sum(piece_importance * mismatch_per_piece) / usable_count
    multiplier = piece_importance * (SOFTENING_HEAT * WORD_LEXICON * WINDOW_PIECES) / usable_count
    student_grad = (jnp.exp(learner_logarithmic_odds) - mentor_likelihoods) * multiplier[:, None]
    return mismatch_per_piece, mean_loss, student_grad
```

```python
import functools

import jax
import jax.numpy as jnp
from jax import lax
from jax.experimental import pallas as pl
from jax.experimental.pallas import tpu as pltpu
from jax.sharding import PartitionSpec as P

SOFTENING_HEAT = 2.0
CORES = 2
TEACHER_CHUNKS = 4
MESH = pl.DeviceIdType.MESH


def kernel(
    sizes,
    ts_hbm, tw_hbm, ss_hbm, sw_hbm, mask_hbm,
    small_ref, grad_ref,
    ts, tw, ss, sw, mask_v,
    t_own, t_all, s_all, d_send, d_recv, own, z_send, z_recv,
    st_all, cnt_all, los_all,
    ld_sem, tt_ssem, tt_rsem, dd_ssem, dd_rsem, zz_ssem, zz_rsem,
    ag_ssem, ag_rsem, rl_ssem, rl_rsem, st_ssem, st_rsem, dp_ssem, dp_rsem,
):
    n_dp, n_mx, n_my = sizes
    group = n_mx * n_my
    dp, mx, my = lax.axis_index("dp"), lax.axis_index("mx"), lax.axis_index("my")
    zz, cc = mx // CORES, mx % CORES
    oz, oc = 1 - zz, 1 - cc
    me = mx * n_my + my
    partner = {"mx": zz * CORES + oc}
    across = {"mx": oz * CORES + cc}
    far = oz * CORES + cc
    tokens, bc = t_own.shape
    kc = tw.shape[0] // TEACHER_CHUNKS

    def remote(src, dst, ssem, rsem, dev):
        return pltpu.make_async_remote_copy(
            src_ref=src, dst_ref=dst, send_sem=ssem, recv_sem=rsem, device_id=dev, device_id_type=MESH
        )

    blocks = [oz * CORES + oc, far, zz * CORES + oc, mx]
    student = [pltpu.make_async_copy(ss_hbm, ss, ld_sem.at[0])]
    for k, block in enumerate(blocks):
        cols = pl.ds(pl.multiple_of(block * bc, bc), bc)
        student.append(pltpu.make_async_copy(sw_hbm.at[:, cols], sw.at[k], ld_sem.at[1 + k]))
    base = 1 + n_mx
    teacher = [pltpu.make_async_copy(ts_hbm, ts, ld_sem.at[base])]
    for k in range(TEACHER_CHUNKS):
        rows = pl.ds(k * kc, kc)
        teacher.append(pltpu.make_async_copy(tw_hbm.at[rows, :], tw.at[rows, :], ld_sem.at[base + 1 + k]))
    mask_load = pltpu.make_async_copy(mask_hbm, mask_v, ld_sem.at[base + 1 + TEACHER_CHUNKS])
    for c in student:
        c.start()
    mask_load.start()

    barrier = pltpu.get_barrier_semaphore()
    for k in range(1, group):
        peer = (me + k) % group
        pl.semaphore_signal(
            barrier, inc=1, device_id={"mx": peer // n_my, "my": peer % n_my}, device_id_type=MESH
        )
    for k in range(1, n_dp):
        pl.semaphore_signal(barrier, inc=1, device_id={"dp": (dp + k) % n_dp}, device_id_type=MESH)

    def dot(k):
        student[1 + k].wait()
        return jnp.dot(ss[...], sw[k], preferred_element_type=jnp.float32)

    student[0].wait()
    d_send[0] = dot(0)
    for c in teacher:
        c.start()
    pl.semaphore_wait(barrier, group - 1 + n_dp - 1)
    d_copies = [
        remote(d_send.at[k], d_recv.at[k], dd_ssem.at[k], dd_rsem.at[k], partner) for k in range(2)
    ]
    d_copies[0].start()
    own[0] = dot(1)
    d_send[1] = dot(2)
    d_copies[1].start()
    own[1] = dot(3)
    d_copies[0].wait_recv()
    z_send[...] = own[0] + d_recv[0]
    z_copy = remote(z_send, z_recv, zz_ssem.at[0], zz_rsem.at[0], across)
    z_copy.start()

    def dp_copies(buf, which):
        return [
            remote(buf.at[dp], buf.at[dp], dp_ssem.at[which, k], dp_rsem.at[which, k], {"dp": (dp + k) % n_dp})
            for k in range(1, n_dp)
        ]

    mask_load.wait()
    mask = mask_v[...].astype(jnp.float32)
    cnt_all[dp] = jnp.broadcast_to(jnp.sum(mask, axis=1, keepdims=True), cnt_all.shape[1:])
    cnt_copies = dp_copies(cnt_all, 0)
    for c in cnt_copies:
        c.start()

    teacher[0].wait()
    acc = jnp.zeros((tokens, bc), jnp.float32)
    for k in range(TEACHER_CHUNKS):
        teacher[1 + k].wait()
        rows = slice(k * kc, (k + 1) * kc)
        acc += jnp.dot(ts[:, rows], tw[rows, :], preferred_element_type=jnp.float32)
    t_own[...] = acc * (1.0 / SOFTENING_HEAT)

    mine = mx == my
    swap = remote(t_own, t_all.at[my], tt_ssem.at[0], tt_rsem.at[0], {"mx": my, "my": mx})
    my_far = (1 - my // CORES) * CORES + my % CORES
    swap_far = remote(t_own, t_all.at[my], tt_ssem.at[1], tt_rsem.at[1], {"mx": my_far, "my": mx})

    @pl.when(jnp.logical_not(mine))
    def _():
        swap.start()

    @pl.when(mine)
    def _():
        t_all[mx] = t_own[...]

    d_copies[1].wait_recv()
    near = own[1] + d_recv[1]
    z_copy.wait_recv()
    s_blk = (near + z_recv[...]) * (1.0 / SOFTENING_HEAT)
    s_all[mx] = s_blk

    @pl.when(jnp.logical_not(mine))
    def _():
        swap.wait_recv()

    t_blk = t_all[mx]
    mt = jnp.max(t_blk, axis=1, keepdims=True)
    ms = jnp.max(s_blk, axis=1, keepdims=True)
    td, sd = t_blk - mt, s_blk - ms
    et = jnp.exp(td)
    st = jnp.sum(et, axis=1, keepdims=True)
    sS = jnp.sum(jnp.exp(sd), axis=1, keepdims=True)
    cr = jnp.sum(et * (td - sd), axis=1, keepdims=True)
    log_st, log_ss = jnp.log(st), jnp.log(sS)
    kl = cr / st - log_st + log_ss
    lane = lax.broadcasted_iota(jnp.int32, (tokens, 128), 1)
    upper = jnp.where(lane == 0, mt + log_st, kl)
    lower = jnp.broadcast_to(ms + log_ss, (tokens, 128))
    st_all[me] = jnp.concatenate([upper, lower], axis=0).T[:2, :]
    st_copies = []
    for k in range(1, group):
        peer = (me + k) % group
        c = remote(st_all.at[me], st_all.at[me], st_ssem.at[k], st_rsem.at[k],
                   {"mx": peer // n_my, "my": peer % n_my})
        c.start()
        st_copies.append(c)

    s_far = remote(s_all.at[mx], s_all.at[mx], ag_ssem.at[0], ag_rsem.at[0], across)
    s_far.start()

    swap_far.start()

    relays = [
        remote(buf.at[slot], buf.at[slot], rl_ssem.at[i], rl_rsem.at[i], partner)
        for i, (buf, slot) in enumerate(((s_all, mx), (t_all, mx), (s_all, far), (t_all, far)))
    ]
    relays[0].start()
    relays[1].start()

    for c in cnt_copies:
        c.wait_recv()
    count = jnp.sum(cnt_all[:, 0, :], axis=0, keepdims=True)
    for c in st_copies:
        c.wait_recv()
    both = st_all[:, 0, :]
    kls = st_all[:, 1, :][:, :tokens]
    top = jnp.max(both, axis=0, keepdims=True)
    lse = top + jnp.log(jnp.sum(jnp.exp(both - top), axis=0, keepdims=True))
    rel = both - lse
    rel_t, rel_s = rel[:, :tokens], rel[:, tokens:2 * tokens]
    mism = (SOFTENING_HEAT * SOFTENING_HEAT) * jnp.sum(
        jnp.exp(rel_t) * (kls + (rel_t - rel_s)), axis=0, keepdims=True
    )
    small_ref[0:1, :tokens] = mism
    los_all[dp] = jnp.broadcast_to(jnp.sum(mask * mism, axis=1, keepdims=True), los_all.shape[1:])
    los_copies = dp_copies(los_all, 1)
    for c in los_copies:
        c.start()

    multiplier = SOFTENING_HEAT * n_mx * n_my * bc * n_dp * tokens
    mult = mask * multiplier / count[:, :tokens]
    mult = jnp.concatenate([mult, mult], axis=1)
    row = lax.broadcasted_iota(jnp.int32, (128, 128), 0)
    back = jnp.where(row == 0, lse, mult).T
    lt, ls, mu = back[:tokens, 0:1], back[tokens:2 * tokens, 0:1], back[:tokens, 1:2]

    s_far.wait_recv()
    relays[2].start()

    swap_far.wait_recv()
    relays[3].start()
    for c in relays:
        c.wait_recv()
    for j in range(n_mx):
        grad_ref[:, j * bc:(j + 1) * bc] = (jnp.exp(s_all[j] - ls) - jnp.exp(t_all[j] - lt)) * mu

    for c in los_copies:
        c.wait_recv()
    small_ref[1:2, :] = jnp.sum(los_all[:, 0, :], axis=0, keepdims=True) / count

    @pl.when(jnp.logical_not(mine))
    def _():
        swap.wait_send()

    for c in cnt_copies + los_copies + d_copies + [z_copy, s_far, swap_far] + relays + st_copies:
        c.wait_send()


def deliver(small_ref, grad_ref, mism_ref, loss_ref, out_ref, sem):
    copy = pltpu.make_async_copy(grad_ref, out_ref, sem)
    copy.start()
    mism_ref[...] = small_ref[0:1, :mism_ref.shape[1]]
    loss_ref[...] = small_ref[1:2, 0:1]
    copy.wait()


def shards(sizes, ts, tw, ss, sw, mask):
    n_dp, n_mx, n_my = sizes
    tokens, bc = ts.shape[0], tw.shape[1]
    cols = sw.shape[1]
    group = n_mx * n_my
    f32 = jnp.float32
    V, D = pltpu.VMEM, pltpu.SemaphoreType.DMA
    hbm = pl.BlockSpec(memory_space=pltpu.HBM)
    vm = pl.BlockSpec(memory_space=pltpu.VMEM)
    small, grad = pl.pallas_call(
        functools.partial(kernel, sizes),
        out_shape=(V((8, 128), f32), V((tokens, cols), f32)),
        in_specs=[hbm, hbm, hbm, hbm, hbm],
        out_specs=(vm, vm),
        scratch_shapes=[
            V(ts.shape, ts.dtype), V(tw.shape, tw.dtype), V(ss.shape, ss.dtype),
            V((n_mx, sw.shape[0], bc), sw.dtype), V((1, tokens), mask.dtype),
            V((tokens, bc), f32), V((n_mx, tokens, bc), f32), V((n_mx, tokens, bc), f32),
            V((2, tokens, bc), f32), V((2, tokens, bc), f32), V((2, tokens, bc), f32),
            V((tokens, bc), f32), V((tokens, bc), f32),
            V((group, 2, 128), f32), V((n_dp, 1, 128), f32), V((n_dp, 1, 128), f32),
            D((3 + TEACHER_CHUNKS + n_mx,)), D((2,)), D((2,)), D((2,)), D((2,)), D((1,)), D((1,)),
            D((1,)), D((1,)), D((4,)), D((4,)), D((group,)), D((group,)), D((2, n_dp)), D((2, n_dp)),
        ],
        compiler_params=pltpu.CompilerParams(
            collective_id=0, has_side_effects=True, vmem_limit_bytes=64_000_000
        ),
    )(ts, tw, ss, sw, mask.reshape(1, tokens))
    mism, loss, grad = pl.pallas_call(
        deliver,
        out_shape=(
            jax.ShapeDtypeStruct((1, tokens), f32),
            jax.ShapeDtypeStruct((1, 1), f32),
            jax.ShapeDtypeStruct((tokens, cols), f32),
        ),
        in_specs=[vm, vm],
        out_specs=(vm, vm, hbm),
        scratch_shapes=[D],
        compiler_params=pltpu.CompilerParams(vmem_limit_bytes=16 * 1024 * 1024),
    )(
        pltpu.with_memory_space_constraint(small, pltpu.VMEM),
        pltpu.with_memory_space_constraint(grad, pltpu.VMEM),
    )
    return mism.reshape(tokens), loss.reshape(()), grad


def solution(mesh):
    sizes = (mesh.shape["dp"], mesh.shape["mx"], mesh.shape["my"])
    placed = (P("dp", None), P(None, ("mx", "my")), P("dp", "mx"), P("mx", "my"), P("dp"))
    return jax.shard_map(
        functools.partial(shards, sizes), mesh=mesh, in_specs=placed,
        out_specs=(P("dp"), P(), P("dp", "my")), check_vma=False,
    )
```

```python
import functools

import jax
import jax.numpy as jnp
from jax import lax
from jax.experimental import pallas as pl
from jax.experimental.pallas import tpu as pltpu
from jax.sharding import PartitionSpec as P

SOFTENING_HEAT = 2.0
CORES = 2
TEACHER_CHUNKS = 4
MESH = pl.DeviceIdType.MESH


def kernel(
    sizes,
    ts_hbm, tw_hbm, ss_hbm, sw_hbm, mask_hbm,
    small_ref, grad_ref,
    ts, tw, ss, sw, mask_v,
    t_own, t_in, d_send, d_recv, own, z_send, z_recv,
    st_all, cnt_all, los_all,
    ld_sem, tt_sem, dd_ssem, dd_rsem, zz_sem, ag_sem, rl_ssem, rl_rsem, st_sem, dp_ssem, dp_rsem,
):
    n_dp, n_mx, n_my = sizes
    group = n_mx * n_my
    dp, mx, my = lax.axis_index("dp"), lax.axis_index("mx"), lax.axis_index("my")
    zz, cc = mx // CORES, mx % CORES
    oz, oc = 1 - zz, 1 - cc
    me = mx * n_my + my
    partner = {"mx": zz * CORES + oc}
    across = {"mx": oz * CORES + cc}
    far = oz * CORES + cc
    tokens, bc = t_own.shape
    kc = tw.shape[0] // TEACHER_CHUNKS

    def remote(src, dst, ssem, rsem, dev):
        return pltpu.make_async_remote_copy(
            src_ref=src, dst_ref=dst, send_sem=ssem, recv_sem=rsem, device_id=dev, device_id_type=MESH
        )

    blocks = [oz * CORES + oc, far, zz * CORES + oc, mx]
    student = [pltpu.make_async_copy(ss_hbm, ss, ld_sem.at[0])]
    for k, block in enumerate(blocks):
        cols = pl.ds(pl.multiple_of(block * bc, bc), bc)
        student.append(pltpu.make_async_copy(sw_hbm.at[:, cols], sw.at[k], ld_sem.at[1 + k]))
    base = 1 + n_mx
    teacher = [pltpu.make_async_copy(ts_hbm, ts, ld_sem.at[base])]
    for k in range(TEACHER_CHUNKS):
        rows = pl.ds(k * kc, kc)
        teacher.append(pltpu.make_async_copy(tw_hbm.at[rows, :], tw.at[rows, :], ld_sem.at[base + 1 + k]))
    mask_load = pltpu.make_async_copy(mask_hbm, mask_v, ld_sem.at[base + 1 + TEACHER_CHUNKS])
    for c in student:
        c.start()
    mask_load.start()

    barrier = pltpu.get_barrier_semaphore()
    for k in range(1, group):
        peer = (me + k) % group
        pl.semaphore_signal(
            barrier, inc=1, device_id={"mx": peer // n_my, "my": peer % n_my}, device_id_type=MESH
        )
    for k in range(1, n_dp):
        pl.semaphore_signal(barrier, inc=1, device_id={"dp": (dp + k) % n_dp}, device_id_type=MESH)

    def dot(k):
        student[1 + k].wait()
        return jnp.dot(ss[...], sw[k], preferred_element_type=jnp.float32)

    student[0].wait()
    d_send[0] = dot(0)
    for c in teacher:
        c.start()
    pl.semaphore_wait(barrier, group - 1 + n_dp - 1)
    d_copies = [
        remote(d_send.at[k], d_recv.at[k], dd_ssem.at[k], dd_rsem.at[k], partner) for k in range(2)
    ]
    d_copies[0].start()
    own[0] = dot(1)
    d_send[1] = dot(2)
    d_copies[1].start()
    own[1] = dot(3)
    d_copies[0].wait_recv()
    z_send[...] = own[0] + d_recv[0]
    z_copy = remote(z_send, z_recv, zz_sem.at[0], zz_sem.at[1], across)
    z_copy.start()

    def dp_send(buf, which):
        for k in range(1, n_dp):
            remote(buf.at[dp], buf.at[dp], dp_ssem.at[which], dp_rsem.at[which], {"dp": (dp + k) % n_dp}).start()
        others = buf.at[pl.ds(0, n_dp - 1)]
        return remote(others, others, dp_ssem.at[which], dp_rsem.at[which], {"dp": (dp + 1) % n_dp})

    mask_load.wait()
    mask = mask_v[...].astype(jnp.float32)
    cnt_all[dp] = jnp.broadcast_to(jnp.sum(mask, axis=1, keepdims=True), cnt_all.shape[1:])
    counts = dp_send(cnt_all, 0)

    teacher[0].wait()
    acc = jnp.zeros((tokens, bc), jnp.float32)
    for k in range(TEACHER_CHUNKS):
        teacher[1 + k].wait()
        rows = slice(k * kc, (k + 1) * kc)
        acc += jnp.dot(ts[:, rows], tw[rows, :], preferred_element_type=jnp.float32)
    t_own[...] = acc * (1.0 / SOFTENING_HEAT)

    mine = mx == my
    swap = remote(t_own, t_in, tt_sem.at[0], tt_sem.at[1], {"mx": my, "my": mx})

    @pl.when(jnp.logical_not(mine))
    def _():
        swap.start()

    @pl.when(mine)
    def _():
        t_in[...] = t_own[...]

    d_copies[1].wait_recv()
    near = own[1] + d_recv[1]
    z_copy.wait_recv()
    s_blk = (near + z_recv[...]) * (1.0 / SOFTENING_HEAT)

    @pl.when(jnp.logical_not(mine))
    def _():
        swap.wait_recv()

    t_blk = t_in[...]
    mt = jnp.max(t_blk, axis=1, keepdims=True)
    ms = jnp.max(s_blk, axis=1, keepdims=True)
    td, sd = t_blk - mt, s_blk - ms
    et = jnp.exp(td)
    st = jnp.sum(et, axis=1, keepdims=True)
    sS = jnp.sum(jnp.exp(sd), axis=1, keepdims=True)
    cr = jnp.sum(et * (td - sd), axis=1, keepdims=True)
    log_st, log_ss = jnp.log(st), jnp.log(sS)
    kl = cr / st - log_st + log_ss
    lane = lax.broadcasted_iota(jnp.int32, (tokens, 128), 1)
    upper = jnp.where(lane == 0, mt + log_st, kl)
    lower = jnp.broadcast_to(ms + log_ss, (tokens, 128))
    st_all[me] = jnp.concatenate([upper, lower], axis=0).T[:2, :]
    for k in range(1, group):
        peer = (me + k) % group
        remote(st_all.at[me], st_all.at[me], st_sem.at[0], st_sem.at[1],
               {"mx": peer // n_my, "my": peer % n_my}).start()
    others = st_all.at[pl.ds(0, group - 1)]
    stats = remote(others, others, st_sem.at[0], st_sem.at[1], partner)

    counts.wait_recv()
    count = jnp.sum(cnt_all[:, 0, :], axis=0, keepdims=True)
    stats.wait_recv()
    both = st_all[:, 0, :]
    kls = st_all[:, 1, :][:, :tokens]
    top = jnp.max(both, axis=0, keepdims=True)
    lse = top + jnp.log(jnp.sum(jnp.exp(both - top), axis=0, keepdims=True))
    rel = both - lse
    rel_t, rel_s = rel[:, :tokens], rel[:, tokens:2 * tokens]
    mism = (SOFTENING_HEAT * SOFTENING_HEAT) * jnp.sum(
        jnp.exp(rel_t) * (kls + (rel_t - rel_s)), axis=0, keepdims=True
    )
    los_all[dp] = jnp.broadcast_to(jnp.sum(mask * mism, axis=1, keepdims=True), los_all.shape[1:])
    losses = dp_send(los_all, 1)
    small_ref[0:1, :tokens] = mism

    multiplier = SOFTENING_HEAT * n_mx * n_my * bc * n_dp * tokens
    mult = mask * multiplier / count[:, :tokens]
    mult = jnp.concatenate([mult, mult], axis=1)
    row = lax.broadcasted_iota(jnp.int32, (128, 128), 0)
    back = jnp.where(row == 0, lse, mult).T
    lt, ls, mu = back[:tokens, 0:1], back[tokens:2 * tokens, 0:1], back[:tokens, 1:2]
    grad_ref[mx] = (jnp.exp(s_blk - ls) - jnp.exp(t_blk - lt)) * mu

    g_far = remote(grad_ref.at[mx], grad_ref.at[mx], ag_sem.at[0], ag_sem.at[1], across)
    relays = [
        remote(grad_ref.at[slot], grad_ref.at[slot], rl_ssem.at[i], rl_rsem.at[i], partner)
        for i, slot in enumerate((mx, far))
    ]
    g_far.start()
    relays[0].start()
    g_far.wait_recv()
    relays[1].start()

    losses.wait_recv()
    small_ref[1:2, :] = jnp.sum(los_all[:, 0, :], axis=0, keepdims=True) / count
    for c in relays:
        c.wait_recv()

    @pl.when(jnp.logical_not(mine))
    def _():
        swap.wait_send()

    for c in [counts, losses, stats, z_copy, g_far] + d_copies + relays:
        c.wait_send()


def deliver(small_ref, grad_ref, mism_out, loss_out, grad_out, mism_v, loss_v, sem):
    bc = grad_ref.shape[2]
    copies = [
        pltpu.make_async_copy(grad_ref.at[j], grad_out.at[:, j * bc:(j + 1) * bc], sem.at[j])
        for j in range(grad_ref.shape[0])
    ]
    for c in copies:
        c.start()
    mism_v[...] = small_ref[0:1, :mism_v.shape[1]]
    loss_v[...] = small_ref[1:2, 0:1]
    for src, dst in ((mism_v, mism_out), (loss_v, loss_out)):
        copies.append(pltpu.make_async_copy(src, dst, sem.at[len(copies)]))
        copies[-1].start()
    for c in copies:
        c.wait()


def shards(sizes, ts, tw, ss, sw, mask):
    n_dp, n_mx, n_my = sizes
    tokens, bc = ts.shape[0], tw.shape[1]
    cols = sw.shape[1]
    group = n_mx * n_my
    f32 = jnp.float32
    V, D = pltpu.VMEM, pltpu.SemaphoreType.DMA
    hbm = pl.BlockSpec(memory_space=pltpu.HBM)
    vm = pl.BlockSpec(memory_space=pltpu.VMEM)
    held = pl.pallas_call(
        functools.partial(kernel, sizes),
        out_shape=(V((8, 128), f32), V((n_mx, tokens, bc), f32)),
        in_specs=[hbm, hbm, hbm, hbm, hbm],
        out_specs=(vm, vm),
        scratch_shapes=[
            V(ts.shape, ts.dtype), V(tw.shape, tw.dtype), V(ss.shape, ss.dtype),
            V((n_mx, sw.shape[0], bc), sw.dtype), V((1, tokens), mask.dtype),
            V((tokens, bc), f32), V((tokens, bc), f32),
            V((2, tokens, bc), f32), V((2, tokens, bc), f32), V((2, tokens, bc), f32),
            V((tokens, bc), f32), V((tokens, bc), f32),
            V((group, 2, 128), f32), V((n_dp, 1, 128), f32), V((n_dp, 1, 128), f32),
            D((3 + TEACHER_CHUNKS + n_mx,)), D((2,)), D((2,)), D((2,)), D((2,)), D((2,)),
            D((2,)), D((2,)), D((2,)), D((2,)), D((2,)),
        ],
        compiler_params=pltpu.CompilerParams(
            collective_id=0, has_side_effects=True, vmem_limit_bytes=64_000_000
        ),
    )(ts, tw, ss, sw, mask.reshape(1, tokens))
    mism, loss, grad = pl.pallas_call(
        deliver,
        out_shape=(
            jax.ShapeDtypeStruct((1, tokens), f32),
            jax.ShapeDtypeStruct((1, 1), f32),
            jax.ShapeDtypeStruct((tokens, cols), f32),
        ),
        in_specs=[vm, vm],
        out_specs=(hbm, hbm, hbm),
        scratch_shapes=[V((1, tokens), f32), V((1, 1), f32), D((2 + n_mx,))],
        compiler_params=pltpu.CompilerParams(vmem_limit_bytes=16 * 1024 * 1024),
    )(*[pltpu.with_memory_space_constraint(x, pltpu.VMEM) for x in held])
    return mism.reshape(tokens), loss.reshape(()), grad


def solution(mesh):
    sizes = (mesh.shape["dp"], mesh.shape["mx"], mesh.shape["my"])
    placed = (P("dp", None), P(None, ("mx", "my")), P("dp", "mx"), P("mx", "my"), P("dp"))
    return jax.shard_map(
        functools.partial(shards, sizes), mesh=mesh, in_specs=placed,
        out_specs=(P("dp"), P(), P("dp", "my")), check_vma=False,
    )
```

```python
import functools

import jax
import jax.numpy as jnp
from jax import lax
from jax.experimental import pallas as pl
from jax.experimental.pallas import tpu as pltpu
from jax.sharding import PartitionSpec as P

SOFTENING_HEAT = 2.0
CORES = 2
RING_Y = 8
TEACHER_CHUNKS = 4
MESH = pl.DeviceIdType.MESH


def kernel(
    sizes,
    ts_hbm, tw_hbm, ss_hbm, sw_hbm, mask_hbm,
    small_ref, grad_ref,
    ts, tw, ss, sw, mask_v,
    t_own, t_in, d_send, d_recv, own, z_send, z_recv,
    st_all, cnt_all, los_all,
    ld_sem, tt_sem, dd_ssem, dd_rsem, zz_sem, ag_sem, rl_ssem, rl_rsem, st_sem, dp_ssem, dp_rsem, token,
):
    n_dp, n_mx, n_my = sizes
    group = n_mx * n_my
    dp, mx, my = lax.axis_index("dp"), lax.axis_index("mx"), lax.axis_index("my")
    zz, cc = lax.div(mx, CORES), lax.rem(mx, CORES)
    oz, oc = 1 - zz, 1 - cc
    me = mx * n_my + my
    partner = {"mx": zz * CORES + oc}
    across = {"mx": oz * CORES + cc}
    far = oz * CORES + cc
    tokens, bc = t_own.shape
    kc = tw.shape[0] // TEACHER_CHUNKS

    def remote(src, dst, ssem, rsem, dev):
        return pltpu.make_async_remote_copy(
            src_ref=src, dst_ref=dst, send_sem=ssem, recv_sem=rsem, device_id=dev, device_id_type=MESH
        )

    blocks = [oz * CORES + oc, far, zz * CORES + oc, mx]
    student = [pltpu.make_async_copy(ss_hbm, ss, ld_sem.at[0])]
    for k, block in enumerate(blocks):
        cols = pl.ds(pl.multiple_of(block * bc, bc), bc)
        student.append(pltpu.make_async_copy(sw_hbm.at[:, cols], sw.at[k], ld_sem.at[1 + k]))
    base = 1 + n_mx
    teacher = [pltpu.make_async_copy(ts_hbm, ts, ld_sem.at[base])]
    for k in range(TEACHER_CHUNKS):
        rows = pl.ds(k * kc, kc)
        teacher.append(pltpu.make_async_copy(tw_hbm.at[rows, :], tw.at[rows, :], ld_sem.at[base + 1 + k]))
    mask_load = pltpu.make_async_copy(mask_hbm, mask_v, ld_sem.at[base + 1 + TEACHER_CHUNKS])
    for c in student:
        c.start()
    mask_load.start()

    line = [
        {"mx": lax.rem(mx + i, n_mx), "my": lax.rem(my + j, n_my)}
        for i in (2, 3, 1, 0) for j in range(n_my) if (i, j) != (0, 0)
    ]
    ring_x = n_dp // RING_Y
    px, py = lax.div(dp, RING_Y), lax.rem(dp, RING_Y)

    def plane(i, j):
        return {"dp": lax.rem(px + i, ring_x) * RING_Y + lax.rem(py + j, RING_Y)}

    near = [plane(1, 0), plane(ring_x - 1, 0), plane(0, 1), plane(0, RING_Y - 1)]

    def tell(sem, devices):
        for device in devices:
            pl.semaphore_signal(sem, inc=1, device_id=device, device_id_type=MESH)

    barrier = pltpu.get_barrier_semaphore()
    tell(barrier, line + near)

    def dot(k):
        student[1 + k].wait()
        return jnp.dot(ss[...], sw[k], preferred_element_type=jnp.float32)

    d_copies = [
        remote(d_send.at[k], d_recv.at[k], dd_ssem.at[k], dd_rsem.at[k], partner) for k in range(2)
    ]
    mine = mx == my
    swap = remote(t_own, t_in, tt_sem.at[0], tt_sem.at[1], {"mx": my, "my": mx})

    def teacher_block():
        teacher[0].wait()
        acc = jnp.zeros((tokens, bc), jnp.float32)
        for k in range(TEACHER_CHUNKS):
            teacher[1 + k].wait()
            rows = slice(k * kc, (k + 1) * kc)
            acc += jnp.dot(ts[:, rows], tw[rows, :], preferred_element_type=jnp.float32)
        t_own[...] = acc * (1.0 / SOFTENING_HEAT)

    def hand_over():
        @pl.when(jnp.logical_not(mine))
        def _():
            swap.start()

        @pl.when(mine)
        def _():
            t_in[...] = t_own[...]

    first, last = zz == 0, zz != 0
    student[0].wait()
    d_send[0] = dot(0)
    for c in teacher:
        c.start()

    @pl.when(first)
    def _():
        own[0] = dot(1)
        d_send[1] = dot(2)
        own[1] = dot(3)
        teacher_block()

    pl.semaphore_wait(barrier, len(line) + len(near))
    d_copies[0].start()
    tell(token.at[0], near)

    @pl.when(first)
    def _():
        d_copies[1].start()
        hand_over()

    @pl.when(last)
    def _():
        own[0] = dot(1)
        d_send[1] = dot(2)
        d_copies[1].start()
        own[1] = dot(3)

    d_copies[0].wait_recv()
    z_send[...] = own[0] + d_recv[0]
    z_copy = remote(z_send, z_recv, zz_sem.at[0], zz_sem.at[1], across)
    z_copy.start()

    @pl.when(last)
    def _():
        teacher_block()
        hand_over()

    pl.semaphore_wait(token.at[0], len(near))
    tell(token.at[1], [plane(0, 2), plane(0, RING_Y - 2)])
    pl.semaphore_wait(token.at[1], 2)
    tell(token.at[2], [plane(i, 0) for i in range(1, ring_x)])
    pl.semaphore_wait(token.at[2], ring_x - 1)

    def dp_send(buf, which):
        for k in range(1, n_dp):
            peer = {"dp": lax.rem(dp + k, n_dp)}
            remote(buf.at[dp], buf.at[dp], dp_ssem.at[which], dp_rsem.at[which], peer).start()
        others = buf.at[pl.ds(0, n_dp - 1)]
        return remote(others, others, dp_ssem.at[which], dp_rsem.at[which], partner)

    mask_load.wait()
    mask = mask_v[...].astype(jnp.float32)
    cnt_all[dp] = jnp.broadcast_to(jnp.sum(mask, axis=1, keepdims=True), cnt_all.shape[1:])
    counts = dp_send(cnt_all, 0)

    d_copies[1].wait_recv()
    mine_sum = own[1] + d_recv[1]
    z_copy.wait_recv()
    s_blk = (mine_sum + z_recv[...]) * (1.0 / SOFTENING_HEAT)

    @pl.when(jnp.logical_not(mine))
    def _():
        swap.wait_recv()

    t_blk = t_in[...]
    mt = jnp.max(t_blk, axis=1, keepdims=True)
    ms = jnp.max(s_blk, axis=1, keepdims=True)
    td, sd = t_blk - mt, s_blk - ms
    et = jnp.exp(td)
    st = jnp.sum(et, axis=1, keepdims=True)
    sS = jnp.sum(jnp.exp(sd), axis=1, keepdims=True)
    cr = jnp.sum(et * (td - sd), axis=1, keepdims=True)
    log_st, log_ss = jnp.log(st), jnp.log(sS)
    kl = cr / st - log_st + log_ss
    lane = lax.broadcasted_iota(jnp.int32, (tokens, 128), 1)
    upper = jnp.where(lane == 0, mt + log_st, kl)
    lower = jnp.broadcast_to(ms + log_ss, (tokens, 128))
    st_all[me] = jnp.concatenate([upper, lower], axis=0).T[:2, :]
    for device in line:
        remote(st_all.at[me], st_all.at[me], st_sem.at[0], st_sem.at[1], device).start()
    others = st_all.at[pl.ds(0, group - 1)]
    stats = remote(others, others, st_sem.at[0], st_sem.at[1], partner)

    stats.wait_recv()
    both = st_all[:, 0, :]
    kls = st_all[:, 1, :][:, :tokens]
    top = jnp.max(both, axis=0, keepdims=True)
    lse = top + jnp.log(jnp.sum(jnp.exp(both - top), axis=0, keepdims=True))
    rel = both - lse
    rel_t, rel_s = rel[:, :tokens], rel[:, tokens:2 * tokens]
    mism = (SOFTENING_HEAT * SOFTENING_HEAT) * jnp.sum(
        jnp.exp(rel_t) * (kls + (rel_t - rel_s)), axis=0, keepdims=True
    )
    los_all[dp] = jnp.broadcast_to(jnp.sum(mask * mism, axis=1, keepdims=True), los_all.shape[1:])
    losses = dp_send(los_all, 1)
    small_ref[0:1, :tokens] = mism

    counts.wait_recv()
    count = jnp.sum(cnt_all[:, 0, :], axis=0, keepdims=True)
    multiplier = SOFTENING_HEAT * n_mx * n_my * bc * n_dp * tokens
    mult = mask * multiplier / count[:, :tokens]
    mult = jnp.concatenate([mult, mult], axis=1)
    row = lax.broadcasted_iota(jnp.int32, (128, 128), 0)
    back = jnp.where(row == 0, lse, mult).T
    lt, ls, mu = back[:tokens, 0:1], back[tokens:2 * tokens, 0:1], back[:tokens, 1:2]
    grad_ref[mx] = (jnp.exp(s_blk - ls) - jnp.exp(t_blk - lt)) * mu

    g_far = remote(grad_ref.at[mx], grad_ref.at[mx], ag_sem.at[0], ag_sem.at[1], across)
    relays = [
        remote(grad_ref.at[slot], grad_ref.at[slot], rl_ssem.at[i], rl_rsem.at[i], partner)
        for i, slot in enumerate((mx, far))
    ]
    g_far.start()
    relays[0].start()
    g_far.wait_recv()
    relays[1].start()

    losses.wait_recv()
    small_ref[1:2, :] = jnp.sum(los_all[:, 0, :], axis=0, keepdims=True) / count
    for c in relays:
        c.wait_recv()

    @pl.when(jnp.logical_not(mine))
    def _():
        swap.wait_send()

    for c in [counts, losses, stats, z_copy, g_far] + d_copies + relays:
        c.wait_send()


def deliver(small_ref, grad_ref, mism_out, loss_out, grad_out, mism_v, loss_v, sem):
    bc = grad_ref.shape[2]
    copies = [
        pltpu.make_async_copy(grad_ref.at[j], grad_out.at[:, j * bc:(j + 1) * bc], sem.at[j])
        for j in range(grad_ref.shape[0])
    ]
    for c in copies:
        c.start()
    mism_v[...] = small_ref[0:1, :mism_v.shape[1]]
    loss_v[...] = small_ref[1:2, 0:1]
    for src, dst in ((mism_v, mism_out), (loss_v, loss_out)):
        copies.append(pltpu.make_async_copy(src, dst, sem.at[len(copies)]))
        copies[-1].start()
    for c in copies:
        c.wait()


def shards(sizes, ts, tw, ss, sw, mask):
    n_dp, n_mx, n_my = sizes
    tokens, bc = ts.shape[0], tw.shape[1]
    cols = sw.shape[1]
    group = n_mx * n_my
    f32 = jnp.float32
    V, D = pltpu.VMEM, pltpu.SemaphoreType.DMA
    hbm = pl.BlockSpec(memory_space=pltpu.HBM)
    vm = pl.BlockSpec(memory_space=pltpu.VMEM)
    held = pl.pallas_call(
        functools.partial(kernel, sizes),
        out_shape=(V((8, 128), f32), V((n_mx, tokens, bc), f32)),
        in_specs=[hbm, hbm, hbm, hbm, hbm],
        out_specs=(vm, vm),
        scratch_shapes=[
            V(ts.shape, ts.dtype), V(tw.shape, tw.dtype), V(ss.shape, ss.dtype),
            V((n_mx, sw.shape[0], bc), sw.dtype), V((1, tokens), mask.dtype),
            V((tokens, bc), f32), V((tokens, bc), f32),
            V((2, tokens, bc), f32), V((2, tokens, bc), f32), V((2, tokens, bc), f32),
            V((tokens, bc), f32), V((tokens, bc), f32),
            V((group, 2, 128), f32), V((n_dp, 1, 128), f32), V((n_dp, 1, 128), f32),
            D((3 + TEACHER_CHUNKS + n_mx,)), D((2,)), D((2,)), D((2,)), D((2,)), D((2,)),
            D((2,)), D((2,)), D((2,)), D((2,)), D((2,)), pltpu.SemaphoreType.REGULAR((3,)),
        ],
        compiler_params=pltpu.CompilerParams(
            collective_id=0, has_side_effects=True, vmem_limit_bytes=64_000_000
        ),
    )(ts, tw, ss, sw, mask.reshape(1, tokens))
    mism, loss, grad = pl.pallas_call(
        deliver,
        out_shape=(
            jax.ShapeDtypeStruct((1, tokens), f32),
            jax.ShapeDtypeStruct((1, 1), f32),
            jax.ShapeDtypeStruct((tokens, cols), f32),
        ),
        in_specs=[vm, vm],
        out_specs=(hbm, hbm, hbm),
        scratch_shapes=[V((1, tokens), f32), V((1, 1), f32), D((2 + n_mx,))],
        compiler_params=pltpu.CompilerParams(vmem_limit_bytes=16 * 1024 * 1024),
    )(*[pltpu.with_memory_space_constraint(x, pltpu.VMEM) for x in held])
    return mism.reshape(tokens), loss.reshape(()), grad


def solution(mesh):
    sizes = (mesh.shape["dp"], mesh.shape["mx"], mesh.shape["my"])
    placed = (P("dp", None), P(None, ("mx", "my")), P("dp", "mx"), P("mx", "my"), P("dp"))
    return jax.shard_map(
        functools.partial(shards, sizes), mesh=mesh, in_specs=placed,
        out_specs=(P("dp"), P(), P("dp", "my")), check_vma=False,
    )
```

```python
import functools

import jax
import jax.numpy as jnp
from jax import lax
from jax.experimental import pallas as pl
from jax.experimental.pallas import tpu as pltpu
from jax.sharding import PartitionSpec as P

SOFTENING_HEAT = 2.0
CORES = 2
RING_Y = 8
TEACHER_CHUNKS = 4
MESH = pl.DeviceIdType.MESH


def kernel(
    sizes,
    ts_hbm, tw_hbm, ss_hbm, sw_hbm, mask_hbm,
    small_ref, grad_ref,
    ts, tw, ss, sw, mask_v,
    t_own, t_in, d_send, d_recv, own, z_send, z_recv,
    st_all, los_all,
    ld_sem, tt_sem, dd_ssem, dd_rsem, zz_sem, ag_sem, rl_ssem, rl_rsem, st_sem, dp_sem, token,
):
    n_dp, n_mx, n_my = sizes
    group = n_mx * n_my
    dp, mx, my = lax.axis_index("dp"), lax.axis_index("mx"), lax.axis_index("my")
    zz, cc = lax.div(mx, CORES), lax.rem(mx, CORES)
    oz, oc = 1 - zz, 1 - cc
    me = mx * n_my + my
    partner = {"mx": zz * CORES + oc}
    across = {"mx": oz * CORES + cc}

    def block_of(owner, a):
        one, two = lax.rem(a, 2) * (1 - lax.div(a, 2)), (1 - lax.rem(a, 2)) * lax.div(a, 2)
        core = lax.rem(owner, CORES)
        return lax.rem(owner + 2 * (one * (1 - core) + two * core), n_mx)

    owned, far = block_of(mx, my), block_of(oz * CORES + cc, my)
    tokens, bc = t_own.shape
    kc = tw.shape[0] // TEACHER_CHUNKS

    def remote(src, dst, ssem, rsem, dev):
        return pltpu.make_async_remote_copy(
            src_ref=src, dst_ref=dst, send_sem=ssem, recv_sem=rsem, device_id=dev, device_id_type=MESH
        )

    blocks = [block_of(oz * CORES + oc, my), far, block_of(zz * CORES + oc, my), owned]
    student = [pltpu.make_async_copy(ss_hbm, ss, ld_sem.at[0])]
    for k, block in enumerate(blocks):
        cols = pl.ds(pl.multiple_of(block * bc, bc), bc)
        student.append(pltpu.make_async_copy(sw_hbm.at[:, cols], sw.at[k], ld_sem.at[1 + k]))
    base = 1 + n_mx
    teacher = [pltpu.make_async_copy(ts_hbm, ts, ld_sem.at[base])]
    for k in range(TEACHER_CHUNKS):
        rows = pl.ds(k * kc, kc)
        teacher.append(pltpu.make_async_copy(tw_hbm.at[rows, :], tw.at[rows, :], ld_sem.at[base + 1 + k]))
    mask_load = pltpu.make_async_copy(mask_hbm, mask_v, ld_sem.at[base + 1 + TEACHER_CHUNKS])
    for c in student:
        c.start()
    mask_load.start()

    line = [
        {"mx": lax.rem(mx + i, n_mx), "my": lax.rem(my + j, n_my)}
        for i in (2, 3, 1, 0) for j in range(n_my) if (i, j) != (0, 0)
    ]
    ring_x = n_dp // RING_Y
    px, py = lax.div(dp, RING_Y), lax.rem(dp, RING_Y)

    def plane(i, j):
        return {"dp": lax.rem(px + i, ring_x) * RING_Y + lax.rem(py + j, RING_Y)}

    near = [plane(1, 0), plane(ring_x - 1, 0), plane(0, 1), plane(0, RING_Y - 1)]

    def tell(sem, devices):
        for device in devices:
            pl.semaphore_signal(sem, inc=1, device_id=device, device_id_type=MESH)

    heads = [
        {"mx": (oz if i else zz) * CORES, "my": lax.rem(my + j, n_my)}
        for i in (1, 0) for j in range(n_my) if (i, j) != (0, 0)
    ] + [dict(device, mx=zz * CORES) for device in near]
    barrier = pltpu.get_barrier_semaphore()
    tell(barrier, heads)

    @pl.when(cc == 0)
    def _():
        tell(barrier, [partner])

    def dot(k):
        student[1 + k].wait()
        return jnp.dot(ss[...], sw[k], preferred_element_type=jnp.float32)

    d_copies = [
        remote(d_send.at[k], d_recv.at[k], dd_ssem.at[k], dd_rsem.at[k], partner) for k in range(2)
    ]
    mine = mx == my
    swap = remote(t_own, t_in, tt_sem.at[0], tt_sem.at[1], {"mx": block_of(my, mx), "my": mx})

    def teacher_block():
        teacher[0].wait()
        acc = jnp.zeros((tokens, bc), jnp.float32)
        for k in range(TEACHER_CHUNKS):
            teacher[1 + k].wait()
            rows = slice(k * kc, (k + 1) * kc)
            acc += jnp.dot(ts[:, rows], tw[rows, :], preferred_element_type=jnp.float32)
        t_own[...] = acc * (1.0 / SOFTENING_HEAT)

    def hand_over():
        @pl.when(jnp.logical_not(mine))
        def _():
            swap.start()

        @pl.when(mine)
        def _():
            t_in[...] = t_own[...]

    first = jnp.logical_or(zz == 0, my == 0)
    last = jnp.logical_not(first)
    student[0].wait()
    d_send[0] = dot(0)
    for c in teacher:
        c.start()

    @pl.when(cc == 1)
    def _():
        pl.semaphore_wait(barrier, 1)
        tell(token.at[3], [partner])

    @pl.when(cc == 0)
    def _():
        pl.semaphore_wait(token.at[3], 1)

    d_copies[0].start()
    own[0] = dot(1)
    d_send[1] = dot(2)
    d_copies[1].start()
    own[1] = dot(3)

    @pl.when(first)
    def _():
        teacher_block()

    d_copies[0].wait_recv()
    z_send[...] = own[0] + d_recv[0]
    z_copy = remote(z_send, z_recv, zz_sem.at[0], zz_sem.at[1], across)

    @pl.when(cc == 0)
    def _():
        pl.semaphore_wait(barrier, CORES * len(heads))
        tell(token.at[4], [partner])

    @pl.when(cc == 1)
    def _():
        pl.semaphore_wait(token.at[4], 1)

    z_copy.start()

    @pl.when(first)
    def _():
        hand_over()

    @pl.when(last)
    def _():
        teacher_block()
        hand_over()

    tell(token.at[0], near)

    d_copies[1].wait_recv()
    mine_sum = own[1] + d_recv[1]
    z_copy.wait_recv()
    s_blk = (mine_sum + z_recv[...]) * (1.0 / SOFTENING_HEAT)

    @pl.when(jnp.logical_not(mine))
    def _():
        swap.wait_recv()

    t_blk = t_in[...]
    mt = jnp.max(t_blk, axis=1, keepdims=True)
    ms = jnp.max(s_blk, axis=1, keepdims=True)
    td, sd = t_blk - mt, s_blk - ms
    et = jnp.exp(td)
    st = jnp.sum(et, axis=1, keepdims=True)
    sS = jnp.sum(jnp.exp(sd), axis=1, keepdims=True)
    cr = jnp.sum(et * (td - sd), axis=1, keepdims=True)
    log_st, log_ss = jnp.log(st), jnp.log(sS)
    kl = cr / st - log_st + log_ss
    lane = lax.broadcasted_iota(jnp.int32, (tokens, 128), 1)
    upper = jnp.where(lane == 0, mt + log_st, kl)
    lower = jnp.broadcast_to(ms + log_ss, (tokens, 128))
    st_all[me] = jnp.concatenate([upper, lower], axis=0).T[:2, :]
    for device in line:
        remote(st_all.at[me], st_all.at[me], st_sem.at[0], st_sem.at[1], device).start()
    others = st_all.at[pl.ds(0, group - 1)]
    stats = remote(others, others, st_sem.at[0], st_sem.at[1], partner)

    pl.semaphore_wait(token.at[0], len(near))
    tell(token.at[1], [plane(0, 2), plane(0, RING_Y - 2)])
    pl.semaphore_wait(token.at[1], 2)
    tell(token.at[2], [plane(i, 0) for i in range(1, ring_x)])
    mask_load.wait()
    mask = mask_v[...].astype(jnp.float32)
    pl.semaphore_wait(token.at[2], ring_x - 1)

    stats.wait_recv()
    both = st_all[:, 0, :]
    kls = st_all[:, 1, :][:, :tokens]
    top = jnp.max(both, axis=0, keepdims=True)
    lse = top + jnp.log(jnp.sum(jnp.exp(both - top), axis=0, keepdims=True))
    rel = both - lse
    rel_t, rel_s = rel[:, :tokens], rel[:, tokens:2 * tokens]
    mism = (SOFTENING_HEAT * SOFTENING_HEAT) * jnp.sum(
        jnp.exp(rel_t) * (kls + (rel_t - rel_s)), axis=0, keepdims=True
    )
    half = lax.broadcasted_iota(jnp.int32, los_all.shape[1:], 1) < 64
    los_all[dp] = jnp.where(
        half, jnp.sum(mask * mism, axis=1, keepdims=True), jnp.sum(mask, axis=1, keepdims=True)
    )
    for k in range(1, n_dp):
        peer = {"dp": lax.rem(dp + k, n_dp)}
        remote(los_all.at[dp], los_all.at[dp], dp_sem.at[0], dp_sem.at[1], peer).start()
    others = los_all.at[pl.ds(0, n_dp - 1)]
    losses = remote(others, others, dp_sem.at[0], dp_sem.at[1], partner)
    small_ref[0:1, :tokens] = mism

    mult = mask * (SOFTENING_HEAT * n_mx * n_my * bc * n_dp * tokens)
    mult = jnp.concatenate([mult, mult], axis=1)
    row = lax.broadcasted_iota(jnp.int32, (128, 128), 0)
    back = jnp.where(row == 0, lse, mult).T
    lt, ls, mu = back[:tokens, 0:1], back[tokens:2 * tokens, 0:1], back[:tokens, 1:2]
    grad_ref[owned] = (jnp.exp(s_blk - ls) - jnp.exp(t_blk - lt)) * mu

    g_far = remote(grad_ref.at[owned], grad_ref.at[owned], ag_sem.at[0], ag_sem.at[1], across)
    relays = [
        remote(grad_ref.at[slot], grad_ref.at[slot], rl_ssem.at[i], rl_rsem.at[i], partner)
        for i, slot in enumerate((owned, far))
    ]
    g_far.start()
    relays[0].start()
    g_far.wait_recv()
    relays[1].start()

    for c in relays:
        c.wait_recv()
    losses.wait_recv()
    totals = jnp.sum(los_all[:, 0, :], axis=0, keepdims=True)
    count = totals[:, 64:65]
    small_ref[1:2, :] = totals / count

    @pl.when(jnp.logical_not(mine))
    def _():
        swap.wait_send()

    for c in [losses, stats, z_copy, g_far] + d_copies + relays:
        c.wait_send()
    grad_ref[...] = grad_ref[...] * (1.0 / count).reshape(1, 1, 1)


def deliver(small_ref, grad_ref, mism_out, loss_out, grad_out, mism_v, loss_v, sem):
    bc = grad_ref.shape[2]
    copies = [
        pltpu.make_async_copy(grad_ref.at[j], grad_out.at[:, j * bc:(j + 1) * bc], sem.at[j])
        for j in range(grad_ref.shape[0])
    ]
    for c in copies:
        c.start()
    mism_v[...] = small_ref[0:1, :mism_v.shape[1]]
    loss_v[...] = small_ref[1:2, 0:1]
    for src, dst in ((mism_v, mism_out), (loss_v, loss_out)):
        copies.append(pltpu.make_async_copy(src, dst, sem.at[len(copies)]))
        copies[-1].start()
    for c in copies:
        c.wait()


def shards(sizes, ts, tw, ss, sw, mask):
    n_dp, n_mx, n_my = sizes
    tokens, bc = ts.shape[0], tw.shape[1]
    cols = sw.shape[1]
    group = n_mx * n_my
    f32 = jnp.float32
    V, D = pltpu.VMEM, pltpu.SemaphoreType.DMA
    hbm = pl.BlockSpec(memory_space=pltpu.HBM)
    vm = pl.BlockSpec(memory_space=pltpu.VMEM)
    held = pl.pallas_call(
        functools.partial(kernel, sizes),
        out_shape=(V((8, 128), f32), V((n_mx, tokens, bc), f32)),
        in_specs=[hbm, hbm, hbm, hbm, hbm],
        out_specs=(vm, vm),
        scratch_shapes=[
            V(ts.shape, ts.dtype), V(tw.shape, tw.dtype), V(ss.shape, ss.dtype),
            V((n_mx, sw.shape[0], bc), sw.dtype), V((1, tokens), mask.dtype),
            V((tokens, bc), f32), V((tokens, bc), f32),
            V((2, tokens, bc), f32), V((2, tokens, bc), f32), V((2, tokens, bc), f32),
            V((tokens, bc), f32), V((tokens, bc), f32),
            V((group, 2, 128), f32), V((n_dp, 1, 128), f32),
            D((3 + TEACHER_CHUNKS + n_mx,)), D((2,)), D((2,)), D((2,)), D((2,)), D((2,)),
            D((2,)), D((2,)), D((2,)), D((2,)), pltpu.SemaphoreType.REGULAR((5,)),
        ],
        compiler_params=pltpu.CompilerParams(
            collective_id=0, has_side_effects=True, vmem_limit_bytes=64_000_000
        ),
    )(ts, tw, ss, sw, mask.reshape(1, tokens))
    mism, loss, grad = pl.pallas_call(
        deliver,
        out_shape=(
            jax.ShapeDtypeStruct((1, tokens), f32),
            jax.ShapeDtypeStruct((1, 1), f32),
            jax.ShapeDtypeStruct((tokens, cols), f32),
        ),
        in_specs=[vm, vm],
        out_specs=(hbm, hbm, hbm),
        scratch_shapes=[V((1, tokens), f32), V((1, 1), f32), D((2 + n_mx,))],
        compiler_params=pltpu.CompilerParams(vmem_limit_bytes=16 * 1024 * 1024),
    )(*[pltpu.with_memory_space_constraint(x, pltpu.VMEM) for x in held])
    return mism.reshape(tokens), loss.reshape(()), grad


def solution(mesh):
    sizes = (mesh.shape["dp"], mesh.shape["mx"], mesh.shape["my"])
    placed = (P("dp", None), P(None, ("mx", "my")), P("dp", "mx"), P("mx", "my"), P("dp"))
    return jax.shard_map(
        functools.partial(shards, sizes), mesh=mesh, in_specs=placed,
        out_specs=(P("dp"), P(), P("dp", "my")), check_vma=False,
    )
```

```python
import functools

import jax
import jax.numpy as jnp
from jax import lax
from jax.experimental import pallas as pl
from jax.experimental.pallas import tpu as pltpu
from jax.sharding import PartitionSpec as P

SOFTENING_HEAT = 2.0
CORES = 2
RING_Y = 8
TEACHER_CHUNKS = 4
MESH = pl.DeviceIdType.MESH


def kernel(
    sizes,
    ts_hbm, tw_hbm, ss_hbm, sw_hbm, mask_hbm,
    small_ref, grad_ref,
    ts, tw, ss, sw, mask_v,
    t_own, t_in, d_send, d_recv, own, z_send, z_recv,
    st_all, los_all,
    ld_sem, tt_sem, dd_ssem, dd_rsem, zz_sem, ag_sem, rl_ssem, rl_rsem, st_sem, dp_sem, token,
):
    n_dp, n_mx, n_my = sizes
    group = n_mx * n_my
    dp, mx, my = lax.axis_index("dp"), lax.axis_index("mx"), lax.axis_index("my")
    zz, cc = lax.div(mx, CORES), lax.rem(mx, CORES)
    oz, oc = 1 - zz, 1 - cc
    me = mx * n_my + my
    partner = {"mx": zz * CORES + oc}
    across = {"mx": oz * CORES + cc}

    def block_of(owner, a):
        one, two = lax.rem(a, 2) * (1 - lax.div(a, 2)), (1 - lax.rem(a, 2)) * lax.div(a, 2)
        core = lax.rem(owner, CORES)
        return lax.rem(owner + 2 * (one * (1 - core) + two * core), n_mx)

    owned, far = block_of(mx, my), block_of(oz * CORES + cc, my)
    tokens, bc = t_own.shape
    kc = tw.shape[0] // TEACHER_CHUNKS

    def remote(src, dst, ssem, rsem, dev):
        return pltpu.make_async_remote_copy(
            src_ref=src, dst_ref=dst, send_sem=ssem, recv_sem=rsem, device_id=dev, device_id_type=MESH
        )

    blocks = [block_of(oz * CORES + oc, my), far, block_of(zz * CORES + oc, my), owned]
    student = [pltpu.make_async_copy(ss_hbm, ss, ld_sem.at[0])]
    for k, block in enumerate(blocks):
        cols = pl.ds(pl.multiple_of(block * bc, bc), bc)
        student.append(pltpu.make_async_copy(sw_hbm.at[:, cols], sw.at[k], ld_sem.at[1 + k]))
    base = 1 + n_mx
    teacher = [pltpu.make_async_copy(ts_hbm, ts, ld_sem.at[base])]
    for k in range(TEACHER_CHUNKS):
        rows = pl.ds(k * kc, kc)
        teacher.append(pltpu.make_async_copy(tw_hbm.at[rows, :], tw.at[rows, :], ld_sem.at[base + 1 + k]))
    mask_load = pltpu.make_async_copy(mask_hbm, mask_v, ld_sem.at[base + 1 + TEACHER_CHUNKS])
    for c in student:
        c.start()
    mask_load.start()

    line = [
        {"mx": lax.rem(mx + i, n_mx), "my": lax.rem(my + j, n_my)}
        for i in (2, 3, 1, 0) for j in range(n_my) if (i, j) != (0, 0)
    ]
    ring_x = n_dp // RING_Y
    px, py = lax.div(dp, RING_Y), lax.rem(dp, RING_Y)

    def plane(i, j):
        return {"dp": lax.rem(px + i, ring_x) * RING_Y + lax.rem(py + j, RING_Y)}

    near = [plane(1, 0), plane(ring_x - 1, 0), plane(0, 1), plane(0, RING_Y - 1)]

    def tell(sem, devices):
        for device in devices:
            pl.semaphore_signal(sem, inc=1, device_id=device, device_id_type=MESH)

    heads = [
        {"mx": (oz if i else zz) * CORES, "my": lax.rem(my + j, n_my)}
        for i in (1, 0) for j in range(n_my) if (i, j) != (0, 0)
    ] + [dict(device, mx=zz * CORES) for device in near]
    barrier = pltpu.get_barrier_semaphore()
    tell(barrier, heads)

    @pl.when(cc == 0)
    def _():
        tell(barrier, [partner])

    def dot(k):
        student[1 + k].wait()
        return jnp.dot(ss[...], sw[k], preferred_element_type=jnp.float32)

    d_copies = [
        remote(d_send.at[k], d_recv.at[k], dd_ssem.at[k], dd_rsem.at[k], partner) for k in range(2)
    ]
    mine = mx == my
    swap = remote(t_own, t_in, tt_sem.at[0], tt_sem.at[1], {"mx": block_of(my, mx), "my": mx})

    def teacher_block():
        teacher[0].wait()
        acc = jnp.zeros((tokens, bc), jnp.float32)
        for k in range(TEACHER_CHUNKS):
            teacher[1 + k].wait()
            rows = slice(k * kc, (k + 1) * kc)
            acc += jnp.dot(ts[:, rows], tw[rows, :], preferred_element_type=jnp.float32)
        t_own[...] = acc * (1.0 / SOFTENING_HEAT)

    def hand_over():
        @pl.when(jnp.logical_not(mine))
        def _():
            swap.start()

        @pl.when(mine)
        def _():
            t_in[...] = t_own[...]

    first = jnp.logical_or(zz == 0, my == 0)
    last = jnp.logical_not(first)
    student[0].wait()
    d_send[0] = dot(0)
    for c in teacher:
        c.start()

    @pl.when(cc == 1)
    def _():
        pl.semaphore_wait(barrier, 1)
        tell(token.at[3], [partner])

    @pl.when(cc == 0)
    def _():
        pl.semaphore_wait(token.at[3], 1)

    d_copies[0].start()
    own[0] = dot(1)
    d_send[1] = dot(2)
    d_copies[1].start()
    own[1] = dot(3)

    @pl.when(first)
    def _():
        teacher_block()

    d_copies[0].wait_recv()
    z_send[...] = own[0] + d_recv[0]
    z_copy = remote(z_send, z_recv, zz_sem.at[0], zz_sem.at[1], across)

    @pl.when(cc == 0)
    def _():
        pl.semaphore_wait(barrier, CORES * len(heads))
        tell(token.at[4], [partner])

    @pl.when(cc == 1)
    def _():
        pl.semaphore_wait(token.at[4], 1)

    z_copy.start()
    tell(token.at[0], near)

    @pl.when(first)
    def _():
        hand_over()

    @pl.when(last)
    def _():
        teacher_block()
        hand_over()

    pl.semaphore_wait(token.at[0], len(near))
    tell(token.at[1], [plane(0, 2), plane(0, RING_Y - 2)])
    pl.semaphore_wait(token.at[1], 2)
    tell(token.at[2], [plane(i, 0) for i in range(1, ring_x)])
    mask_load.wait()
    mask = mask_v[...].astype(jnp.float32)

    d_copies[1].wait_recv()
    mine_sum = own[1] + d_recv[1]
    z_copy.wait_recv()
    s_blk = (mine_sum + z_recv[...]) * (1.0 / SOFTENING_HEAT)

    @pl.when(jnp.logical_not(mine))
    def _():
        swap.wait_recv()

    t_blk = t_in[...]
    mt = jnp.max(t_blk, axis=1, keepdims=True)
    ms = jnp.max(s_blk, axis=1, keepdims=True)
    td, sd = t_blk - mt, s_blk - ms
    et = jnp.exp(td)
    st = jnp.sum(et, axis=1, keepdims=True)
    sS = jnp.sum(jnp.exp(sd), axis=1, keepdims=True)
    cr = jnp.sum(et * (td - sd), axis=1, keepdims=True)
    log_st, log_ss = jnp.log(st), jnp.log(sS)
    kl = cr / st - log_st + log_ss
    lane = lax.broadcasted_iota(jnp.int32, (tokens, 128), 1)
    upper = jnp.where(lane == 0, mt + log_st, kl)
    lower = jnp.broadcast_to(ms + log_ss, (tokens, 128))
    st_all[me] = jnp.concatenate([upper, lower], axis=0).T[:2, :]
    for device in line:
        remote(st_all.at[me], st_all.at[me], st_sem.at[0], st_sem.at[1], device).start()
    others = st_all.at[pl.ds(0, group - 1)]
    stats = remote(others, others, st_sem.at[0], st_sem.at[1], partner)

    stats.wait_recv()
    both = st_all[:, 0, :]
    kls = st_all[:, 1, :][:, :tokens]
    top = jnp.max(both, axis=0, keepdims=True)
    lse = top + jnp.log(jnp.sum(jnp.exp(both - top), axis=0, keepdims=True))
    rel = both - lse
    rel_t, rel_s = rel[:, :tokens], rel[:, tokens:2 * tokens]
    mism = (SOFTENING_HEAT * SOFTENING_HEAT) * jnp.sum(
        jnp.exp(rel_t) * (kls + (rel_t - rel_s)), axis=0, keepdims=True
    )
    half = lax.broadcasted_iota(jnp.int32, los_all.shape[1:], 1) < 64
    los_all[dp] = jnp.where(
        half, jnp.sum(mask * mism, axis=1, keepdims=True), jnp.sum(mask, axis=1, keepdims=True)
    )
    pl.semaphore_wait(token.at[2], ring_x - 1)
    away = [(i, j) for i in range(ring_x) for j in range(RING_Y) if (i, j) != (0, 0)]
    for i, j in sorted(away, key=lambda p: -min(p[0], ring_x - p[0]) - min(p[1], RING_Y - p[1])):
        remote(los_all.at[dp], los_all.at[dp], dp_sem.at[0], dp_sem.at[1], plane(i, j)).start()
    others = los_all.at[pl.ds(0, n_dp - 1)]
    losses = remote(others, others, dp_sem.at[0], dp_sem.at[1], partner)
    small_ref[0:1, :tokens] = mism

    mult = mask * (SOFTENING_HEAT * n_mx * n_my * bc * n_dp * tokens)
    mult = jnp.concatenate([mult, mult], axis=1)
    row = lax.broadcasted_iota(jnp.int32, (128, 128), 0)
    back = jnp.where(row == 0, lse, mult).T
    lt, ls, mu = back[:tokens, 0:1], back[tokens:2 * tokens, 0:1], back[:tokens, 1:2]
    grad_ref[owned] = (jnp.exp(s_blk - ls) - jnp.exp(t_blk - lt)) * mu

    g_far = remote(grad_ref.at[owned], grad_ref.at[owned], ag_sem.at[0], ag_sem.at[1], across)
    relays = [
        remote(grad_ref.at[slot], grad_ref.at[slot], rl_ssem.at[i], rl_rsem.at[i], partner)
        for i, slot in enumerate((owned, far))
    ]
    g_far.start()
    relays[0].start()
    g_far.wait_recv()
    relays[1].start()

    for c in relays:
        c.wait_recv()
    losses.wait_recv()
    totals = jnp.sum(los_all[:, 0, :], axis=0, keepdims=True)
    count = totals[:, 64:65]
    small_ref[1:2, :] = totals / count

    @pl.when(jnp.logical_not(mine))
    def _():
        swap.wait_send()

    for c in [losses, stats, z_copy, g_far] + d_copies + relays:
        c.wait_send()
    grad_ref[...] = grad_ref[...] * (1.0 / count).reshape(1, 1, 1)


def deliver(small_ref, grad_ref, mism_out, loss_out, grad_out, mism_v, loss_v, sem):
    bc = grad_ref.shape[2]
    copies = [
        pltpu.make_async_copy(grad_ref.at[j], grad_out.at[:, j * bc:(j + 1) * bc], sem.at[j])
        for j in range(grad_ref.shape[0])
    ]
    for c in copies:
        c.start()
    mism_v[...] = small_ref[0:1, :mism_v.shape[1]]
    loss_v[...] = small_ref[1:2, 0:1]
    for src, dst in ((mism_v, mism_out), (loss_v, loss_out)):
        copies.append(pltpu.make_async_copy(src, dst, sem.at[len(copies)]))
        copies[-1].start()
    for c in copies:
        c.wait()


def shards(sizes, ts, tw, ss, sw, mask):
    n_dp, n_mx, n_my = sizes
    tokens, bc = ts.shape[0], tw.shape[1]
    cols = sw.shape[1]
    group = n_mx * n_my
    f32 = jnp.float32
    V, D = pltpu.VMEM, pltpu.SemaphoreType.DMA
    hbm = pl.BlockSpec(memory_space=pltpu.HBM)
    vm = pl.BlockSpec(memory_space=pltpu.VMEM)
    held = pl.pallas_call(
        functools.partial(kernel, sizes),
        out_shape=(V((8, 128), f32), V((n_mx, tokens, bc), f32)),
        in_specs=[hbm, hbm, hbm, hbm, hbm],
        out_specs=(vm, vm),
        scratch_shapes=[
            V(ts.shape, ts.dtype), V(tw.shape, tw.dtype), V(ss.shape, ss.dtype),
            V((n_mx, sw.shape[0], bc), sw.dtype), V((1, tokens), mask.dtype),
            V((tokens, bc), f32), V((tokens, bc), f32),
            V((2, tokens, bc), f32), V((2, tokens, bc), f32), V((2, tokens, bc), f32),
            V((tokens, bc), f32), V((tokens, bc), f32),
            V((group, 2, 128), f32), V((n_dp, 1, 128), f32),
            D((3 + TEACHER_CHUNKS + n_mx,)), D((2,)), D((2,)), D((2,)), D((2,)), D((2,)),
            D((2,)), D((2,)), D((2,)), D((2,)), pltpu.SemaphoreType.REGULAR((5,)),
        ],
        compiler_params=pltpu.CompilerParams(
            collective_id=0, has_side_effects=True, vmem_limit_bytes=64_000_000
        ),
    )(ts, tw, ss, sw, mask.reshape(1, tokens))
    mism, loss, grad = pl.pallas_call(
        deliver,
        out_shape=(
            jax.ShapeDtypeStruct((1, tokens), f32),
            jax.ShapeDtypeStruct((1, 1), f32),
            jax.ShapeDtypeStruct((tokens, cols), f32),
        ),
        in_specs=[vm, vm],
        out_specs=(hbm, hbm, hbm),
        scratch_shapes=[V((1, tokens), f32), V((1, 1), f32), D((2 + n_mx,))],
        compiler_params=pltpu.CompilerParams(vmem_limit_bytes=16 * 1024 * 1024),
    )(*[pltpu.with_memory_space_constraint(x, pltpu.VMEM) for x in held])
    return mism.reshape(tokens), loss.reshape(()), grad


def solution(mesh):
    sizes = (mesh.shape["dp"], mesh.shape["mx"], mesh.shape["my"])
    placed = (P("dp", None), P(None, ("mx", "my")), P("dp", "mx"), P("mx", "my"), P("dp"))
    return jax.shard_map(
        functools.partial(shards, sizes), mesh=mesh, in_specs=placed,
        out_specs=(P("dp"), P(), P("dp", "my")), check_vma=False,
    )
```

```python
import functools

import jax
import jax.numpy as jnp
from jax import lax
from jax.experimental import pallas as pl
from jax.experimental.pallas import tpu as pltpu
from jax.sharding import PartitionSpec as P

SOFTENING_HEAT = 2.0
CORES = 2
RING_Y = 8
MESH = pl.DeviceIdType.MESH


def kernel(
    sizes,
    ts_hbm, tw_hbm, ss_hbm, sw_hbm, mask_hbm,
    small_ref, grad_ref,
    ts, tw, ss, sw, mask_v,
    d_send, d_recv, own, z_send, z_recv, g_send,
    st_all, los_all,
    ld_sem, dd_ssem, dd_rsem, zz_ssem, zz_rsem, ag_ssem, ag_rsem, rl_sem, st_sem, dp_sem, token,
):
    n_dp, n_mx, n_my = sizes
    group = n_mx * n_my
    dp, mx, my = lax.axis_index("dp"), lax.axis_index("mx"), lax.axis_index("my")
    zz, cc = lax.div(mx, CORES), lax.rem(mx, CORES)
    oz, oc = 1 - zz, 1 - cc
    me = mx * n_my + my
    partner = {"mx": zz * CORES + oc}
    far = oz * CORES + cc
    tokens, bc = own.shape[1:]

    def remote(src, dst, ssem, rsem, dev):
        return pltpu.make_async_remote_copy(
            src_ref=src, dst_ref=dst, send_sem=ssem, recv_sem=rsem, device_id=dev, device_id_type=MESH
        )

    line = [
        {"mx": lax.rem(mx + i, n_mx), "my": lax.rem(my + j, n_my)}
        for i in (2, 3, 1, 0) for j in range(n_my) if (i, j) != (0, 0)
    ]
    ring_x = n_dp // RING_Y
    px, py = lax.div(dp, RING_Y), lax.rem(dp, RING_Y)

    def plane(i, j):
        return {"dp": lax.rem(px + i, ring_x) * RING_Y + lax.rem(py + j, RING_Y)}

    near = [plane(1, 0), plane(ring_x - 1, 0), plane(0, 1), plane(0, RING_Y - 1)]

    def tell(sem, devices):
        for device in devices:
            pl.semaphore_signal(sem, inc=1, device_id=device, device_id_type=MESH)

    heads = [
        {"mx": (oz if i else zz) * CORES, "my": lax.rem(my + j, n_my)}
        for i in (1, 0) for j in range(n_my) if (i, j) != (0, 0)
    ] + [dict(device, mx=zz * CORES) for device in near]
    barrier = pltpu.get_barrier_semaphore()
    tell(barrier, heads)

    @pl.when(cc == 0)
    def _():
        tell(barrier, [partner])

    blocks = [oz * CORES + oc, far, zz * CORES + oc, mx]
    student = [pltpu.make_async_copy(ss_hbm, ss, ld_sem.at[0])]
    for k, block in enumerate(blocks):
        cols = pl.ds(pl.multiple_of(block * bc, bc), bc)
        student.append(pltpu.make_async_copy(sw_hbm.at[:, cols], sw.at[k], ld_sem.at[1 + k]))
    teacher = [
        pltpu.make_async_copy(ts_hbm, ts, ld_sem.at[1 + n_mx]),
        pltpu.make_async_copy(tw_hbm, tw, ld_sem.at[2 + n_mx]),
    ]
    mask_load = pltpu.make_async_copy(mask_hbm, mask_v, ld_sem.at[3 + n_mx])
    for c in student:
        c.start()

    def dot(k):
        student[1 + k].wait()
        return jnp.dot(ss[...], sw[k], preferred_element_type=jnp.float32)

    d_copies = [
        remote(d_send.at[k], d_recv.at[k], dd_ssem.at[0], dd_rsem.at[k], partner) for k in range(2)
    ]
    here = mx == my
    s_near = remote(z_send.at[0], z_recv.at[0], zz_ssem.at[0], zz_rsem.at[0], {"mx": my, "my": mx})
    s_far = remote(z_send.at[1], z_recv.at[1], zz_ssem.at[1], zz_rsem.at[1], {"mx": my, "my": far})

    student[0].wait()
    d_send[0] = dot(0)
    for c in teacher:
        c.start()
    mask_load.start()

    @pl.when(cc == 1)
    def _():
        pl.semaphore_wait(barrier, 1)
        tell(token.at[3], [partner])

    @pl.when(cc == 0)
    def _():
        pl.semaphore_wait(token.at[3], 1)

    d_copies[0].start()
    own[0] = dot(1)
    d_send[1] = dot(2)
    d_copies[1].start()
    own[1] = dot(3)
    d_copies[0].wait_recv()
    z_send[1] = own[0] + d_recv[0]

    @pl.when(cc == 0)
    def _():
        pl.semaphore_wait(barrier, CORES * len(heads))
        tell(token.at[4], [partner])

    @pl.when(cc == 1)
    def _():
        pl.semaphore_wait(token.at[4], 1)

    s_far.start()
    d_copies[1].wait_recv()

    @pl.when(here)
    def _():
        z_recv[0] = own[1] + d_recv[1]

    @pl.when(jnp.logical_not(here))
    def _():
        z_send[0] = own[1] + d_recv[1]
        s_near.start()

    tell(token.at[0], near)

    for c in teacher:
        c.wait()
    t_blk = jnp.dot(ts[...], tw[...], preferred_element_type=jnp.float32) * (1.0 / SOFTENING_HEAT)
    mt = jnp.max(t_blk, axis=1, keepdims=True)
    td = t_blk - mt
    et = jnp.exp(td)
    st = jnp.sum(et, axis=1, keepdims=True)
    log_st = jnp.log(st)
    tt = jnp.sum(et * td, axis=1, keepdims=True)

    pl.semaphore_wait(token.at[0], len(near))
    tell(token.at[1], [plane(0, 2), plane(0, RING_Y - 2)])
    pl.semaphore_wait(token.at[1], 2)
    tell(token.at[2], [plane(i, 0) for i in range(1, ring_x)])
    mask_load.wait()
    mask = mask_v[...].astype(jnp.float32)

    @pl.when(jnp.logical_not(here))
    def _():
        s_near.wait_recv()

    s_far.wait_recv()
    s_blk = (z_recv[0] + z_recv[1]) * (1.0 / SOFTENING_HEAT)
    ms = jnp.max(s_blk, axis=1, keepdims=True)
    sd = s_blk - ms
    log_ss = jnp.log(jnp.sum(jnp.exp(sd), axis=1, keepdims=True))
    kl = (tt - jnp.sum(et * sd, axis=1, keepdims=True)) / st - log_st + log_ss
    lane = lax.broadcasted_iota(jnp.int32, (tokens, 128), 1)
    upper = jnp.where(lane == 0, mt + log_st, kl)
    lower = jnp.broadcast_to(ms + log_ss, (tokens, 128))
    st_all[me] = jnp.concatenate([upper, lower], axis=0).T[:2, :]
    for device in line:
        remote(st_all.at[me], st_all.at[me], st_sem.at[0], st_sem.at[1], device).start()
    others = st_all.at[pl.ds(0, group - 1)]
    stats = remote(others, others, st_sem.at[0], st_sem.at[1], partner)

    stats.wait_recv()
    both = st_all[:, 0, :]
    kls = st_all[:, 1, :][:, :tokens]
    top = jnp.max(both, axis=0, keepdims=True)
    lse = top + jnp.log(jnp.sum(jnp.exp(both - top), axis=0, keepdims=True))
    rel = both - lse
    rel_t, rel_s = rel[:, :tokens], rel[:, tokens:2 * tokens]
    mism = (SOFTENING_HEAT * SOFTENING_HEAT) * jnp.sum(
        jnp.exp(rel_t) * (kls + (rel_t - rel_s)), axis=0, keepdims=True
    )
    half = lax.broadcasted_iota(jnp.int32, los_all.shape[1:], 1) < 64
    los_all[dp] = jnp.where(
        half, jnp.sum(mask * mism, axis=1, keepdims=True), jnp.sum(mask, axis=1, keepdims=True)
    )
    pl.semaphore_wait(token.at[2], ring_x - 1)
    away = [(i, j) for i in range(ring_x) for j in range(RING_Y) if (i, j) != (0, 0)]
    for i, j in sorted(away, key=lambda p: -min(p[0], ring_x - p[0]) - min(p[1], RING_Y - p[1])):
        remote(los_all.at[dp], los_all.at[dp], dp_sem.at[0], dp_sem.at[1], plane(i, j)).start()
    others = los_all.at[pl.ds(0, n_dp - 1)]
    losses = remote(others, others, dp_sem.at[0], dp_sem.at[1], partner)
    small_ref[0:1, :tokens] = mism

    mult = mask * (SOFTENING_HEAT * n_mx * n_my * bc * n_dp * tokens)
    mult = jnp.concatenate([mult, mult], axis=1)
    row = lax.broadcasted_iota(jnp.int32, (128, 128), 0)
    back = jnp.where(row == 0, lse, mult).T
    lt, ls, mu = back[:tokens, 0:1], back[tokens:2 * tokens, 0:1], back[:tokens, 1:2]
    g_send[...] = (jnp.exp(s_blk - ls) - jnp.exp(t_blk - lt)) * mu

    my_far = (1 - lax.div(my, CORES)) * CORES + lax.rem(my, CORES)
    g_near = remote(g_send, grad_ref.at[my], ag_ssem.at[0], ag_rsem.at[0], {"mx": my, "my": mx})
    g_far = remote(g_send, grad_ref.at[my], ag_ssem.at[1], ag_rsem.at[1], {"mx": my_far, "my": mx})

    @pl.when(jnp.logical_not(here))
    def _():
        g_near.start()

    g_far.start()

    @pl.when(here)
    def _():
        grad_ref[mx] = g_send[...]

    relays = [
        remote(grad_ref.at[slot], grad_ref.at[slot], rl_sem.at[0], rl_sem.at[1], partner) for slot in (mx, far)
    ]

    @pl.when(jnp.logical_not(here))
    def _():
        g_near.wait_recv()

    relays[0].start()
    g_far.wait_recv()
    relays[1].start()
    pair = grad_ref.at[pl.ds(0, 2)]
    relayed = remote(pair, pair, rl_sem.at[0], rl_sem.at[1], partner)
    relayed.wait_recv()
    losses.wait_recv()
    totals = jnp.sum(los_all[:, 0, :], axis=0, keepdims=True)
    count = totals[:, 64:65]
    small_ref[1:2, :] = totals / count

    @pl.when(jnp.logical_not(here))
    def _():
        s_near.wait_send()
        g_near.wait_send()

    halves = remote(d_send, d_recv, dd_ssem.at[0], dd_rsem.at[0], partner)
    for c in [losses, stats, s_far, g_far, halves, relayed]:
        c.wait_send()
    grad_ref[...] = grad_ref[...] * (1.0 / count).reshape(1, 1, 1)


def deliver(small_ref, grad_ref, mism_out, loss_out, grad_out, mism_v, loss_v, sem):
    bc = grad_ref.shape[2]
    copies = [
        pltpu.make_async_copy(grad_ref.at[j], grad_out.at[:, j * bc:(j + 1) * bc], sem.at[j])
        for j in range(grad_ref.shape[0])
    ]
    for c in copies:
        c.start()
    mism_v[...] = small_ref[0:1, :mism_v.shape[1]]
    loss_v[...] = small_ref[1:2, 0:1]
    for src, dst in ((mism_v, mism_out), (loss_v, loss_out)):
        copies.append(pltpu.make_async_copy(src, dst, sem.at[len(copies)]))
        copies[-1].start()
    for c in copies:
        c.wait()


def shards(sizes, ts, tw, ss, sw, mask):
    n_dp, n_mx, n_my = sizes
    tokens, bc = ts.shape[0], tw.shape[1]
    cols = sw.shape[1]
    group = n_mx * n_my
    f32 = jnp.float32
    V, D = pltpu.VMEM, pltpu.SemaphoreType.DMA
    hbm = pl.BlockSpec(memory_space=pltpu.HBM)
    vm = pl.BlockSpec(memory_space=pltpu.VMEM)
    held = pl.pallas_call(
        functools.partial(kernel, sizes),
        out_shape=(V((8, 128), f32), V((n_mx, tokens, bc), f32)),
        in_specs=[hbm, hbm, hbm, hbm, hbm],
        out_specs=(vm, vm),
        scratch_shapes=[
            V(ts.shape, ts.dtype), V(tw.shape, tw.dtype), V(ss.shape, ss.dtype),
            V((n_mx, sw.shape[0], bc), sw.dtype), V((1, tokens), mask.dtype),
            V((2, tokens, bc), f32), V((2, tokens, bc), f32), V((2, tokens, bc), f32),
            V((2, tokens, bc), f32), V((2, tokens, bc), f32), V((tokens, bc), f32),
            V((group, 2, 128), f32), V((n_dp, 1, 128), f32),
            D((4 + n_mx,)), D((1,)), D((2,)), D((2,)), D((2,)), D((2,)), D((2,)), D((2,)), D((2,)), D((2,)),
            pltpu.SemaphoreType.REGULAR((5,)),
        ],
        compiler_params=pltpu.CompilerParams(
            collective_id=0, has_side_effects=True, vmem_limit_bytes=64_000_000
        ),
    )(ts, tw, ss, sw, mask.reshape(1, tokens))
    mism, loss, grad = pl.pallas_call(
        deliver,
        out_shape=(
            jax.ShapeDtypeStruct((1, tokens), f32),
            jax.ShapeDtypeStruct((1, 1), f32),
            jax.ShapeDtypeStruct((tokens, cols), f32),
        ),
        in_specs=[vm, vm],
        out_specs=(hbm, hbm, hbm),
        scratch_shapes=[V((1, tokens), f32), V((1, 1), f32), D((2 + n_mx,))],
        compiler_params=pltpu.CompilerParams(vmem_limit_bytes=16 * 1024 * 1024),
    )(*[pltpu.with_memory_space_constraint(x, pltpu.VMEM) for x in held])
    return mism.reshape(tokens), loss.reshape(()), grad


def solution(mesh):
    sizes = (mesh.shape["dp"], mesh.shape["mx"], mesh.shape["my"])
    placed = (P("dp", None), P(None, ("mx", "my")), P("dp", "mx"), P("mx", "my"), P("dp"))
    return jax.shard_map(
        functools.partial(shards, sizes), mesh=mesh, in_specs=placed,
        out_specs=(P("dp"), P(), P("dp", "my")), check_vma=False,
    )
```

```python
import functools

import jax
import jax.numpy as jnp
from jax import lax
from jax.experimental import pallas as pl
from jax.experimental.pallas import tpu as pltpu
from jax.sharding import PartitionSpec as P

SOFTENING_HEAT = 2.0
CORES = 2
RING_Y = 8
MESH = pl.DeviceIdType.MESH


def kernel(
    sizes,
    ts_hbm, tw_hbm, ss_hbm, sw_hbm, mask_hbm,
    small_ref, grad_ref,
    ts, tw, ss, sw, mask_v,
    d_send, d_recv, own, z_send, z_recv, g_send,
    st_all, los_all,
    ld_sem, dd_ssem, dd_rsem, zz_ssem, zz_rsem, ag_ssem, ag_rsem, rl_sem, st_sem, dp_sem, token,
):
    n_dp, n_mx, n_my = sizes
    group = n_mx * n_my
    dp, mx, my = lax.axis_index("dp"), lax.axis_index("mx"), lax.axis_index("my")
    zz, cc = lax.div(mx, CORES), lax.rem(mx, CORES)
    oz, oc = 1 - zz, 1 - cc
    me = mx * n_my + my
    partner = {"mx": zz * CORES + oc}
    far = oz * CORES + cc
    tokens, bc = own.shape[1:]

    def remote(src, dst, ssem, rsem, dev):
        return pltpu.make_async_remote_copy(
            src_ref=src, dst_ref=dst, send_sem=ssem, recv_sem=rsem, device_id=dev, device_id_type=MESH
        )

    line = [
        {"mx": lax.rem(mx + i, n_mx), "my": lax.rem(my + j, n_my)}
        for i in (2, 3, 1, 0) for j in range(n_my) if (i, j) != (0, 0)
    ]
    ring_x = n_dp // RING_Y
    px, py = lax.div(dp, RING_Y), lax.rem(dp, RING_Y)

    def plane(i, j):
        return {"dp": lax.rem(px + i, ring_x) * RING_Y + lax.rem(py + j, RING_Y)}

    near = [plane(1, 0), plane(ring_x - 1, 0), plane(0, 1), plane(0, RING_Y - 1)]

    def tell(sem, devices):
        for device in devices:
            pl.semaphore_signal(sem, inc=1, device_id=device, device_id_type=MESH)

    ring_z = n_mx // CORES * n_my
    z = zz * n_my + my

    def along(k, core):
        to = lax.rem(z + k, ring_z)
        return {"mx": lax.div(to, n_my) * CORES + core, "my": lax.rem(to, n_my)}

    steps = [4, 3, 5, 2, 6]
    heads = [along(k, 0) for k in steps] + [dict(device, mx=zz * CORES) for device in near]
    beside = [along(k, 1) for k in (1, ring_z - 1)]
    barrier = pltpu.get_barrier_semaphore()
    tell(barrier, heads + beside)

    @pl.when(cc == 0)
    def _():
        tell(barrier, [partner])

    blocks = [oz * CORES + oc, far, zz * CORES + oc, mx]
    student = [pltpu.make_async_copy(ss_hbm, ss, ld_sem.at[0])]
    for k, block in enumerate(blocks):
        cols = pl.ds(pl.multiple_of(block * bc, bc), bc)
        student.append(pltpu.make_async_copy(sw_hbm.at[:, cols], sw.at[k], ld_sem.at[1 + k]))
    teacher = [
        pltpu.make_async_copy(ts_hbm, ts, ld_sem.at[1 + n_mx]),
        pltpu.make_async_copy(tw_hbm, tw, ld_sem.at[2 + n_mx]),
    ]
    mask_load = pltpu.make_async_copy(mask_hbm, mask_v, ld_sem.at[3 + n_mx])
    for c in student:
        c.start()

    def dot(k):
        student[1 + k].wait()
        return jnp.dot(ss[...], sw[k], preferred_element_type=jnp.float32)

    d_copies = [
        remote(d_send.at[k], d_recv.at[k], dd_ssem.at[0], dd_rsem.at[k], partner) for k in range(2)
    ]
    here = mx == my
    s_near = remote(z_send.at[0], z_recv.at[0], zz_ssem.at[0], zz_rsem.at[0], {"mx": my, "my": mx})
    s_far = remote(z_send.at[1], z_recv.at[1], zz_ssem.at[1], zz_rsem.at[1], {"mx": my, "my": far})

    student[0].wait()
    d_send[0] = dot(0)
    for c in teacher:
        c.start()
    mask_load.start()

    @pl.when(cc == 1)
    def _():
        pl.semaphore_wait(barrier, 1 + CORES * len(beside))
        tell(token.at[3], [partner])
        tell(token.at[5], [along(k, core) for k in (1, ring_z - 1) for core in range(CORES)])

    @pl.when(cc == 0)
    def _():
        pl.semaphore_wait(token.at[3], 1)

    d_copies[0].start()
    own[0] = dot(1)
    d_send[1] = dot(2)
    d_copies[1].start()
    own[1] = dot(3)
    d_copies[0].wait_recv()
    z_send[1] = own[0] + d_recv[0]

    def finish_near():
        d_copies[1].wait_recv()

        @pl.when(here)
        def _():
            z_recv[0] = own[1] + d_recv[1]

        @pl.when(jnp.logical_not(here))
        def _():
            z_send[0] = own[1] + d_recv[1]

    away_by = lax.rem(lax.div(my, CORES) * n_my + mx + ring_z - z, ring_z)
    short = jnp.logical_or(away_by <= 2, away_by >= ring_z - 2)
    soon = jnp.logical_and(short, jnp.logical_or(zz == 0, my == 0))

    @pl.when(soon)
    def _():
        finish_near()

    pl.semaphore_wait(token.at[5], len(beside))

    @pl.when(jnp.logical_and(soon, jnp.logical_not(here)))
    def _():
        s_near.start()

    @pl.when(cc == 0)
    def _():
        pl.semaphore_wait(barrier, CORES * len(heads))
        tell(token.at[4], [partner])

    @pl.when(cc == 1)
    def _():
        pl.semaphore_wait(token.at[4], 1)

    s_far.start()

    @pl.when(jnp.logical_not(soon))
    def _():
        finish_near()

    @pl.when(jnp.logical_and(jnp.logical_not(soon), jnp.logical_not(here)))
    def _():
        s_near.start()

    tell(token.at[0], near)

    for c in teacher:
        c.wait()
    t_blk = jnp.dot(ts[...], tw[...], preferred_element_type=jnp.float32) * (1.0 / SOFTENING_HEAT)
    mt = jnp.max(t_blk, axis=1, keepdims=True)
    td = t_blk - mt
    et = jnp.exp(td)
    st = jnp.sum(et, axis=1, keepdims=True)
    log_st = jnp.log(st)
    tt = jnp.sum(et * td, axis=1, keepdims=True)

    pl.semaphore_wait(token.at[0], len(near))
    tell(token.at[1], [plane(0, 2), plane(0, RING_Y - 2)])
    pl.semaphore_wait(token.at[1], 2)
    tell(token.at[2], [plane(i, 0) for i in range(1, ring_x)])
    mask_load.wait()
    mask = mask_v[...].astype(jnp.float32)

    @pl.when(jnp.logical_not(here))
    def _():
        s_near.wait_recv()

    s_far.wait_recv()
    s_blk = (z_recv[0] + z_recv[1]) * (1.0 / SOFTENING_HEAT)
    ms = jnp.max(s_blk, axis=1, keepdims=True)
    sd = s_blk - ms
    log_ss = jnp.log(jnp.sum(jnp.exp(sd), axis=1, keepdims=True))
    kl = (tt - jnp.sum(et * sd, axis=1, keepdims=True)) / st - log_st + log_ss
    lane = lax.broadcasted_iota(jnp.int32, (tokens, 128), 1)
    upper = jnp.where(lane == 0, mt + log_st, kl)
    lower = jnp.broadcast_to(ms + log_ss, (tokens, 128))
    st_all[me] = jnp.concatenate([upper, lower], axis=0).T[:2, :]
    for device in line:
        remote(st_all.at[me], st_all.at[me], st_sem.at[0], st_sem.at[1], device).start()
    others = st_all.at[pl.ds(0, group - 1)]
    stats = remote(others, others, st_sem.at[0], st_sem.at[1], partner)

    stats.wait_recv()
    both = st_all[:, 0, :]
    kls = st_all[:, 1, :][:, :tokens]
    top = jnp.max(both, axis=0, keepdims=True)
    lse = top + jnp.log(jnp.sum(jnp.exp(both - top), axis=0, keepdims=True))
    rel = both - lse
    rel_t, rel_s = rel[:, :tokens], rel[:, tokens:2 * tokens]
    mism = (SOFTENING_HEAT * SOFTENING_HEAT) * jnp.sum(
        jnp.exp(rel_t) * (kls + (rel_t - rel_s)), axis=0, keepdims=True
    )
    half = lax.broadcasted_iota(jnp.int32, los_all.shape[1:], 1) < 64
    los_all[dp] = jnp.where(
        half, jnp.sum(mask * mism, axis=1, keepdims=True), jnp.sum(mask, axis=1, keepdims=True)
    )
    pl.semaphore_wait(token.at[2], ring_x - 1)
    away = [(i, j) for i in range(ring_x) for j in range(RING_Y) if (i, j) != (0, 0)]
    for i, j in sorted(away, key=lambda p: -min(p[0], ring_x - p[0]) - min(p[1], RING_Y - p[1])):
        remote(los_all.at[dp], los_all.at[dp], dp_sem.at[0], dp_sem.at[1], plane(i, j)).start()
    others = los_all.at[pl.ds(0, n_dp - 1)]
    losses = remote(others, others, dp_sem.at[0], dp_sem.at[1], partner)
    small_ref[0:1, :tokens] = mism

    mult = mask * (SOFTENING_HEAT * n_mx * n_my * bc * n_dp * tokens)
    mult = jnp.concatenate([mult, mult], axis=1)
    row = lax.broadcasted_iota(jnp.int32, (128, 128), 0)
    back = jnp.where(row == 0, lse, mult).T
    lt, ls, mu = back[:tokens, 0:1], back[tokens:2 * tokens, 0:1], back[:tokens, 1:2]
    g_send[...] = (jnp.exp(s_blk - ls) - jnp.exp(t_blk - lt)) * mu

    my_far = (1 - lax.div(my, CORES)) * CORES + lax.rem(my, CORES)
    g_near = remote(g_send, grad_ref.at[my], ag_ssem.at[0], ag_rsem.at[0], {"mx": my, "my": mx})
    g_far = remote(g_send, grad_ref.at[my], ag_ssem.at[1], ag_rsem.at[1], {"mx": my_far, "my": mx})

    @pl.when(jnp.logical_not(here))
    def _():
        g_near.start()

    g_far.start()

    @pl.when(here)
    def _():
        grad_ref[mx] = g_send[...]

    relays = [
        remote(grad_ref.at[slot], grad_ref.at[slot], rl_sem.at[0], rl_sem.at[1], partner) for slot in (mx, far)
    ]

    @pl.when(jnp.logical_not(here))
    def _():
        g_near.wait_recv()

    relays[0].start()
    g_far.wait_recv()
    relays[1].start()
    pair = grad_ref.at[pl.ds(0, 2)]
    relayed = remote(pair, pair, rl_sem.at[0], rl_sem.at[1], partner)
    relayed.wait_recv()
    losses.wait_recv()
    totals = jnp.sum(los_all[:, 0, :], axis=0, keepdims=True)
    count = totals[:, 64:65]
    small_ref[1:2, :] = totals / count

    @pl.when(jnp.logical_not(here))
    def _():
        s_near.wait_send()
        g_near.wait_send()

    halves = remote(d_send, d_recv, dd_ssem.at[0], dd_rsem.at[0], partner)
    for c in [losses, stats, s_far, g_far, halves, relayed]:
        c.wait_send()
    grad_ref[...] = grad_ref[...] * (1.0 / count).reshape(1, 1, 1)


def deliver(small_ref, grad_ref, mism_out, loss_out, grad_out, mism_v, loss_v, sem):
    bc = grad_ref.shape[2]
    copies = [
        pltpu.make_async_copy(grad_ref.at[j], grad_out.at[:, j * bc:(j + 1) * bc], sem.at[j])
        for j in range(grad_ref.shape[0])
    ]
    for c in copies:
        c.start()
    mism_v[...] = small_ref[0:1, :mism_v.shape[1]]
    loss_v[...] = small_ref[1:2, 0:1]
    for src, dst in ((mism_v, mism_out), (loss_v, loss_out)):
        copies.append(pltpu.make_async_copy(src, dst, sem.at[len(copies)]))
        copies[-1].start()
    for c in copies:
        c.wait()


def shards(sizes, ts, tw, ss, sw, mask):
    n_dp, n_mx, n_my = sizes
    tokens, bc = ts.shape[0], tw.shape[1]
    cols = sw.shape[1]
    group = n_mx * n_my
    f32 = jnp.float32
    V, D = pltpu.VMEM, pltpu.SemaphoreType.DMA
    hbm = pl.BlockSpec(memory_space=pltpu.HBM)
    vm = pl.BlockSpec(memory_space=pltpu.VMEM)
    held = pl.pallas_call(
        functools.partial(kernel, sizes),
        out_shape=(V((8, 128), f32), V((n_mx, tokens, bc), f32)),
        in_specs=[hbm, hbm, hbm, hbm, hbm],
        out_specs=(vm, vm),
        scratch_shapes=[
            V(ts.shape, ts.dtype), V(tw.shape, tw.dtype), V(ss.shape, ss.dtype),
            V((n_mx, sw.shape[0], bc), sw.dtype), V((1, tokens), mask.dtype),
            V((2, tokens, bc), f32), V((2, tokens, bc), f32), V((2, tokens, bc), f32),
            V((2, tokens, bc), f32), V((2, tokens, bc), f32), V((tokens, bc), f32),
            V((group, 2, 128), f32), V((n_dp, 1, 128), f32),
            D((4 + n_mx,)), D((1,)), D((2,)), D((2,)), D((2,)), D((2,)), D((2,)), D((2,)), D((2,)), D((2,)),
            pltpu.SemaphoreType.REGULAR((6,)),
        ],
        compiler_params=pltpu.CompilerParams(
            collective_id=0, has_side_effects=True, vmem_limit_bytes=64_000_000
        ),
    )(ts, tw, ss, sw, mask.reshape(1, tokens))
    mism, loss, grad = pl.pallas_call(
        deliver,
        out_shape=(
            jax.ShapeDtypeStruct((1, tokens), f32),
            jax.ShapeDtypeStruct((1, 1), f32),
            jax.ShapeDtypeStruct((tokens, cols), f32),
        ),
        in_specs=[vm, vm],
        out_specs=(hbm, hbm, hbm),
        scratch_shapes=[V((1, tokens), f32), V((1, 1), f32), D((2 + n_mx,))],
        compiler_params=pltpu.CompilerParams(vmem_limit_bytes=16 * 1024 * 1024),
    )(*[pltpu.with_memory_space_constraint(x, pltpu.VMEM) for x in held])
    return mism.reshape(tokens), loss.reshape(()), grad


def solution(mesh):
    sizes = (mesh.shape["dp"], mesh.shape["mx"], mesh.shape["my"])
    placed = (P("dp", None), P(None, ("mx", "my")), P("dp", "mx"), P("mx", "my"), P("dp"))
    return jax.shard_map(
        functools.partial(shards, sizes), mesh=mesh, in_specs=placed,
        out_specs=(P("dp"), P(), P("dp", "my")), check_vma=False,
    )
```

```python
import functools

import jax
import jax.numpy as jnp
from jax import lax
from jax.experimental import pallas as pl
from jax.experimental.pallas import tpu as pltpu
from jax.sharding import PartitionSpec as P

SOFTENING_HEAT = 2.0
CORES = 2
RING_Y = 8
MESH = pl.DeviceIdType.MESH


def kernel(
    sizes,
    ts_hbm, tw_hbm, ss_hbm, sw_hbm, mask_hbm,
    small_ref, grad_ref,
    ts, tw, ss, sw, mask_v,
    d_send, d_recv, own, z_send, z_recv, g_send,
    st_all, los_all,
    ld_sem, dd_ssem, dd_rsem, zz_ssem, zz_rsem, ag_ssem, ag_rsem, rl_sem, st_sem, dp_sem, token,
):
    n_dp, n_mx, n_my = sizes
    group = n_mx * n_my
    dp, mx, my = lax.axis_index("dp"), lax.axis_index("mx"), lax.axis_index("my")
    zz, cc = lax.div(mx, CORES), lax.rem(mx, CORES)
    oz, oc = 1 - zz, 1 - cc
    me = mx * n_my + my
    partner = {"mx": zz * CORES + oc}
    far = oz * CORES + cc
    tokens, bc = own.shape[1:]

    def remote(src, dst, ssem, rsem, dev):
        return pltpu.make_async_remote_copy(
            src_ref=src, dst_ref=dst, send_sem=ssem, recv_sem=rsem, device_id=dev, device_id_type=MESH
        )

    line = [
        {"mx": lax.rem(mx + i, n_mx), "my": lax.rem(my + j, n_my)}
        for i in (2, 3, 1, 0) for j in range(n_my) if (i, j) != (0, 0)
    ]
    ring_x = n_dp // RING_Y
    px, py = lax.div(dp, RING_Y), lax.rem(dp, RING_Y)

    def plane(i, j):
        return {"dp": lax.rem(px + i, ring_x) * RING_Y + lax.rem(py + j, RING_Y)}

    near = [plane(1, 0), plane(ring_x - 1, 0), plane(0, 1), plane(0, RING_Y - 1)]

    def tell(sem, devices):
        for device in devices:
            pl.semaphore_signal(sem, inc=1, device_id=device, device_id_type=MESH)

    ring_z = n_mx // CORES * n_my
    z = zz * n_my + my

    def along(k, core):
        to = lax.rem(z + k, ring_z)
        return {"mx": lax.div(to, n_my) * CORES + core, "my": lax.rem(to, n_my)}

    below, above = lax.div(z + ring_z - 1, ring_z), 1 - lax.div(z + 1, ring_z)
    steps = [4, 3, 5, 2, 6]
    heads = [along(k, 0) for k in steps] + [dict(device, mx=zz * CORES) for device in near]
    barrier = pltpu.get_barrier_semaphore()
    tell(barrier, heads + [along(ring_z - 1, below), along(1, above)])

    @pl.when(cc == 0)
    def _():
        tell(barrier, [partner])

    blocks = [oz * CORES + oc, far, zz * CORES + oc, mx]
    student = [pltpu.make_async_copy(ss_hbm, ss, ld_sem.at[0])]
    for k, block in enumerate(blocks):
        cols = pl.ds(pl.multiple_of(block * bc, bc), bc)
        student.append(pltpu.make_async_copy(sw_hbm.at[:, cols], sw.at[k], ld_sem.at[1 + k]))
    teacher = [
        pltpu.make_async_copy(ts_hbm, ts, ld_sem.at[1 + n_mx]),
        pltpu.make_async_copy(tw_hbm, tw, ld_sem.at[2 + n_mx]),
    ]
    mask_load = pltpu.make_async_copy(mask_hbm, mask_v, ld_sem.at[3 + n_mx])
    for c in student:
        c.start()

    def dot(k):
        student[1 + k].wait()
        return jnp.dot(ss[...], sw[k], preferred_element_type=jnp.float32)

    d_copies = [
        remote(d_send.at[k], d_recv.at[k], dd_ssem.at[0], dd_rsem.at[k], partner) for k in range(2)
    ]
    here = mx == my
    s_near = remote(z_send.at[0], z_recv.at[0], zz_ssem.at[0], zz_rsem.at[0], {"mx": my, "my": mx})
    s_far = remote(z_send.at[1], z_recv.at[1], zz_ssem.at[1], zz_rsem.at[1], {"mx": my, "my": far})

    student[0].wait()
    d_send[0] = dot(0)
    for c in teacher:
        c.start()
    mask_load.start()

    @pl.when(cc == 1)
    def _():
        pl.semaphore_wait(barrier, 1 + CORES * (below + above))
        tell(token.at[3], [partner])

        @pl.when(below == 1)
        def _():
            tell(token.at[5], [along(ring_z - 1, core) for core in range(CORES)])

        @pl.when(above == 1)
        def _():
            tell(token.at[5], [along(1, core) for core in range(CORES)])

    @pl.when(cc == 0)
    def _():
        pl.semaphore_wait(token.at[3], 1)

    d_copies[0].start()
    own[0] = dot(1)
    d_send[1] = dot(2)
    d_copies[1].start()
    own[1] = dot(3)
    d_copies[0].wait_recv()
    z_send[1] = own[0] + d_recv[0]

    def finish_near():
        d_copies[1].wait_recv()

        @pl.when(here)
        def _():
            z_recv[0] = own[1] + d_recv[1]

        @pl.when(jnp.logical_not(here))
        def _():
            z_send[0] = own[1] + d_recv[1]

    away_by = lax.rem(lax.div(my, CORES) * n_my + mx + ring_z - z, ring_z)
    short = jnp.logical_or(away_by <= 2, away_by >= ring_z - 2)
    soon = jnp.logical_and(short, zz == 0)

    @pl.when(soon)
    def _():
        finish_near()
        pl.semaphore_wait(token.at[5], below + above)

    @pl.when(jnp.logical_and(soon, jnp.logical_not(here)))
    def _():
        s_near.start()

    @pl.when(cc == 0)
    def _():
        pl.semaphore_wait(barrier, CORES * (len(heads) + 2 - below - above))
        tell(token.at[4], [partner])

    @pl.when(cc == 1)
    def _():
        pl.semaphore_wait(token.at[4], 1)

    s_far.start()

    @pl.when(jnp.logical_not(soon))
    def _():
        finish_near()

    @pl.when(jnp.logical_and(jnp.logical_not(soon), jnp.logical_not(here)))
    def _():
        s_near.start()

    tell(token.at[0], near)

    for c in teacher:
        c.wait()
    t_blk = jnp.dot(ts[...], tw[...], preferred_element_type=jnp.float32) * (1.0 / SOFTENING_HEAT)
    mt = jnp.max(t_blk, axis=1, keepdims=True)
    td = t_blk - mt
    et = jnp.exp(td)
    st = jnp.sum(et, axis=1, keepdims=True)
    log_st = jnp.log(st)
    tt = jnp.sum(et * td, axis=1, keepdims=True)

    @pl.when(jnp.logical_not(soon))
    def _():
        pl.semaphore_wait(token.at[5], below + above)

    pl.semaphore_wait(token.at[0], len(near))
    tell(token.at[1], [plane(0, 2), plane(0, RING_Y - 2)])
    pl.semaphore_wait(token.at[1], 2)
    tell(token.at[2], [plane(i, 0) for i in range(1, ring_x)])
    mask_load.wait()
    mask = mask_v[...].astype(jnp.float32)

    @pl.when(jnp.logical_not(here))
    def _():
        s_near.wait_recv()

    s_far.wait_recv()
    s_blk = (z_recv[0] + z_recv[1]) * (1.0 / SOFTENING_HEAT)
    ms = jnp.max(s_blk, axis=1, keepdims=True)
    sd = s_blk - ms
    log_ss = jnp.log(jnp.sum(jnp.exp(sd), axis=1, keepdims=True))
    kl = (tt - jnp.sum(et * sd, axis=1, keepdims=True)) / st - log_st + log_ss
    lane = lax.broadcasted_iota(jnp.int32, (tokens, 128), 1)
    upper = jnp.where(lane == 0, mt + log_st, kl)
    lower = jnp.broadcast_to(ms + log_ss, (tokens, 128))
    st_all[me] = jnp.concatenate([upper, lower], axis=0).T[:2, :]
    for device in line:
        remote(st_all.at[me], st_all.at[me], st_sem.at[0], st_sem.at[1], device).start()
    others = st_all.at[pl.ds(0, group - 1)]
    stats = remote(others, others, st_sem.at[0], st_sem.at[1], partner)

    stats.wait_recv()
    both = st_all[:, 0, :]
    kls = st_all[:, 1, :][:, :tokens]
    top = jnp.max(both, axis=0, keepdims=True)
    lse = top + jnp.log(jnp.sum(jnp.exp(both - top), axis=0, keepdims=True))
    rel = both - lse
    rel_t, rel_s = rel[:, :tokens], rel[:, tokens:2 * tokens]
    mism = (SOFTENING_HEAT * SOFTENING_HEAT) * jnp.sum(
        jnp.exp(rel_t) * (kls + (rel_t - rel_s)), axis=0, keepdims=True
    )
    half = lax.broadcasted_iota(jnp.int32, los_all.shape[1:], 1) < 64
    los_all[dp] = jnp.where(
        half, jnp.sum(mask * mism, axis=1, keepdims=True), jnp.sum(mask, axis=1, keepdims=True)
    )
    pl.semaphore_wait(token.at[2], ring_x - 1)
    away = [(i, j) for i in range(ring_x) for j in range(RING_Y) if (i, j) != (0, 0)]
    for i, j in sorted(away, key=lambda p: -min(p[0], ring_x - p[0]) - min(p[1], RING_Y - p[1])):
        remote(los_all.at[dp], los_all.at[dp], dp_sem.at[0], dp_sem.at[1], plane(i, j)).start()
    others = los_all.at[pl.ds(0, n_dp - 1)]
    losses = remote(others, others, dp_sem.at[0], dp_sem.at[1], partner)
    small_ref[0:1, :tokens] = mism

    mult = mask * (SOFTENING_HEAT * n_mx * n_my * bc * n_dp * tokens)
    mult = jnp.concatenate([mult, mult], axis=1)
    row = lax.broadcasted_iota(jnp.int32, (128, 128), 0)
    back = jnp.where(row == 0, lse, mult).T
    lt, ls, mu = back[:tokens, 0:1], back[tokens:2 * tokens, 0:1], back[:tokens, 1:2]
    g_send[...] = (jnp.exp(s_blk - ls) - jnp.exp(t_blk - lt)) * mu

    my_far = (1 - lax.div(my, CORES)) * CORES + lax.rem(my, CORES)
    g_near = remote(g_send, grad_ref.at[my], ag_ssem.at[0], ag_rsem.at[0], {"mx": my, "my": mx})
    g_far = remote(g_send, grad_ref.at[my], ag_ssem.at[1], ag_rsem.at[1], {"mx": my_far, "my": mx})

    @pl.when(jnp.logical_not(here))
    def _():
        g_near.start()

    g_far.start()

    @pl.when(here)
    def _():
        grad_ref[mx] = g_send[...]

    relays = [
        remote(grad_ref.at[slot], grad_ref.at[slot], rl_sem.at[0], rl_sem.at[1], partner) for slot in (mx, far)
    ]

    @pl.when(jnp.logical_not(here))
    def _():
        g_near.wait_recv()

    relays[0].start()
    g_far.wait_recv()
    relays[1].start()
    pair = grad_ref.at[pl.ds(0, 2)]
    relayed = remote(pair, pair, rl_sem.at[0], rl_sem.at[1], partner)
    relayed.wait_recv()
    losses.wait_recv()
    totals = jnp.sum(los_all[:, 0, :], axis=0, keepdims=True)
    count = totals[:, 64:65]
    small_ref[1:2, :] = totals / count

    @pl.when(jnp.logical_not(here))
    def _():
        s_near.wait_send()
        g_near.wait_send()

    halves = remote(d_send, d_recv, dd_ssem.at[0], dd_rsem.at[0], partner)
    for c in [losses, stats, s_far, g_far, halves, relayed]:
        c.wait_send()
    grad_ref[...] = grad_ref[...] * (1.0 / count).reshape(1, 1, 1)


def deliver(small_ref, grad_ref, mism_out, loss_out, grad_out, mism_v, loss_v, sem):
    bc = grad_ref.shape[2]
    copies = [
        pltpu.make_async_copy(grad_ref.at[j], grad_out.at[:, j * bc:(j + 1) * bc], sem.at[j])
        for j in range(grad_ref.shape[0])
    ]
    for c in copies:
        c.start()
    mism_v[...] = small_ref[0:1, :mism_v.shape[1]]
    loss_v[...] = small_ref[1:2, 0:1]
    for src, dst in ((mism_v, mism_out), (loss_v, loss_out)):
        copies.append(pltpu.make_async_copy(src, dst, sem.at[len(copies)]))
        copies[-1].start()
    for c in copies:
        c.wait()


def shards(sizes, ts, tw, ss, sw, mask):
    n_dp, n_mx, n_my = sizes
    tokens, bc = ts.shape[0], tw.shape[1]
    cols = sw.shape[1]
    group = n_mx * n_my
    f32 = jnp.float32
    V, D = pltpu.VMEM, pltpu.SemaphoreType.DMA
    hbm = pl.BlockSpec(memory_space=pltpu.HBM)
    vm = pl.BlockSpec(memory_space=pltpu.VMEM)
    held = pl.pallas_call(
        functools.partial(kernel, sizes),
        out_shape=(V((8, 128), f32), V((n_mx, tokens, bc), f32)),
        in_specs=[hbm, hbm, hbm, hbm, hbm],
        out_specs=(vm, vm),
        scratch_shapes=[
            V(ts.shape, ts.dtype), V(tw.shape, tw.dtype), V(ss.shape, ss.dtype),
            V((n_mx, sw.shape[0], bc), sw.dtype), V((1, tokens), mask.dtype),
            V((2, tokens, bc), f32), V((2, tokens, bc), f32), V((2, tokens, bc), f32),
            V((2, tokens, bc), f32), V((2, tokens, bc), f32), V((tokens, bc), f32),
            V((group, 2, 128), f32), V((n_dp, 1, 128), f32),
            D((4 + n_mx,)), D((1,)), D((2,)), D((2,)), D((2,)), D((2,)), D((2,)), D((2,)), D((2,)), D((2,)),
            pltpu.SemaphoreType.REGULAR((6,)),
        ],
        compiler_params=pltpu.CompilerParams(
            collective_id=0, has_side_effects=True, vmem_limit_bytes=64_000_000
        ),
    )(ts, tw, ss, sw, mask.reshape(1, tokens))
    mism, loss, grad = pl.pallas_call(
        deliver,
        out_shape=(
            jax.ShapeDtypeStruct((1, tokens), f32),
            jax.ShapeDtypeStruct((1, 1), f32),
            jax.ShapeDtypeStruct((tokens, cols), f32),
        ),
        in_specs=[vm, vm],
        out_specs=(hbm, hbm, hbm),
        scratch_shapes=[V((1, tokens), f32), V((1, 1), f32), D((2 + n_mx,))],
        compiler_params=pltpu.CompilerParams(vmem_limit_bytes=16 * 1024 * 1024),
    )(*[pltpu.with_memory_space_constraint(x, pltpu.VMEM) for x in held])
    return mism.reshape(tokens), loss.reshape(()), grad


def solution(mesh):
    sizes = (mesh.shape["dp"], mesh.shape["mx"], mesh.shape["my"])
    placed = (P("dp", None), P(None, ("mx", "my")), P("dp", "mx"), P("mx", "my"), P("dp"))
    return jax.shard_map(
        functools.partial(shards, sizes), mesh=mesh, in_specs=placed,
        out_specs=(P("dp"), P(), P("dp", "my")), check_vma=False,
    )
```

```python
import functools

import jax
import jax.numpy as jnp
from jax import lax
from jax.experimental import pallas as pl
from jax.experimental.pallas import tpu as pltpu
from jax.sharding import PartitionSpec as P

SOFTENING_HEAT = 2.0
CORES = 2
RING_Y = 8
MESH = pl.DeviceIdType.MESH


def kernel(
    sizes,
    ts_hbm, tw_hbm, ss_hbm, sw_hbm, mask_hbm,
    small_ref, grad_ref,
    ts, tw, ss, sw, mask_v,
    d_send, d_recv, own, z_send, z_recv, g_send,
    st_all, los_all,
    ld_sem, dd_ssem, dd_rsem, zz_ssem, zz_rsem, ag_ssem, ag_rsem, rl_sem, st_sem, dp_sem, token,
):
    n_dp, n_mx, n_my = sizes
    group = n_mx * n_my
    dp, mx, my = lax.axis_index("dp"), lax.axis_index("mx"), lax.axis_index("my")
    zz, cc = lax.div(mx, CORES), lax.rem(mx, CORES)
    oz, oc = 1 - zz, 1 - cc
    me = mx * n_my + my
    partner = {"mx": zz * CORES + oc}
    far = oz * CORES + cc
    tokens, bc = own.shape[1:]

    def remote(src, dst, ssem, rsem, dev):
        return pltpu.make_async_remote_copy(
            src_ref=src, dst_ref=dst, send_sem=ssem, recv_sem=rsem, device_id=dev, device_id_type=MESH
        )

    line = [
        {"mx": lax.rem(mx + i, n_mx), "my": lax.rem(my + j, n_my)}
        for i in (2, 3, 1, 0) for j in range(n_my) if (i, j) != (0, 0)
    ]
    ring_x = n_dp // RING_Y
    px, py = lax.div(dp, RING_Y), lax.rem(dp, RING_Y)

    def plane(i, j):
        return {"dp": lax.rem(px + i, ring_x) * RING_Y + lax.rem(py + j, RING_Y)}

    near = [plane(1, 0), plane(ring_x - 1, 0), plane(0, 1), plane(0, RING_Y - 1)]

    def tell(sem, devices):
        for device in devices:
            pl.semaphore_signal(sem, inc=1, device_id=device, device_id_type=MESH)

    ring_z = n_mx // CORES * n_my
    z = zz * n_my + my

    def along(k, core):
        to = lax.rem(z + k, ring_z)
        return {"mx": lax.div(to, n_my) * CORES + core, "my": lax.rem(to, n_my)}

    below, above = lax.div(z + ring_z - 1, ring_z), 1 - lax.div(z + 1, ring_z)
    steps = [4, 3, 5, 2, 6]
    heads = [along(k, 0) for k in steps] + [dict(device, mx=zz * CORES) for device in near]
    barrier = pltpu.get_barrier_semaphore()
    tell(barrier, heads + [along(ring_z - 1, below), along(1, above)])

    @pl.when(cc == 0)
    def _():
        tell(barrier, [partner])

    blocks = [oz * CORES + oc, far, zz * CORES + oc, mx]
    student = [pltpu.make_async_copy(ss_hbm, ss, ld_sem.at[0])]
    for k, block in enumerate(blocks):
        cols = pl.ds(pl.multiple_of(block * bc, bc), bc)
        student.append(pltpu.make_async_copy(sw_hbm.at[:, cols], sw.at[k], ld_sem.at[1 + k]))
    teacher = [
        pltpu.make_async_copy(ts_hbm, ts, ld_sem.at[1 + n_mx]),
        pltpu.make_async_copy(tw_hbm, tw, ld_sem.at[2 + n_mx]),
    ]
    mask_load = pltpu.make_async_copy(mask_hbm, mask_v, ld_sem.at[3 + n_mx])
    for c in student:
        c.start()

    def dot(k):
        student[1 + k].wait()
        return jnp.dot(ss[...], sw[k], preferred_element_type=jnp.float32)

    d_copies = [
        remote(d_send.at[k], d_recv.at[k], dd_ssem.at[0], dd_rsem.at[k], partner) for k in range(2)
    ]
    here = mx == my
    s_near = remote(z_send.at[0], z_recv.at[0], zz_ssem.at[0], zz_rsem.at[0], {"mx": my, "my": mx})
    s_far = remote(z_send.at[1], z_recv.at[1], zz_ssem.at[1], zz_rsem.at[1], {"mx": my, "my": far})

    student[0].wait()
    d_send[0] = dot(0)
    for c in teacher:
        c.start()
    mask_load.start()

    @pl.when(cc == 1)
    def _():
        pl.semaphore_wait(barrier, 1 + CORES * (below + above))
        tell(token.at[3], [partner])

        @pl.when(below == 1)
        def _():
            tell(token.at[5], [along(ring_z - 1, core) for core in range(CORES)])

        @pl.when(above == 1)
        def _():
            tell(token.at[5], [along(1, core) for core in range(CORES)])

    @pl.when(cc == 0)
    def _():
        pl.semaphore_wait(token.at[3], 1)

    d_copies[0].start()
    own[0] = dot(1)
    d_send[1] = dot(2)
    d_copies[1].start()
    own[1] = dot(3)
    d_copies[0].wait_recv()
    z_send[1] = own[0] + d_recv[0]

    def finish_near():
        d_copies[1].wait_recv()

        @pl.when(here)
        def _():
            z_recv[0] = own[1] + d_recv[1]

        @pl.when(jnp.logical_not(here))
        def _():
            z_send[0] = own[1] + d_recv[1]

    away_by = lax.rem(lax.div(my, CORES) * n_my + mx + ring_z - z, ring_z)
    short = jnp.logical_or(away_by <= 2, away_by >= ring_z - 2)
    soon = jnp.logical_and(short, jnp.logical_or(zz == 0, my == 0))
    far_soon = jnp.logical_and(zz == 0, my < 2)

    @pl.when(soon)
    def _():
        finish_near()
        pl.semaphore_wait(token.at[5], below + above)

    @pl.when(z == 1)
    def _():
        tell(token.at[6], [along(ring_z - 1, cc)])

    @pl.when(z == 0)
    def _():
        pl.semaphore_wait(token.at[6], 1)

    @pl.when(far_soon)
    def _():
        s_far.start()

    @pl.when(jnp.logical_and(soon, jnp.logical_not(here)))
    def _():
        s_near.start()

    @pl.when(cc == 0)
    def _():
        pl.semaphore_wait(barrier, CORES * (len(heads) + 2 - below - above))
        tell(token.at[4], [partner])

    @pl.when(cc == 1)
    def _():
        pl.semaphore_wait(token.at[4], 1)

    @pl.when(jnp.logical_not(far_soon))
    def _():
        s_far.start()

    @pl.when(jnp.logical_not(soon))
    def _():
        finish_near()

    @pl.when(jnp.logical_and(jnp.logical_not(soon), jnp.logical_not(here)))
    def _():
        s_near.start()

    tell(token.at[0], near)

    for c in teacher:
        c.wait()
    t_blk = jnp.dot(ts[...], tw[...], preferred_element_type=jnp.float32) * (1.0 / SOFTENING_HEAT)
    mt = jnp.max(t_blk, axis=1, keepdims=True)
    td = t_blk - mt
    et = jnp.exp(td)
    st = jnp.sum(et, axis=1, keepdims=True)
    log_st = jnp.log(st)
    tt = jnp.sum(et * td, axis=1, keepdims=True)

    @pl.when(jnp.logical_not(soon))
    def _():
        pl.semaphore_wait(token.at[5], below + above)

    pl.semaphore_wait(token.at[0], len(near))
    tell(token.at[1], [plane(0, 2), plane(0, RING_Y - 2)])
    pl.semaphore_wait(token.at[1], 2)
    tell(token.at[2], [plane(i, 0) for i in range(1, ring_x)])
    mask_load.wait()
    mask = mask_v[...].astype(jnp.float32)

    @pl.when(jnp.logical_not(here))
    def _():
        s_near.wait_recv()

    s_far.wait_recv()
    s_blk = (z_recv[0] + z_recv[1]) * (1.0 / SOFTENING_HEAT)
    ms = jnp.max(s_blk, axis=1, keepdims=True)
    sd = s_blk - ms
    log_ss = jnp.log(jnp.sum(jnp.exp(sd), axis=1, keepdims=True))
    kl = (tt - jnp.sum(et * sd, axis=1, keepdims=True)) / st - log_st + log_ss
    lane = lax.broadcasted_iota(jnp.int32, (tokens, 128), 1)
    upper = jnp.where(lane == 0, mt + log_st, kl)
    lower = jnp.broadcast_to(ms + log_ss, (tokens, 128))
    st_all[me] = jnp.concatenate([upper, lower], axis=0).T[:2, :]
    for device in line:
        remote(st_all.at[me], st_all.at[me], st_sem.at[0], st_sem.at[1], device).start()
    others = st_all.at[pl.ds(0, group - 1)]
    stats = remote(others, others, st_sem.at[0], st_sem.at[1], partner)

    stats.wait_recv()
    both = st_all[:, 0, :]
    kls = st_all[:, 1, :][:, :tokens]
    top = jnp.max(both, axis=0, keepdims=True)
    lse = top + jnp.log(jnp.sum(jnp.exp(both - top), axis=0, keepdims=True))
    rel = both - lse
    rel_t, rel_s = rel[:, :tokens], rel[:, tokens:2 * tokens]
    mism = (SOFTENING_HEAT * SOFTENING_HEAT) * jnp.sum(
        jnp.exp(rel_t) * (kls + (rel_t - rel_s)), axis=0, keepdims=True
    )
    half = lax.broadcasted_iota(jnp.int32, los_all.shape[1:], 1) < 64
    los_all[dp] = jnp.where(
        half, jnp.sum(mask * mism, axis=1, keepdims=True), jnp.sum(mask, axis=1, keepdims=True)
    )
    pl.semaphore_wait(token.at[2], ring_x - 1)
    away = [(i, j) for i in range(ring_x) for j in range(RING_Y) if (i, j) != (0, 0)]
    for i, j in sorted(away, key=lambda p: -min(p[0], ring_x - p[0]) - min(p[1], RING_Y - p[1])):
        remote(los_all.at[dp], los_all.at[dp], dp_sem.at[0], dp_sem.at[1], plane(i, j)).start()
    others = los_all.at[pl.ds(0, n_dp - 1)]
    losses = remote(others, others, dp_sem.at[0], dp_sem.at[1], partner)
    small_ref[0:1, :tokens] = mism

    mult = mask * (SOFTENING_HEAT * n_mx * n_my * bc * n_dp * tokens)
    mult = jnp.concatenate([mult, mult], axis=1)
    row = lax.broadcasted_iota(jnp.int32, (128, 128), 0)
    back = jnp.where(row == 0, lse, mult).T
    lt, ls, mu = back[:tokens, 0:1], back[tokens:2 * tokens, 0:1], back[:tokens, 1:2]
    g_send[...] = (jnp.exp(s_blk - ls) - jnp.exp(t_blk - lt)) * mu

    my_far = (1 - lax.div(my, CORES)) * CORES + lax.rem(my, CORES)
    g_near = remote(g_send, grad_ref.at[my], ag_ssem.at[0], ag_rsem.at[0], {"mx": my, "my": mx})
    g_far = remote(g_send, grad_ref.at[my], ag_ssem.at[1], ag_rsem.at[1], {"mx": my_far, "my": mx})

    @pl.when(jnp.logical_not(here))
    def _():
        g_near.start()

    g_far.start()

    @pl.when(here)
    def _():
        grad_ref[mx] = g_send[...]

    relays = [
        remote(grad_ref.at[slot], grad_ref.at[slot], rl_sem.at[0], rl_sem.at[1], partner) for slot in (mx, far)
    ]

    @pl.when(jnp.logical_not(here))
    def _():
        g_near.wait_recv()

    relays[0].start()
    g_far.wait_recv()
    relays[1].start()
    pair = grad_ref.at[pl.ds(0, 2)]
    relayed = remote(pair, pair, rl_sem.at[0], rl_sem.at[1], partner)
    relayed.wait_recv()
    losses.wait_recv()
    totals = jnp.sum(los_all[:, 0, :], axis=0, keepdims=True)
    count = totals[:, 64:65]
    small_ref[1:2, :] = totals / count

    @pl.when(jnp.logical_not(here))
    def _():
        s_near.wait_send()
        g_near.wait_send()

    halves = remote(d_send, d_recv, dd_ssem.at[0], dd_rsem.at[0], partner)
    for c in [losses, stats, s_far, g_far, halves, relayed]:
        c.wait_send()
    grad_ref[...] = grad_ref[...] * (1.0 / count).reshape(1, 1, 1)


def deliver(small_ref, grad_ref, mism_out, loss_out, grad_out, mism_v, loss_v, sem):
    bc = grad_ref.shape[2]
    copies = [
        pltpu.make_async_copy(grad_ref.at[j], grad_out.at[:, j * bc:(j + 1) * bc], sem.at[j])
        for j in range(grad_ref.shape[0])
    ]
    for c in copies:
        c.start()
    mism_v[...] = small_ref[0:1, :mism_v.shape[1]]
    loss_v[...] = small_ref[1:2, 0:1]
    for src, dst in ((mism_v, mism_out), (loss_v, loss_out)):
        copies.append(pltpu.make_async_copy(src, dst, sem.at[len(copies)]))
        copies[-1].start()
    for c in copies:
        c.wait()


def shards(sizes, ts, tw, ss, sw, mask):
    n_dp, n_mx, n_my = sizes
    tokens, bc = ts.shape[0], tw.shape[1]
    cols = sw.shape[1]
    group = n_mx * n_my
    f32 = jnp.float32
    V, D = pltpu.VMEM, pltpu.SemaphoreType.DMA
    hbm = pl.BlockSpec(memory_space=pltpu.HBM)
    vm = pl.BlockSpec(memory_space=pltpu.VMEM)
    held = pl.pallas_call(
        functools.partial(kernel, sizes),
        out_shape=(V((8, 128), f32), V((n_mx, tokens, bc), f32)),
        in_specs=[hbm, hbm, hbm, hbm, hbm],
        out_specs=(vm, vm),
        scratch_shapes=[
            V(ts.shape, ts.dtype), V(tw.shape, tw.dtype), V(ss.shape, ss.dtype),
            V((n_mx, sw.shape[0], bc), sw.dtype), V((1, tokens), mask.dtype),
            V((2, tokens, bc), f32), V((2, tokens, bc), f32), V((2, tokens, bc), f32),
            V((2, tokens, bc), f32), V((2, tokens, bc), f32), V((tokens, bc), f32),
            V((group, 2, 128), f32), V((n_dp, 1, 128), f32),
            D((4 + n_mx,)), D((1,)), D((2,)), D((2,)), D((2,)), D((2,)), D((2,)), D((2,)), D((2,)), D((2,)),
            pltpu.SemaphoreType.REGULAR((7,)),
        ],
        compiler_params=pltpu.CompilerParams(
            collective_id=0, has_side_effects=True, vmem_limit_bytes=64_000_000
        ),
    )(ts, tw, ss, sw, mask.reshape(1, tokens))
    mism, loss, grad = pl.pallas_call(
        deliver,
        out_shape=(
            jax.ShapeDtypeStruct((1, tokens), f32),
            jax.ShapeDtypeStruct((1, 1), f32),
            jax.ShapeDtypeStruct((tokens, cols), f32),
        ),
        in_specs=[vm, vm],
        out_specs=(hbm, hbm, hbm),
        scratch_shapes=[V((1, tokens), f32), V((1, 1), f32), D((2 + n_mx,))],
        compiler_params=pltpu.CompilerParams(vmem_limit_bytes=16 * 1024 * 1024),
    )(*[pltpu.with_memory_space_constraint(x, pltpu.VMEM) for x in held])
    return mism.reshape(tokens), loss.reshape(()), grad


def solution(mesh):
    sizes = (mesh.shape["dp"], mesh.shape["mx"], mesh.shape["my"])
    placed = (P("dp", None), P(None, ("mx", "my")), P("dp", "mx"), P("mx", "my"), P("dp"))
    return jax.shard_map(
        functools.partial(shards, sizes), mesh=mesh, in_specs=placed,
        out_specs=(P("dp"), P(), P("dp", "my")), check_vma=False,
    )
```

```python
import functools

import jax
import jax.numpy as jnp
from jax import lax
from jax.experimental import pallas as pl
from jax.experimental.pallas import tpu as pltpu
from jax.sharding import PartitionSpec as P

SOFTENING_HEAT = 2.0
CORES = 2
RING_Y = 8
MESH = pl.DeviceIdType.MESH


def kernel(
    sizes,
    ts_hbm, tw_hbm, ss_hbm, sw_hbm, mask_hbm,
    small_ref, grad_ref,
    ts, tw, ss, sw, mask_v,
    d_send, d_recv, own, z_send, z_recv, g_send,
    st_all, los_all,
    ld_sem, dd_ssem, dd_rsem, zz_rsem, ag_rsem, rl_sem, st_sem, dp_sem, token,
):
    n_dp, n_mx, n_my = sizes
    group = n_mx * n_my
    dp, mx, my = lax.axis_index("dp"), lax.axis_index("mx"), lax.axis_index("my")
    zz, cc = lax.div(mx, CORES), lax.rem(mx, CORES)
    oz, oc = 1 - zz, 1 - cc
    me = mx * n_my + my
    partner = {"mx": zz * CORES + oc}
    far = oz * CORES + cc
    tokens, bc = own.shape[1:]

    def remote(src, dst, ssem, rsem, dev):
        return pltpu.make_async_remote_copy(
            src_ref=src, dst_ref=dst, send_sem=ssem, recv_sem=rsem, device_id=dev, device_id_type=MESH
        )

    line = [
        {"mx": lax.rem(mx + i, n_mx), "my": lax.rem(my + j, n_my)}
        for i in (2, 3, 1, 0) for j in range(n_my) if (i, j) != (0, 0)
    ]
    ring_x = n_dp // RING_Y
    px, py = lax.div(dp, RING_Y), lax.rem(dp, RING_Y)

    def plane(i, j):
        return {"dp": lax.rem(px + i, ring_x) * RING_Y + lax.rem(py + j, RING_Y)}

    near = [plane(1, 0), plane(ring_x - 1, 0), plane(0, 1), plane(0, RING_Y - 1)]

    def tell(sem, devices):
        for device in devices:
            pl.semaphore_signal(sem, inc=1, device_id=device, device_id_type=MESH)

    ring_z = n_mx // CORES * n_my
    z = zz * n_my + my

    def along(k, core):
        to = lax.rem(z + k, ring_z)
        return {"mx": lax.div(to, n_my) * CORES + core, "my": lax.rem(to, n_my)}

    below, above = lax.div(z + ring_z - 1, ring_z), 1 - lax.div(z + 1, ring_z)
    upper_low = zz * (1 - lax.div(my, 2))

    def head(k):
        to = lax.rem(z + k, ring_z)
        return along(k, 1 - (1 - zz) * lax.div(to, n_my) * (1 - lax.div(lax.rem(to, n_my), 2)))

    heads = [head(k) for k in (4, 3, 5, 2, 6)] + [dict(device, mx=zz * CORES + 1) for device in near]
    beside = below + above
    extra = upper_low * (n_my - 1 + my)
    barrier = pltpu.get_barrier_semaphore()
    tell(barrier, heads + [along(ring_z - 1, 1 - below), along(1, 1 - above)])

    @pl.when(cc == 1)
    def _():
        tell(barrier, [partner])

    blocks = [oz * CORES + oc, far, zz * CORES + oc, mx]
    student = [pltpu.make_async_copy(ss_hbm, ss, ld_sem.at[0])]
    for k, block in enumerate(blocks):
        cols = pl.ds(pl.multiple_of(block * bc, bc), bc)
        student.append(pltpu.make_async_copy(sw_hbm.at[:, cols], sw.at[k], ld_sem.at[1 + k]))
    teacher = [
        pltpu.make_async_copy(ts_hbm, ts, ld_sem.at[1 + n_mx]),
        pltpu.make_async_copy(tw_hbm, tw, ld_sem.at[2 + n_mx]),
    ]
    mask_load = pltpu.make_async_copy(mask_hbm, mask_v, ld_sem.at[3 + n_mx])
    for c in student:
        c.start()

    def dot(k):
        student[1 + k].wait()
        return jnp.dot(ss[...], sw[k], preferred_element_type=jnp.float32)

    d_copies = [
        remote(d_send.at[k], d_recv.at[k], dd_ssem.at[0], dd_rsem.at[k], partner) for k in range(2)
    ]
    here = mx == my
    s_near = remote(z_send.at[0], z_recv.at[0], ld_sem.at[0], zz_rsem.at[0], {"mx": my, "my": mx})
    s_far = remote(z_send.at[1], z_recv.at[1], ld_sem.at[1], zz_rsem.at[1], {"mx": my, "my": far})

    student[0].wait()
    d_send[0] = dot(0)
    for c in teacher:
        c.start()
    mask_load.start()

    @pl.when(cc == 0)
    def _():
        pl.semaphore_wait(barrier, 1 + CORES * (beside + extra))
        tell(token.at[3], [partner])

        @pl.when(below == 1)
        def _():
            tell(token.at[4], [along(ring_z - 1, core) for core in range(CORES)])

        @pl.when(above == 1)
        def _():
            tell(token.at[4], [along(1, core) for core in range(CORES)])

    @pl.when(cc == 1)
    def _():
        pl.semaphore_wait(token.at[3], 1)

    d_copies[0].start()
    own[0] = dot(1)
    d_send[1] = dot(2)
    d_copies[1].start()
    own[1] = dot(3)
    d_copies[0].wait_recv()
    z_send[1] = own[0] + d_recv[0]

    def finish_near():
        d_copies[1].wait_recv()

        @pl.when(here)
        def _():
            z_recv[0] = own[1] + d_recv[1]

        @pl.when(jnp.logical_not(here))
        def _():
            z_send[0] = own[1] + d_recv[1]

    away_by = lax.rem(lax.div(my, CORES) * n_my + mx + ring_z - z, ring_z)
    short = jnp.logical_or(away_by <= 2, away_by >= ring_z - 2)
    early = jnp.logical_and(zz == 0, short)
    soon = jnp.logical_or(early, upper_low == 1)

    @pl.when(upper_low == 1)
    def _():
        s_far.start()

    @pl.when(soon)
    def _():
        finish_near()

    @pl.when(early)
    def _():
        pl.semaphore_wait(token.at[4], beside)

    @pl.when(z == 1)
    def _():
        tell(token.at[5], [along(ring_z - 1, cc)])

    @pl.when(z == 0)
    def _():
        pl.semaphore_wait(token.at[5], 1)

    @pl.when(jnp.logical_and(zz == 0, my < 2))
    def _():
        s_far.start()

    @pl.when(jnp.logical_and(soon, jnp.logical_not(here)))
    def _():
        s_near.start()

    @pl.when(cc == 1)
    def _():
        pl.semaphore_wait(barrier, CORES * (len(heads) + 2 - beside - extra))
        tell(token.at[3], [partner])

    @pl.when(cc == 0)
    def _():
        pl.semaphore_wait(token.at[3], 1)

    @pl.when(my >= 2)
    def _():
        s_far.start()

    @pl.when(jnp.logical_not(soon))
    def _():
        finish_near()

    @pl.when(jnp.logical_and(jnp.logical_not(soon), jnp.logical_not(here)))
    def _():
        s_near.start()

    tell(token.at[0], near)

    for c in teacher:
        c.wait()
    t_blk = jnp.dot(ts[...], tw[...], preferred_element_type=jnp.float32) * (1.0 / SOFTENING_HEAT)
    mt = jnp.max(t_blk, axis=1, keepdims=True)
    td = t_blk - mt
    et = jnp.exp(td)
    st = jnp.sum(et, axis=1, keepdims=True)
    log_st = jnp.log(st)
    tt = jnp.sum(et * td, axis=1, keepdims=True)

    @pl.when(jnp.logical_not(early))
    def _():
        pl.semaphore_wait(token.at[4], beside)

    pl.semaphore_wait(token.at[0], len(near))
    tell(token.at[1], [plane(0, 2), plane(0, RING_Y - 2)])
    pl.semaphore_wait(token.at[1], 2)
    tell(token.at[2], [plane(i, 0) for i in range(1, ring_x)])
    mask_load.wait()
    mask = mask_v[...].astype(jnp.float32)

    @pl.when(jnp.logical_not(here))
    def _():
        s_near.wait_recv()

    s_far.wait_recv()
    s_blk = (z_recv[0] + z_recv[1]) * (1.0 / SOFTENING_HEAT)
    ms = jnp.max(s_blk, axis=1, keepdims=True)
    sd = s_blk - ms
    log_ss = jnp.log(jnp.sum(jnp.exp(sd), axis=1, keepdims=True))
    kl = (tt - jnp.sum(et * sd, axis=1, keepdims=True)) / st - log_st + log_ss
    lane = lax.broadcasted_iota(jnp.int32, (tokens, 128), 1)
    upper = jnp.where(lane == 0, mt + log_st, kl)
    lower = jnp.broadcast_to(ms + log_ss, (tokens, 128))
    st_all[me] = jnp.concatenate([upper, lower], axis=0).T[:2, :]
    for device in line:
        remote(st_all.at[me], st_all.at[me], ld_sem.at[5], st_sem.at[0], device).start()
    others = st_all.at[pl.ds(0, group - 1)]
    stats = remote(others, others, ld_sem.at[5], st_sem.at[0], partner)

    stats.wait_recv()
    both = st_all[:, 0, :]
    kls = st_all[:, 1, :][:, :tokens]
    top = jnp.max(both, axis=0, keepdims=True)
    lse = top + jnp.log(jnp.sum(jnp.exp(both - top), axis=0, keepdims=True))
    rel = both - lse
    rel_t, rel_s = rel[:, :tokens], rel[:, tokens:2 * tokens]
    mism = (SOFTENING_HEAT * SOFTENING_HEAT) * jnp.sum(
        jnp.exp(rel_t) * (kls + (rel_t - rel_s)), axis=0, keepdims=True
    )
    half = lax.broadcasted_iota(jnp.int32, los_all.shape[1:], 1) < 64
    los_all[dp] = jnp.where(
        half, jnp.sum(mask * mism, axis=1, keepdims=True), jnp.sum(mask, axis=1, keepdims=True)
    )
    pl.semaphore_wait(token.at[2], ring_x - 1)
    away = [(i, j) for i in range(ring_x) for j in range(RING_Y) if (i, j) != (0, 0)]
    for i, j in sorted(away, key=lambda p: -min(p[0], ring_x - p[0]) - min(p[1], RING_Y - p[1])):
        remote(los_all.at[dp], los_all.at[dp], ld_sem.at[6], dp_sem.at[0], plane(i, j)).start()
    others = los_all.at[pl.ds(0, n_dp - 1)]
    losses = remote(others, others, ld_sem.at[6], dp_sem.at[0], partner)
    small_ref[0:1, :tokens] = mism

    mult = mask * (SOFTENING_HEAT * n_mx * n_my * bc * n_dp * tokens)
    mult = jnp.concatenate([mult, mult], axis=1)
    row = lax.broadcasted_iota(jnp.int32, (128, 128), 0)
    back = jnp.where(row == 0, lse, mult).T
    lt, ls, mu = back[:tokens, 0:1], back[tokens:2 * tokens, 0:1], back[:tokens, 1:2]
    g_send[...] = (jnp.exp(s_blk - ls) - jnp.exp(t_blk - lt)) * mu

    my_far = (1 - lax.div(my, CORES)) * CORES + lax.rem(my, CORES)
    g_near = remote(g_send, grad_ref.at[my], ld_sem.at[2], ag_rsem.at[0], {"mx": my, "my": mx})
    g_far = remote(g_send, grad_ref.at[my], ld_sem.at[3], ag_rsem.at[1], {"mx": my_far, "my": mx})

    @pl.when(jnp.logical_not(here))
    def _():
        g_near.start()

    g_far.start()

    @pl.when(here)
    def _():
        grad_ref[mx] = g_send[...]

    relays = [
        remote(grad_ref.at[slot], grad_ref.at[slot], ld_sem.at[4], rl_sem.at[0], partner) for slot in (mx, far)
    ]

    @pl.when(jnp.logical_not(here))
    def _():
        g_near.wait_recv()

    relays[0].start()
    g_far.wait_recv()
    relays[1].start()
    pair = grad_ref.at[pl.ds(0, 2)]
    relayed = remote(pair, pair, ld_sem.at[4], rl_sem.at[0], partner)
    relayed.wait_recv()
    losses.wait_recv()
    totals = jnp.sum(los_all[:, 0, :], axis=0, keepdims=True)
    count = totals[:, 64:65]
    small_ref[1:2, :] = totals / count

    @pl.when(jnp.logical_not(here))
    def _():
        s_near.wait_send()
        g_near.wait_send()

    halves = remote(d_send, d_recv, dd_ssem.at[0], dd_rsem.at[0], partner)
    for c in [losses, stats, s_far, g_far, halves, relayed]:
        c.wait_send()
    grad_ref[...] = grad_ref[...] * (1.0 / count).reshape(1, 1, 1)


def deliver(small_ref, grad_ref, mism_out, loss_out, grad_out, mism_v, loss_v, sem):
    bc = grad_ref.shape[2]
    for j in range(grad_ref.shape[0]):
        pltpu.make_async_copy(grad_ref.at[j], grad_out.at[:, j * bc:(j + 1) * bc], sem.at[0]).start()
    mism_v[...] = small_ref[0:1, :mism_v.shape[1]]
    loss_v[...] = small_ref[1:2, 0:1]
    copies = [pltpu.make_async_copy(mism_v, mism_out, sem.at[1]), pltpu.make_async_copy(loss_v, loss_out, sem.at[2])]
    for c in copies:
        c.start()
    pltpu.make_async_copy(grad_out, grad_out, sem.at[0]).wait()
    for c in copies:
        c.wait()


def shards(sizes, ts, tw, ss, sw, mask):
    n_dp, n_mx, n_my = sizes
    tokens, bc = ts.shape[0], tw.shape[1]
    cols = sw.shape[1]
    group = n_mx * n_my
    f32 = jnp.float32
    V, D = pltpu.VMEM, pltpu.SemaphoreType.DMA
    hbm = pl.BlockSpec(memory_space=pltpu.HBM)
    vm = pl.BlockSpec(memory_space=pltpu.VMEM)
    held = pl.pallas_call(
        functools.partial(kernel, sizes),
        out_shape=(V((8, 128), f32), V((n_mx, tokens, bc), f32)),
        in_specs=[hbm, hbm, hbm, hbm, hbm],
        out_specs=(vm, vm),
        scratch_shapes=[
            V(ts.shape, ts.dtype), V(tw.shape, tw.dtype), V(ss.shape, ss.dtype),
            V((n_mx, sw.shape[0], bc), sw.dtype), V((1, tokens), mask.dtype),
            V((2, tokens, bc), f32), V((2, tokens, bc), f32), V((2, tokens, bc), f32),
            V((2, tokens, bc), f32), V((2, tokens, bc), f32), V((tokens, bc), f32),
            V((group, 2, 128), f32), V((n_dp, 1, 128), f32),
            D((4 + n_mx,)), D((1,)), D((2,)), D((2,)), D((2,)), D((1,)), D((1,)), D((1,)),
            pltpu.SemaphoreType.REGULAR((6,)),
        ],
        compiler_params=pltpu.CompilerParams(
            collective_id=0, has_side_effects=True, vmem_limit_bytes=64_000_000
        ),
    )(ts, tw, ss, sw, mask.reshape(1, tokens))
    mism, loss, grad = pl.pallas_call(
        deliver,
        out_shape=(
            jax.ShapeDtypeStruct((1, tokens), f32),
            jax.ShapeDtypeStruct((1, 1), f32),
            jax.ShapeDtypeStruct((tokens, cols), f32),
        ),
        in_specs=[vm, vm],
        out_specs=(hbm, hbm, hbm),
        scratch_shapes=[V((1, tokens), f32), V((1, 1), f32), D((3,))],
        compiler_params=pltpu.CompilerParams(vmem_limit_bytes=16 * 1024 * 1024),
    )(*[pltpu.with_memory_space_constraint(x, pltpu.VMEM) for x in held])
    return mism.reshape(tokens), loss.reshape(()), grad


def solution(mesh):
    sizes = (mesh.shape["dp"], mesh.shape["mx"], mesh.shape["my"])
    placed = (P("dp", None), P(None, ("mx", "my")), P("dp", "mx"), P("mx", "my"), P("dp"))
    return jax.shard_map(
        functools.partial(shards, sizes), mesh=mesh, in_specs=placed,
        out_specs=(P("dp"), P(), P("dp", "my")), check_vma=False,
    )
```

```python
import functools

import jax
import jax.numpy as jnp
from jax import lax
from jax.experimental import pallas as pl
from jax.experimental.pallas import tpu as pltpu
from jax.sharding import PartitionSpec as P

SOFTENING_HEAT = 2.0
CORES = 2
RING_Y = 8
MESH = pl.DeviceIdType.MESH


def kernel(
    sizes,
    ts_hbm, tw_hbm, ss_hbm, sw_hbm, mask_hbm,
    small_ref, grad_ref,
    ts, tw, ss, sw, mask_v,
    d_send, d_recv, own, z_send, z_recv, g_send,
    st_all, los_all, cnt_all, g_all,
    ld_sem, dd_ssem, dd_rsem, zz_rsem, ag_rsem, rl_sem, st_sem, dp_sem, cn_sem, token,
):
    n_dp, n_mx, n_my = sizes
    group = n_mx * n_my
    dp, mx, my = lax.axis_index("dp"), lax.axis_index("mx"), lax.axis_index("my")
    zz, cc = lax.div(mx, CORES), lax.rem(mx, CORES)
    oz, oc = 1 - zz, 1 - cc
    me = mx * n_my + my
    partner = {"mx": zz * CORES + oc}
    far = oz * CORES + cc
    tokens, bc = own.shape[1:]

    def remote(src, dst, ssem, rsem, dev):
        return pltpu.make_async_remote_copy(
            src_ref=src, dst_ref=dst, send_sem=ssem, recv_sem=rsem, device_id=dev, device_id_type=MESH
        )

    line = [
        {"mx": lax.rem(mx + i, n_mx), "my": lax.rem(my + j, n_my)}
        for i in (2, 3, 1, 0) for j in range(n_my) if (i, j) != (0, 0)
    ]
    ring_x = n_dp // RING_Y
    px, py = lax.div(dp, RING_Y), lax.rem(dp, RING_Y)

    def plane(i, j):
        return {"dp": lax.rem(px + i, ring_x) * RING_Y + lax.rem(py + j, RING_Y)}

    near = [plane(1, 0), plane(ring_x - 1, 0), plane(0, 1), plane(0, RING_Y - 1)]

    def tell(sem, devices):
        for device in devices:
            pl.semaphore_signal(sem, inc=1, device_id=device, device_id_type=MESH)

    ring_z = n_mx // CORES * n_my
    z = zz * n_my + my

    def along(k, core):
        to = lax.rem(z + k, ring_z)
        return {"mx": lax.div(to, n_my) * CORES + core, "my": lax.rem(to, n_my)}

    below, above = lax.div(z + ring_z - 1, ring_z), 1 - lax.div(z + 1, ring_z)
    upper_low = zz * (1 - lax.div(my, 2))

    def head(k):
        to = lax.rem(z + k, ring_z)
        return along(k, 1 - (1 - zz) * lax.div(to, n_my) * (1 - lax.div(lax.rem(to, n_my), 2)))

    upper_high = zz * lax.div(my, 2)
    low_last = (1 - zz) * lax.div(my, n_my - 1)
    mute = jnp.logical_and(cc == 0, upper_high == 1)
    steps = (4, 3, 5, 2, 6)
    plane_heads = [dict(device, mx=zz * CORES + 1) for device in near]
    beside = below + above
    extra = upper_low * (n_my - 1 + my)
    barrier = pltpu.get_barrier_semaphore()
    blocks = [oz * CORES + oc, far, zz * CORES + oc, mx]
    student = [pltpu.make_async_copy(ss_hbm, ss, ld_sem.at[0])]
    for k, block in enumerate(blocks):
        cols = pl.ds(pl.multiple_of(block * bc, bc), bc)
        student.append(pltpu.make_async_copy(sw_hbm.at[:, cols], sw.at[k], ld_sem.at[1 + k]))
    teacher = [
        pltpu.make_async_copy(ts_hbm, ts, ld_sem.at[1 + n_mx]),
        pltpu.make_async_copy(tw_hbm, tw, ld_sem.at[2 + n_mx]),
    ]
    mask_load = pltpu.make_async_copy(mask_hbm, mask_v, ld_sem.at[3 + n_mx])
    for c in student[:2]:
        c.start()
    for k in steps:
        @pl.when(jnp.logical_not(jnp.logical_and(mute, lax.rem(z + k, ring_z) == n_my - 1)))
        def _():
            tell(barrier, [head(k)])

    tell(barrier, plane_heads + [along(ring_z - 1, 1 - below), along(1, 1 - above)])

    @pl.when(cc == 1)
    def _():
        tell(barrier, [partner])

    for c in student[2:]:
        c.start()

    def dot(k):
        student[1 + k].wait()
        return jnp.dot(ss[...], sw[k], preferred_element_type=jnp.float32)

    d_copies = [
        remote(d_send.at[k], d_recv.at[k], dd_ssem.at[0], dd_rsem.at[k], partner) for k in range(2)
    ]
    here = mx == my
    s_near = remote(z_send.at[0], z_recv.at[0], ld_sem.at[0], zz_rsem.at[0], {"mx": my, "my": mx})
    s_far = remote(z_send.at[1], z_recv.at[1], ld_sem.at[1], zz_rsem.at[1], {"mx": my, "my": far})

    student[0].wait()
    d_send[0] = dot(0)
    for c in teacher:
        c.start()
    mask_load.start()

    @pl.when(cc == 0)
    def _():
        pl.semaphore_wait(barrier, 1 + CORES * (beside + extra))
        tell(token.at[3], [partner])

        @pl.when(below == 1)
        def _():
            tell(token.at[4], [along(ring_z - 1, core) for core in range(CORES)])

        @pl.when(above == 1)
        def _():
            tell(token.at[4], [along(1, core) for core in range(CORES)])

    @pl.when(cc == 1)
    def _():
        pl.semaphore_wait(token.at[3], 1)

    d_copies[0].start()
    own[0] = dot(1)
    d_send[1] = dot(2)
    d_copies[1].start()
    own[1] = dot(3)
    d_copies[0].wait_recv()
    z_send[1] = own[0] + d_recv[0]

    def finish_near():
        d_copies[1].wait_recv()

        @pl.when(here)
        def _():
            z_recv[0] = own[1] + d_recv[1]

        @pl.when(jnp.logical_not(here))
        def _():
            z_send[0] = own[1] + d_recv[1]

    away_by = lax.rem(lax.div(my, CORES) * n_my + mx + ring_z - z, ring_z)
    short = jnp.logical_or(away_by <= 2, away_by >= ring_z - 2)
    early = jnp.logical_and(zz == 0, short)
    soon = jnp.logical_or(early, upper_low == 1)

    @pl.when(upper_low == 1)
    def _():
        s_far.start()

    @pl.when(soon)
    def _():
        finish_near()

    @pl.when(early)
    def _():
        pl.semaphore_wait(token.at[4], beside)

    @pl.when(z == 1)
    def _():
        tell(token.at[5], [along(ring_z - 1, cc)])

    @pl.when(z == 0)
    def _():
        pl.semaphore_wait(token.at[5], 1)

    @pl.when(jnp.logical_and(zz == 0, my < 2))
    def _():
        s_far.start()

    @pl.when(jnp.logical_and(soon, jnp.logical_not(here)))
    def _():
        s_near.start()

    @pl.when(cc == 1)
    def _():
        pl.semaphore_wait(barrier, CORES * (len(steps) + len(near) + 2 - beside - extra - low_last))
        tell(token.at[3], [partner])

    @pl.when(cc == 0)
    def _():
        pl.semaphore_wait(token.at[3], 1)

    @pl.when(my >= 2)
    def _():
        s_far.start()

    @pl.when(jnp.logical_not(soon))
    def _():
        finish_near()

    @pl.when(jnp.logical_and(jnp.logical_not(soon), jnp.logical_not(here)))
    def _():
        s_near.start()

    tell(token.at[0], near)

    @pl.when(mute)
    def _():
        for core in range(CORES):
            tell(token.at[6], [{"mx": core, "my": n_my - 1}])

    for c in teacher:
        c.wait()
    t_blk = jnp.dot(ts[...], tw[...], preferred_element_type=jnp.float32) * (1.0 / SOFTENING_HEAT)
    mt = jnp.max(t_blk, axis=1, keepdims=True)
    td = t_blk - mt
    et = jnp.exp(td)
    st = jnp.sum(et, axis=1, keepdims=True)
    log_st = jnp.log(st)
    tt = jnp.sum(et * td, axis=1, keepdims=True)

    @pl.when(jnp.logical_not(early))
    def _():
        pl.semaphore_wait(token.at[4], beside)

    pl.semaphore_wait(token.at[0], len(near))
    tell(token.at[1], [plane(0, 2), plane(0, RING_Y - 2)])

    @pl.when(jnp.logical_not(here))
    def _():
        s_near.wait_recv()

    s_far.wait_recv()
    s_blk = (z_recv[0] + z_recv[1]) * (1.0 / SOFTENING_HEAT)
    ms = jnp.max(s_blk, axis=1, keepdims=True)
    sd = s_blk - ms
    log_ss = jnp.log(jnp.sum(jnp.exp(sd), axis=1, keepdims=True))
    kl = (tt - jnp.sum(et * sd, axis=1, keepdims=True)) / st - log_st + log_ss
    lane = lax.broadcasted_iota(jnp.int32, (tokens, 128), 1)
    upper = jnp.where(lane == 0, mt + log_st, kl)
    lower = jnp.broadcast_to(ms + log_ss, (tokens, 128))
    st_all[me] = jnp.concatenate([upper, lower], axis=0).T[:2, :]
    @pl.when(low_last == 1)
    def _():
        pl.semaphore_wait(token.at[6], 2)

    for device in line:
        remote(st_all.at[me], st_all.at[me], ld_sem.at[5], st_sem.at[0], device).start()
    others = st_all.at[pl.ds(0, group - 1)]
    stats = remote(others, others, ld_sem.at[5], st_sem.at[0], partner)

    pl.semaphore_wait(token.at[1], 2)
    tell(token.at[2], [plane(i, 0) for i in range(1, ring_x)])
    mask_load.wait()
    mask = mask_v[...].astype(jnp.float32)
    cnt_all[dp] = jnp.broadcast_to(jnp.sum(mask, axis=1, keepdims=True), cnt_all.shape[1:])
    pl.semaphore_wait(token.at[2], ring_x - 1)
    away = [(i, j) for i in range(ring_x) for j in range(RING_Y) if (i, j) != (0, 0)]
    away.sort(key=lambda p: -min(p[0], ring_x - p[0]) - min(p[1], RING_Y - p[1]))

    def spread(buf, ssem, rsem):
        for i, j in away:
            remote(buf.at[dp], buf.at[dp], ssem, rsem, plane(i, j)).start()
        others = buf.at[pl.ds(0, n_dp - 1)]
        return remote(others, others, ssem, rsem, partner)

    counts = spread(cnt_all, ld_sem.at[7], cn_sem.at[0])
    stats.wait_recv()
    both = st_all[:, 0, :]
    kls = st_all[:, 1, :][:, :tokens]
    top = jnp.max(both, axis=0, keepdims=True)
    lse = top + jnp.log(jnp.sum(jnp.exp(both - top), axis=0, keepdims=True))
    rel = both - lse
    rel_t, rel_s = rel[:, :tokens], rel[:, tokens:2 * tokens]
    mism = (SOFTENING_HEAT * SOFTENING_HEAT) * jnp.sum(
        jnp.exp(rel_t) * (kls + (rel_t - rel_s)), axis=0, keepdims=True
    )
    los_all[dp] = jnp.broadcast_to(jnp.sum(mask * mism, axis=1, keepdims=True), los_all.shape[1:])
    losses = spread(los_all, ld_sem.at[6], dp_sem.at[0])
    small_ref[0:1, :tokens] = mism

    mult = mask * (SOFTENING_HEAT * n_mx * n_my * bc * n_dp * tokens)
    mult = jnp.concatenate([mult, mult], axis=1)
    row = lax.broadcasted_iota(jnp.int32, (128, 128), 0)
    back = jnp.where(row == 0, lse, mult).T
    lt, ls, mu = back[:tokens, 0:1], back[tokens:2 * tokens, 0:1], back[:tokens, 1:2]
    g_send[...] = (jnp.exp(s_blk - ls) - jnp.exp(t_blk - lt)) * mu

    my_far = (1 - lax.div(my, CORES)) * CORES + lax.rem(my, CORES)
    g_near = remote(g_send, g_all.at[my], ld_sem.at[2], ag_rsem.at[0], {"mx": my, "my": mx})
    g_far = remote(g_send, g_all.at[my], ld_sem.at[3], ag_rsem.at[1], {"mx": my_far, "my": mx})

    @pl.when(jnp.logical_not(here))
    def _():
        g_near.start()

    g_far.start()

    @pl.when(here)
    def _():
        g_all[mx] = g_send[...]

    relays = [
        remote(g_all.at[slot], g_all.at[slot], ld_sem.at[4], rl_sem.at[0], partner) for slot in (mx, far)
    ]

    @pl.when(jnp.logical_not(here))
    def _():
        g_near.wait_recv()

    relays[0].start()
    g_far.wait_recv()
    relays[1].start()
    pair = g_all.at[pl.ds(0, 2)]
    relayed = remote(pair, pair, ld_sem.at[4], rl_sem.at[0], partner)
    relayed.wait_recv()
    counts.wait_recv()
    count = jnp.sum(cnt_all[:, 0, :], axis=0, keepdims=True)
    grad_ref[...] = g_all[...] * (1.0 / count[:, 0:1]).reshape(1, 1, 1)
    losses.wait_recv()
    small_ref[1:2, :] = jnp.sum(los_all[:, 0, :], axis=0, keepdims=True) / count

    @pl.when(jnp.logical_not(here))
    def _():
        s_near.wait_send()
        g_near.wait_send()

    halves = remote(d_send, d_recv, dd_ssem.at[0], dd_rsem.at[0], partner)
    for c in [counts, losses, stats, s_far, g_far, halves, relayed]:
        c.wait_send()


def deliver(small_ref, grad_ref, mism_out, loss_out, grad_out, mism_v, loss_v, sem):
    bc = grad_ref.shape[2]
    for j in range(grad_ref.shape[0]):
        pltpu.make_async_copy(grad_ref.at[j], grad_out.at[:, j * bc:(j + 1) * bc], sem.at[0]).start()
    mism_v[...] = small_ref[0:1, :mism_v.shape[1]]
    loss_v[...] = small_ref[1:2, 0:1]
    copies = [pltpu.make_async_copy(mism_v, mism_out, sem.at[1]), pltpu.make_async_copy(loss_v, loss_out, sem.at[2])]
    for c in copies:
        c.start()
    pltpu.make_async_copy(grad_out, grad_out, sem.at[0]).wait()
    for c in copies:
        c.wait()


def shards(sizes, ts, tw, ss, sw, mask):
    n_dp, n_mx, n_my = sizes
    tokens, bc = ts.shape[0], tw.shape[1]
    cols = sw.shape[1]
    group = n_mx * n_my
    f32 = jnp.float32
    V, D = pltpu.VMEM, pltpu.SemaphoreType.DMA
    hbm = pl.BlockSpec(memory_space=pltpu.HBM)
    vm = pl.BlockSpec(memory_space=pltpu.VMEM)
    held = pl.pallas_call(
        functools.partial(kernel, sizes),
        out_shape=(V((8, 128), f32), V((n_mx, tokens, bc), f32)),
        in_specs=[hbm, hbm, hbm, hbm, hbm],
        out_specs=(vm, vm),
        scratch_shapes=[
            V(ts.shape, ts.dtype), V(tw.shape, tw.dtype), V(ss.shape, ss.dtype),
            V((n_mx, sw.shape[0], bc), sw.dtype), V((1, tokens), mask.dtype),
            V((2, tokens, bc), f32), V((2, tokens, bc), f32), V((2, tokens, bc), f32),
            V((2, tokens, bc), f32), V((2, tokens, bc), f32), V((tokens, bc), f32),
            V((group, 2, 128), f32), V((n_dp, 1, 128), f32), V((n_dp, 1, 128), f32), V((n_mx, tokens, bc), f32),
            D((4 + n_mx,)), D((1,)), D((2,)), D((2,)), D((2,)), D((1,)), D((1,)), D((1,)), D((1,)),
            pltpu.SemaphoreType.REGULAR((7,)),
        ],
        compiler_params=pltpu.CompilerParams(
            collective_id=0, has_side_effects=True, vmem_limit_bytes=64_000_000
        ),
    )(ts, tw, ss, sw, mask.reshape(1, tokens))
    mism, loss, grad = pl.pallas_call(
        deliver,
        out_shape=(
            jax.ShapeDtypeStruct((1, tokens), f32),
            jax.ShapeDtypeStruct((1, 1), f32),
            jax.ShapeDtypeStruct((tokens, cols), f32),
        ),
        in_specs=[vm, vm],
        out_specs=(hbm, hbm, hbm),
        scratch_shapes=[V((1, tokens), f32), V((1, 1), f32), D((3,))],
        compiler_params=pltpu.CompilerParams(vmem_limit_bytes=16 * 1024 * 1024),
    )(*[pltpu.with_memory_space_constraint(x, pltpu.VMEM) for x in held])
    return mism.reshape(tokens), loss.reshape(()), grad


def solution(mesh):
    sizes = (mesh.shape["dp"], mesh.shape["mx"], mesh.shape["my"])
    placed = (P("dp", None), P(None, ("mx", "my")), P("dp", "mx"), P("mx", "my"), P("dp"))
    return jax.shard_map(
        functools.partial(shards, sizes), mesh=mesh, in_specs=placed,
        out_specs=(P("dp"), P(), P("dp", "my")), check_vma=False,
    )
```

```python
import functools

import jax
import jax.numpy as jnp
from jax import lax
from jax.experimental import pallas as pl
from jax.experimental.pallas import tpu as pltpu
from jax.sharding import PartitionSpec as P

SOFTENING_HEAT = 2.0
CORES = 2
RING_Y = 8
MESH = pl.DeviceIdType.MESH


def kernel(
    sizes,
    ts_hbm, tw_hbm, ss_hbm, sw_hbm, mask_hbm,
    small_ref, grad_ref,
    ts, tw, ss, sw, mask_v,
    d_send, d_recv, own, z_send, z_recv, g_send,
    st_all, los_all, cnt_all, g_all,
    ld_sem, dd_ssem, dd_rsem, zz_rsem, ag_rsem, rl_sem, st_sem, dp_sem, cn_sem, token,
):
    n_dp, n_mx, n_my = sizes
    group = n_mx * n_my
    dp, mx, my = lax.axis_index("dp"), lax.axis_index("mx"), lax.axis_index("my")
    zz, cc = lax.div(mx, CORES), lax.rem(mx, CORES)
    oz, oc = 1 - zz, 1 - cc
    me = mx * n_my + my
    partner = {"mx": zz * CORES + oc}
    far = oz * CORES + cc
    tokens, bc = own.shape[1:]

    def remote(src, dst, ssem, rsem, dev):
        return pltpu.make_async_remote_copy(
            src_ref=src, dst_ref=dst, send_sem=ssem, recv_sem=rsem, device_id=dev, device_id_type=MESH
        )

    line = [
        {"mx": lax.rem(mx + i, n_mx), "my": lax.rem(my + j, n_my)}
        for i in (2, 3, 1, 0) for j in range(n_my) if (i, j) != (0, 0)
    ]
    ring_x = n_dp // RING_Y
    px, py = lax.div(dp, RING_Y), lax.rem(dp, RING_Y)

    def plane(i, j):
        return {"dp": lax.rem(px + i, ring_x) * RING_Y + lax.rem(py + j, RING_Y)}

    near = [plane(1, 0), plane(ring_x - 1, 0), plane(0, 1), plane(0, RING_Y - 1)]

    def tell(sem, devices):
        for device in devices:
            pl.semaphore_signal(sem, inc=1, device_id=device, device_id_type=MESH)

    ring_z = n_mx // CORES * n_my
    z = zz * n_my + my

    def along(k, core):
        to = lax.rem(z + k, ring_z)
        return {"mx": lax.div(to, n_my) * CORES + core, "my": lax.rem(to, n_my)}

    below, above = lax.div(z + ring_z - 1, ring_z), 1 - lax.div(z + 1, ring_z)
    upper_low = zz * (1 - lax.div(my, 2))

    def head(k):
        to = lax.rem(z + k, ring_z)
        return along(k, 1 - (1 - zz) * lax.div(to, n_my) * (1 - lax.div(lax.rem(to, n_my), 2)))

    upper_high = zz * lax.div(my, 2)
    low_last = (1 - zz) * lax.div(my, n_my - 1)
    mute = jnp.logical_and(cc == 0, upper_high == 1)
    steps = (4, 3, 5, 2, 6)
    plane_heads = [dict(device, mx=zz * CORES + 1) for device in near]
    beside = below + above
    extra = upper_low * (n_my - 1 + my)
    barrier = pltpu.get_barrier_semaphore()
    blocks = [oz * CORES + oc, far, zz * CORES + oc, mx]
    student = [pltpu.make_async_copy(ss_hbm, ss, ld_sem.at[0])]
    depth = sw.shape[1]
    cut = depth // 256 * 128
    for k, block in enumerate(blocks):
        cols = pl.ds(pl.multiple_of(block * bc, bc), bc)
        rows = pl.ds(0, depth if k else cut)
        student.append(pltpu.make_async_copy(sw_hbm.at[rows, cols], sw.at[k, rows], ld_sem.at[1 + k]))
    rest = pl.ds(cut, depth - cut)
    first_cols = pl.ds(pl.multiple_of(blocks[0] * bc, bc), bc)
    second_half = pltpu.make_async_copy(sw_hbm.at[rest, first_cols], sw.at[0, rest], ld_sem.at[4 + n_mx])
    teacher = [
        pltpu.make_async_copy(ts_hbm, ts, ld_sem.at[1 + n_mx]),
        pltpu.make_async_copy(tw_hbm, tw, ld_sem.at[2 + n_mx]),
    ]
    mask_load = pltpu.make_async_copy(mask_hbm, mask_v, ld_sem.at[3 + n_mx])
    for c in student[:2]:
        c.start()
    second_half.start()
    for k in steps:
        @pl.when(jnp.logical_not(jnp.logical_and(mute, lax.rem(z + k, ring_z) == n_my - 1)))
        def _():
            tell(barrier, [head(k)])

    tell(barrier, plane_heads + [along(ring_z - 1, 1 - below), along(1, 1 - above)])

    @pl.when(cc == 1)
    def _():
        tell(barrier, [partner])

    for c in student[2:]:
        c.start()

    def dot(k):
        student[1 + k].wait()
        return jnp.dot(ss[...], sw[k], preferred_element_type=jnp.float32)

    d_copies = [
        remote(d_send.at[k], d_recv.at[k], dd_ssem.at[0], dd_rsem.at[k], partner) for k in range(2)
    ]
    here = mx == my
    s_near = remote(z_send.at[0], z_recv.at[0], ld_sem.at[0], zz_rsem.at[0], {"mx": my, "my": mx})
    s_far = remote(z_send.at[1], z_recv.at[1], ld_sem.at[1], zz_rsem.at[1], {"mx": my, "my": far})

    student[0].wait()
    student[1].wait()
    part = jnp.dot(ss[:, :cut], sw[0, :cut], preferred_element_type=jnp.float32)
    second_half.wait()
    d_send[0] = part + jnp.dot(ss[:, cut:], sw[0, cut:], preferred_element_type=jnp.float32)
    for c in teacher:
        c.start()
    mask_load.start()

    @pl.when(cc == 0)
    def _():
        pl.semaphore_wait(barrier, 1 + CORES * (beside + extra))
        tell(token.at[3], [partner])

        @pl.when(below == 1)
        def _():
            tell(token.at[4], [along(ring_z - 1, core) for core in range(CORES)])

        @pl.when(above == 1)
        def _():
            tell(token.at[4], [along(1, core) for core in range(CORES)])

    @pl.when(cc == 1)
    def _():
        pl.semaphore_wait(token.at[3], 1)

    d_copies[0].start()
    own[0] = dot(1)
    d_send[1] = dot(2)
    d_copies[1].start()
    own[1] = dot(3)
    d_copies[0].wait_recv()
    z_send[1] = own[0] + d_recv[0]

    def finish_near():
        d_copies[1].wait_recv()

        @pl.when(here)
        def _():
            z_recv[0] = own[1] + d_recv[1]

        @pl.when(jnp.logical_not(here))
        def _():
            z_send[0] = own[1] + d_recv[1]

    away_by = lax.rem(lax.div(my, CORES) * n_my + mx + ring_z - z, ring_z)
    short = jnp.logical_or(away_by <= 2, away_by >= ring_z - 2)
    early = jnp.logical_and(zz == 0, short)
    soon = jnp.logical_or(early, upper_low == 1)

    @pl.when(upper_low == 1)
    def _():
        s_far.start()

    @pl.when(soon)
    def _():
        finish_near()

    @pl.when(early)
    def _():
        pl.semaphore_wait(token.at[4], beside)

    @pl.when(z == 1)
    def _():
        tell(token.at[5], [along(ring_z - 1, cc)])

    @pl.when(z == 0)
    def _():
        pl.semaphore_wait(token.at[5], 1)

    @pl.when(jnp.logical_and(zz == 0, my < 2))
    def _():
        s_far.start()

    @pl.when(jnp.logical_and(soon, jnp.logical_not(here)))
    def _():
        s_near.start()

    @pl.when(cc == 1)
    def _():
        pl.semaphore_wait(barrier, CORES * (len(steps) + len(near) + 2 - beside - extra - low_last))
        tell(token.at[3], [partner])

    @pl.when(cc == 0)
    def _():
        pl.semaphore_wait(token.at[3], 1)

    @pl.when(my >= 2)
    def _():
        s_far.start()

    @pl.when(jnp.logical_not(soon))
    def _():
        finish_near()

    @pl.when(jnp.logical_and(jnp.logical_not(soon), jnp.logical_not(here)))
    def _():
        s_near.start()

    tell(token.at[0], near)

    @pl.when(mute)
    def _():
        for core in range(CORES):
            tell(token.at[6], [{"mx": core, "my": n_my - 1}])

    for c in teacher:
        c.wait()
    t_blk = jnp.dot(ts[...], tw[...], preferred_element_type=jnp.float32) * (1.0 / SOFTENING_HEAT)
    mt = jnp.max(t_blk, axis=1, keepdims=True)
    td = t_blk - mt
    et = jnp.exp(td)
    st = jnp.sum(et, axis=1, keepdims=True)
    log_st = jnp.log(st)
    tt = jnp.sum(et * td, axis=1, keepdims=True)

    @pl.when(jnp.logical_not(early))
    def _():
        pl.semaphore_wait(token.at[4], beside)

    pl.semaphore_wait(token.at[0], len(near))
    tell(token.at[1], [plane(0, 2), plane(0, RING_Y - 2)])

    @pl.when(jnp.logical_not(here))
    def _():
        s_near.wait_recv()

    s_far.wait_recv()
    s_blk = (z_recv[0] + z_recv[1]) * (1.0 / SOFTENING_HEAT)
    ms = jnp.max(s_blk, axis=1, keepdims=True)
    sd = s_blk - ms
    log_ss = jnp.log(jnp.sum(jnp.exp(sd), axis=1, keepdims=True))
    kl = (tt - jnp.sum(et * sd, axis=1, keepdims=True)) / st - log_st + log_ss
    lane = lax.broadcasted_iota(jnp.int32, (tokens, 128), 1)
    upper = jnp.where(lane == 0, mt + log_st, kl)
    lower = jnp.broadcast_to(ms + log_ss, (tokens, 128))
    st_all[me] = jnp.concatenate([upper, lower], axis=0).T[:2, :]
    @pl.when(low_last == 1)
    def _():
        pl.semaphore_wait(token.at[6], 2)

    for device in line:
        remote(st_all.at[me], st_all.at[me], ld_sem.at[5], st_sem.at[0], device).start()
    others = st_all.at[pl.ds(0, group - 1)]
    stats = remote(others, others, ld_sem.at[5], st_sem.at[0], partner)

    pl.semaphore_wait(token.at[1], 2)
    tell(token.at[2], [plane(i, 0) for i in range(1, ring_x)])
    mask_load.wait()
    mask = mask_v[...].astype(jnp.float32)
    cnt_all[dp] = jnp.broadcast_to(jnp.sum(mask, axis=1, keepdims=True), cnt_all.shape[1:])
    pl.semaphore_wait(token.at[2], ring_x - 1)
    away = [(i, j) for i in range(ring_x) for j in range(RING_Y) if (i, j) != (0, 0)]
    away.sort(key=lambda p: -min(p[0], ring_x - p[0]) - min(p[1], RING_Y - p[1]))

    def spread(buf, ssem, rsem):
        for i, j in away:
            remote(buf.at[dp], buf.at[dp], ssem, rsem, plane(i, j)).start()
        others = buf.at[pl.ds(0, n_dp - 1)]
        return remote(others, others, ssem, rsem, partner)

    counts = spread(cnt_all, ld_sem.at[7], cn_sem.at[0])
    stats.wait_recv()
    both = st_all[:, 0, :]
    kls = st_all[:, 1, :][:, :tokens]
    top = jnp.max(both, axis=0, keepdims=True)
    lse = top + jnp.log(jnp.sum(jnp.exp(both - top), axis=0, keepdims=True))
    rel = both - lse
    rel_t, rel_s = rel[:, :tokens], rel[:, tokens:2 * tokens]
    mism = (SOFTENING_HEAT * SOFTENING_HEAT) * jnp.sum(
        jnp.exp(rel_t) * (kls + (rel_t - rel_s)), axis=0, keepdims=True
    )
    los_all[dp] = jnp.broadcast_to(jnp.sum(mask * mism, axis=1, keepdims=True), los_all.shape[1:])
    losses = spread(los_all, ld_sem.at[6], dp_sem.at[0])
    small_ref[0:1, :tokens] = mism

    mult = mask * (SOFTENING_HEAT * n_mx * n_my * bc * n_dp * tokens)
    mult = jnp.concatenate([mult, mult], axis=1)
    row = lax.broadcasted_iota(jnp.int32, (128, 128), 0)
    back = jnp.where(row == 0, lse, mult).T
    lt, ls, mu = back[:tokens, 0:1], back[tokens:2 * tokens, 0:1], back[:tokens, 1:2]
    g_send[...] = (jnp.exp(s_blk - ls) - jnp.exp(t_blk - lt)) * mu

    my_far = (1 - lax.div(my, CORES)) * CORES + lax.rem(my, CORES)
    g_near = remote(g_send, g_all.at[my], ld_sem.at[2], ag_rsem.at[0], {"mx": my, "my": mx})
    g_far = remote(g_send, g_all.at[my], ld_sem.at[3], ag_rsem.at[1], {"mx": my_far, "my": mx})

    @pl.when(jnp.logical_not(here))
    def _():
        g_near.start()

    g_far.start()

    @pl.when(here)
    def _():
        g_all[mx] = g_send[...]

    relays = [
        remote(g_all.at[slot], g_all.at[slot], ld_sem.at[4], rl_sem.at[0], partner) for slot in (mx, far)
    ]

    @pl.when(jnp.logical_not(here))
    def _():
        g_near.wait_recv()

    relays[0].start()
    g_far.wait_recv()
    relays[1].start()
    pair = g_all.at[pl.ds(0, 2)]
    relayed = remote(pair, pair, ld_sem.at[4], rl_sem.at[0], partner)
    relayed.wait_recv()
    counts.wait_recv()
    count = jnp.sum(cnt_all[:, 0, :], axis=0, keepdims=True)
    grad_ref[...] = g_all[...] * (1.0 / count[:, 0:1]).reshape(1, 1, 1)
    losses.wait_recv()
    small_ref[1:2, :] = jnp.sum(los_all[:, 0, :], axis=0, keepdims=True) / count

    @pl.when(jnp.logical_not(here))
    def _():
        s_near.wait_send()
        g_near.wait_send()

    halves = remote(d_send, d_recv, dd_ssem.at[0], dd_rsem.at[0], partner)
    for c in [counts, losses, stats, s_far, g_far, halves, relayed]:
        c.wait_send()


def deliver(small_ref, grad_ref, mism_out, loss_out, grad_out, mism_v, loss_v, sem):
    bc = grad_ref.shape[2]
    for j in range(grad_ref.shape[0]):
        pltpu.make_async_copy(grad_ref.at[j], grad_out.at[:, j * bc:(j + 1) * bc], sem.at[0]).start()
    mism_v[...] = small_ref[0:1, :mism_v.shape[1]]
    loss_v[...] = small_ref[1:2, 0:1]
    copies = [pltpu.make_async_copy(mism_v, mism_out, sem.at[1]), pltpu.make_async_copy(loss_v, loss_out, sem.at[2])]
    for c in copies:
        c.start()
    pltpu.make_async_copy(grad_out, grad_out, sem.at[0]).wait()
    for c in copies:
        c.wait()


def shards(sizes, ts, tw, ss, sw, mask):
    n_dp, n_mx, n_my = sizes
    tokens, bc = ts.shape[0], tw.shape[1]
    cols = sw.shape[1]
    group = n_mx * n_my
    f32 = jnp.float32
    V, D = pltpu.VMEM, pltpu.SemaphoreType.DMA
    hbm = pl.BlockSpec(memory_space=pltpu.HBM)
    vm = pl.BlockSpec(memory_space=pltpu.VMEM)
    held = pl.pallas_call(
        functools.partial(kernel, sizes),
        out_shape=(V((8, 128), f32), V((n_mx, tokens, bc), f32)),
        in_specs=[hbm, hbm, hbm, hbm, hbm],
        out_specs=(vm, vm),
        scratch_shapes=[
            V(ts.shape, ts.dtype), V(tw.shape, tw.dtype), V(ss.shape, ss.dtype),
            V((n_mx, sw.shape[0], bc), sw.dtype), V((1, tokens), mask.dtype),
            V((2, tokens, bc), f32), V((2, tokens, bc), f32), V((2, tokens, bc), f32),
            V((2, tokens, bc), f32), V((2, tokens, bc), f32), V((tokens, bc), f32),
            V((group, 2, 128), f32), V((n_dp, 1, 128), f32), V((n_dp, 1, 128), f32), V((n_mx, tokens, bc), f32),
            D((5 + n_mx,)), D((1,)), D((2,)), D((2,)), D((2,)), D((1,)), D((1,)), D((1,)), D((1,)),
            pltpu.SemaphoreType.REGULAR((7,)),
        ],
        compiler_params=pltpu.CompilerParams(
            collective_id=0, has_side_effects=True, vmem_limit_bytes=64_000_000
        ),
    )(ts, tw, ss, sw, mask.reshape(1, tokens))
    mism, loss, grad = pl.pallas_call(
        deliver,
        out_shape=(
            jax.ShapeDtypeStruct((1, tokens), f32),
            jax.ShapeDtypeStruct((1, 1), f32),
            jax.ShapeDtypeStruct((tokens, cols), f32),
        ),
        in_specs=[vm, vm],
        out_specs=(hbm, hbm, hbm),
        scratch_shapes=[V((1, tokens), f32), V((1, 1), f32), D((3,))],
        compiler_params=pltpu.CompilerParams(vmem_limit_bytes=16 * 1024 * 1024),
    )(*[pltpu.with_memory_space_constraint(x, pltpu.VMEM) for x in held])
    return mism.reshape(tokens), loss.reshape(()), grad


def solution(mesh):
    sizes = (mesh.shape["dp"], mesh.shape["mx"], mesh.shape["my"])
    placed = (P("dp", None), P(None, ("mx", "my")), P("dp", "mx"), P("mx", "my"), P("dp"))
    return jax.shard_map(
        functools.partial(shards, sizes), mesh=mesh, in_specs=placed,
        out_specs=(P("dp"), P(), P("dp", "my")), check_vma=False,
    )
```

```python
import functools

import jax
import jax.numpy as jnp
from jax import lax
from jax.experimental import pallas as pl
from jax.experimental.pallas import tpu as pltpu
from jax.sharding import PartitionSpec as P

SOFTENING_HEAT = 2.0
CORES = 2
RING_Y = 8
MESH = pl.DeviceIdType.MESH


def kernel(
    sizes,
    ts_hbm, tw_hbm, ss_hbm, sw_hbm, mask_hbm,
    small_ref, grad_ref,
    ts, tw, ss, sw, mask_v,
    d_send, d_recv, own, z_send, z_recv, g_send,
    st_all, los_all, cnt_all, g_all,
    ld_sem, dd_ssem, dd_rsem, zz_rsem, ag_rsem, rl_sem, st_sem, dp_sem, cn_sem, token,
):
    n_dp, n_mx, n_my = sizes
    group = n_mx * n_my
    dp, mx, my = lax.axis_index("dp"), lax.axis_index("mx"), lax.axis_index("my")
    zz, cc = lax.div(mx, CORES), lax.rem(mx, CORES)
    oz, oc = 1 - zz, 1 - cc
    me = mx * n_my + my
    partner = {"mx": zz * CORES + oc}
    far = oz * CORES + cc
    tokens, bc = own.shape[1:]

    def remote(src, dst, ssem, rsem, dev):
        return pltpu.make_async_remote_copy(
            src_ref=src, dst_ref=dst, send_sem=ssem, recv_sem=rsem, device_id=dev, device_id_type=MESH
        )

    line = [
        {"mx": lax.rem(mx + i, n_mx), "my": lax.rem(my + j, n_my)}
        for i in (2, 3, 1, 0) for j in range(n_my) if (i, j) != (0, 0)
    ]
    ring_x = n_dp // RING_Y
    px, py = lax.div(dp, RING_Y), lax.rem(dp, RING_Y)

    def plane(i, j):
        return {"dp": lax.rem(px + i, ring_x) * RING_Y + lax.rem(py + j, RING_Y)}

    near = [plane(1, 0), plane(ring_x - 1, 0), plane(0, 1), plane(0, RING_Y - 1)]

    def tell(sem, devices):
        for device in devices:
            pl.semaphore_signal(sem, inc=1, device_id=device, device_id_type=MESH)

    ring_z = n_mx // CORES * n_my
    z = zz * n_my + my

    def along(k, core):
        to = lax.rem(z + k, ring_z)
        return {"mx": lax.div(to, n_my) * CORES + core, "my": lax.rem(to, n_my)}

    below = lax.div(z + ring_z - 1, ring_z)
    upper_low = zz * (1 - lax.div(my, 2))
    low_last = (1 - zz) * lax.div(my, n_my - 1)

    def head(k):
        to = lax.rem(z + k, ring_z)
        up = (1 - zz) * lax.div(to, n_my) * (1 - lax.div(lax.rem(to, n_my), 2))
        return along(k, 1 - up)

    first_chips = (1 - zz) * (1 + below) + n_my * upper_low
    low_down = below * (1 - lax.div(z, n_my + 1))
    low_up = 1 - zz
    rounds = (1 - zz) * (below + 1)
    upper_high = zz * lax.div(my, 2)
    mute = jnp.logical_and(cc == 0, upper_high == 1)
    steps = (4, 3, 5, 2, 6)
    plane_heads = [dict(device, mx=zz * CORES + 1) for device in near]
    barrier = pltpu.get_barrier_semaphore()
    blocks = [oz * CORES + oc, far, zz * CORES + oc, mx]
    student = [pltpu.make_async_copy(ss_hbm, ss, ld_sem.at[0])]
    for k, block in enumerate(blocks):
        cols = pl.ds(pl.multiple_of(block * bc, bc), bc)
        student.append(pltpu.make_async_copy(sw_hbm.at[:, cols], sw.at[k], ld_sem.at[1 + k]))
    teacher = [
        pltpu.make_async_copy(ts_hbm, ts, ld_sem.at[1 + n_mx]),
        pltpu.make_async_copy(tw_hbm, tw, ld_sem.at[2 + n_mx]),
    ]
    mask_load = pltpu.make_async_copy(mask_hbm, mask_v, ld_sem.at[3 + n_mx])
    for c in student[:2]:
        c.start()
    for k in steps:
        @pl.when(jnp.logical_not(jnp.logical_and(mute, lax.rem(z + k, ring_z) == n_my - 1)))
        def _():
            tell(barrier, [head(k)])

    tell(barrier, plane_heads + [along(ring_z - 1, 1 - low_down), along(1, 1 - low_up)])

    @pl.when(cc == 1)
    def _():
        tell(barrier, [partner])

    for c in student[2:]:
        c.start()

    def dot(k):
        student[1 + k].wait()
        return jnp.dot(ss[...], sw[k], preferred_element_type=jnp.float32)

    d_copies = [
        remote(d_send.at[k], d_recv.at[k], dd_ssem.at[0], dd_rsem.at[k], partner) for k in range(2)
    ]
    here = mx == my
    s_near = remote(z_send.at[0], z_recv.at[0], ld_sem.at[0], zz_rsem.at[0], {"mx": my, "my": mx})
    s_far = remote(z_send.at[1], z_recv.at[1], ld_sem.at[1], zz_rsem.at[1], {"mx": my, "my": far})

    student[0].wait()
    d_send[0] = dot(0)
    for c in teacher:
        c.start()
    mask_load.start()

    @pl.when(cc == 0)
    def _():
        pl.semaphore_wait(barrier, 1 + CORES * first_chips)
        tell(token.at[3], [partner])

        @pl.when(jnp.logical_and(zz == 0, my > 0))
        def _():
            tell(token.at[4], [along(ring_z - 1, core) for core in range(CORES)])

        @pl.when(jnp.logical_and(zz == 0, my < n_my - 1))
        def _():
            tell(token.at[4], [along(1, core) for core in range(CORES)])

        @pl.when(z == n_my + 1)
        def _():
            tell(token.at[4], [along(ring_z - 2, core) for core in range(CORES)])

    @pl.when(cc == 1)
    def _():
        pl.semaphore_wait(token.at[3], 1)

    d_copies[0].start()
    own[0] = dot(1)
    d_send[1] = dot(2)
    d_copies[1].start()
    own[1] = dot(3)
    d_copies[0].wait_recv()
    z_send[1] = own[0] + d_recv[0]

    def finish_near():
        d_copies[1].wait_recv()

        @pl.when(here)
        def _():
            z_recv[0] = own[1] + d_recv[1]

        @pl.when(jnp.logical_not(here))
        def _():
            z_send[0] = own[1] + d_recv[1]

    away_by = lax.rem(lax.div(my, CORES) * n_my + mx + ring_z - z, ring_z)
    short = jnp.logical_or(away_by <= 2, away_by >= ring_z - 2)
    early = jnp.logical_and(zz == 0, short)
    soon = jnp.logical_or(early, upper_low == 1)

    @pl.when(soon)
    def _():
        finish_near()

    @pl.when(early)
    def _():
        pl.semaphore_wait(token.at[4], rounds)

    @pl.when(z == 1)
    def _():
        tell(token.at[5], [along(ring_z - 1, cc)])

    @pl.when(z == 0)
    def _():
        pl.semaphore_wait(token.at[5], 1)

    @pl.when(jnp.logical_and(zz == 0, my < 2))
    def _():
        s_far.start()

    @pl.when(jnp.logical_and(soon, jnp.logical_not(here)))
    def _():
        s_near.start()

    @pl.when(upper_low == 1)
    def _():
        s_far.start()

    @pl.when(cc == 1)
    def _():
        pl.semaphore_wait(barrier, CORES * (ring_z - 1 + len(near) - first_chips - low_last))
        tell(token.at[3], [partner])

    @pl.when(cc == 0)
    def _():
        pl.semaphore_wait(token.at[3], 1)

    @pl.when(my >= 2)
    def _():
        s_far.start()

    @pl.when(jnp.logical_not(soon))
    def _():
        finish_near()

    @pl.when(jnp.logical_and(jnp.logical_not(soon), jnp.logical_not(here)))
    def _():
        s_near.start()

    tell(token.at[0], near)

    @pl.when(mute)
    def _():
        for core in range(CORES):
            tell(token.at[6], [{"mx": core, "my": n_my - 1}])

    for c in teacher:
        c.wait()
    t_blk = jnp.dot(ts[...], tw[...], preferred_element_type=jnp.float32) * (1.0 / SOFTENING_HEAT)
    mt = jnp.max(t_blk, axis=1, keepdims=True)
    td = t_blk - mt
    et = jnp.exp(td)
    st = jnp.sum(et, axis=1, keepdims=True)
    log_st = jnp.log(st)
    tt = jnp.sum(et * td, axis=1, keepdims=True)

    @pl.when(jnp.logical_and(zz == 0, jnp.logical_not(early)))
    def _():
        pl.semaphore_wait(token.at[4], rounds)

    pl.semaphore_wait(token.at[0], len(near))
    tell(token.at[1], [plane(0, 2), plane(0, RING_Y - 2)])

    @pl.when(jnp.logical_not(here))
    def _():
        s_near.wait_recv()

    s_far.wait_recv()
    s_blk = (z_recv[0] + z_recv[1]) * (1.0 / SOFTENING_HEAT)
    ms = jnp.max(s_blk, axis=1, keepdims=True)
    sd = s_blk - ms
    log_ss = jnp.log(jnp.sum(jnp.exp(sd), axis=1, keepdims=True))
    kl = (tt - jnp.sum(et * sd, axis=1, keepdims=True)) / st - log_st + log_ss
    lane = lax.broadcasted_iota(jnp.int32, (tokens, 128), 1)
    upper = jnp.where(lane == 0, mt + log_st, kl)
    lower = jnp.broadcast_to(ms + log_ss, (tokens, 128))
    st_all[me] = jnp.concatenate([upper, lower], axis=0).T[:2, :]
    @pl.when(low_last == 1)
    def _():
        pl.semaphore_wait(token.at[6], 2)

    for device in line:
        remote(st_all.at[me], st_all.at[me], ld_sem.at[5], st_sem.at[0], device).start()
    others = st_all.at[pl.ds(0, group - 1)]
    stats = remote(others, others, ld_sem.at[5], st_sem.at[0], partner)

    pl.semaphore_wait(token.at[1], 2)
    tell(token.at[2], [plane(i, 0) for i in range(1, ring_x)])
    mask_load.wait()
    mask = mask_v[...].astype(jnp.float32)
    cnt_all[dp] = jnp.broadcast_to(jnp.sum(mask, axis=1, keepdims=True), cnt_all.shape[1:])
    pl.semaphore_wait(token.at[2], ring_x - 1)
    away = [(i, j) for i in range(ring_x) for j in range(RING_Y) if (i, j) != (0, 0)]
    away.sort(key=lambda p: -min(p[0], ring_x - p[0]) - min(p[1], RING_Y - p[1]))

    def spread(buf, ssem, rsem):
        for i, j in away:
            remote(buf.at[dp], buf.at[dp], ssem, rsem, plane(i, j)).start()
        others = buf.at[pl.ds(0, n_dp - 1)]
        return remote(others, others, ssem, rsem, partner)

    counts = spread(cnt_all, ld_sem.at[7], cn_sem.at[0])
    stats.wait_recv()
    both = st_all[:, 0, :]
    kls = st_all[:, 1, :][:, :tokens]
    top = jnp.max(both, axis=0, keepdims=True)
    lse = top + jnp.log(jnp.sum(jnp.exp(both - top), axis=0, keepdims=True))
    rel = both - lse
    rel_t, rel_s = rel[:, :tokens], rel[:, tokens:2 * tokens]
    mism = (SOFTENING_HEAT * SOFTENING_HEAT) * jnp.sum(
        jnp.exp(rel_t) * (kls + (rel_t - rel_s)), axis=0, keepdims=True
    )
    los_all[dp] = jnp.broadcast_to(jnp.sum(mask * mism, axis=1, keepdims=True), los_all.shape[1:])
    losses = spread(los_all, ld_sem.at[6], dp_sem.at[0])
    small_ref[0:1, :tokens] = mism

    mult = mask * (SOFTENING_HEAT * n_mx * n_my * bc * n_dp * tokens)
    mult = jnp.concatenate([mult, mult], axis=1)
    row = lax.broadcasted_iota(jnp.int32, (128, 128), 0)
    back = jnp.where(row == 0, lse, mult).T
    lt, ls, mu = back[:tokens, 0:1], back[tokens:2 * tokens, 0:1], back[:tokens, 1:2]
    g_send[...] = (jnp.exp(s_blk - ls) - jnp.exp(t_blk - lt)) * mu

    my_far = (1 - lax.div(my, CORES)) * CORES + lax.rem(my, CORES)
    g_near = remote(g_send, g_all.at[my], ld_sem.at[2], ag_rsem.at[0], {"mx": my, "my": mx})
    g_far = remote(g_send, g_all.at[my], ld_sem.at[3], ag_rsem.at[1], {"mx": my_far, "my": mx})

    @pl.when(jnp.logical_not(here))
    def _():
        g_near.start()

    g_far.start()

    @pl.when(here)
    def _():
        g_all[mx] = g_send[...]

    relays = [
        remote(g_all.at[slot], g_all.at[slot], ld_sem.at[4], rl_sem.at[0], partner) for slot in (mx, far)
    ]

    @pl.when(jnp.logical_not(here))
    def _():
        g_near.wait_recv()

    relays[0].start()
    g_far.wait_recv()
    relays[1].start()
    pair = g_all.at[pl.ds(0, 2)]
    relayed = remote(pair, pair, ld_sem.at[4], rl_sem.at[0], partner)
    relayed.wait_recv()
    counts.wait_recv()
    count = jnp.sum(cnt_all[:, 0, :], axis=0, keepdims=True)
    grad_ref[...] = g_all[...] * (1.0 / count[:, 0:1]).reshape(1, 1, 1)
    losses.wait_recv()
    small_ref[1:2, :] = jnp.sum(los_all[:, 0, :], axis=0, keepdims=True) / count

    @pl.when(jnp.logical_not(here))
    def _():
        s_near.wait_send()
        g_near.wait_send()

    halves = remote(d_send, d_recv, dd_ssem.at[0], dd_rsem.at[0], partner)
    for c in [counts, losses, stats, s_far, g_far, halves, relayed]:
        c.wait_send()


def deliver(small_ref, grad_ref, mism_out, loss_out, grad_out, mism_v, loss_v, sem):
    bc = grad_ref.shape[2]
    for j in range(grad_ref.shape[0]):
        pltpu.make_async_copy(grad_ref.at[j], grad_out.at[:, j * bc:(j + 1) * bc], sem.at[0]).start()
    mism_v[...] = small_ref[0:1, :mism_v.shape[1]]
    loss_v[...] = small_ref[1:2, 0:1]
    copies = [pltpu.make_async_copy(mism_v, mism_out, sem.at[1]), pltpu.make_async_copy(loss_v, loss_out, sem.at[2])]
    for c in copies:
        c.start()
    pltpu.make_async_copy(grad_out, grad_out, sem.at[0]).wait()
    for c in copies:
        c.wait()


def shards(sizes, ts, tw, ss, sw, mask):
    n_dp, n_mx, n_my = sizes
    tokens, bc = ts.shape[0], tw.shape[1]
    cols = sw.shape[1]
    group = n_mx * n_my
    f32 = jnp.float32
    V, D = pltpu.VMEM, pltpu.SemaphoreType.DMA
    hbm = pl.BlockSpec(memory_space=pltpu.HBM)
    vm = pl.BlockSpec(memory_space=pltpu.VMEM)
    held = pl.pallas_call(
        functools.partial(kernel, sizes),
        out_shape=(V((8, 128), f32), V((n_mx, tokens, bc), f32)),
        in_specs=[hbm, hbm, hbm, hbm, hbm],
        out_specs=(vm, vm),
        scratch_shapes=[
            V(ts.shape, ts.dtype), V(tw.shape, tw.dtype), V(ss.shape, ss.dtype),
            V((n_mx, sw.shape[0], bc), sw.dtype), V((1, tokens), mask.dtype),
            V((2, tokens, bc), f32), V((2, tokens, bc), f32), V((2, tokens, bc), f32),
            V((2, tokens, bc), f32), V((2, tokens, bc), f32), V((tokens, bc), f32),
            V((group, 2, 128), f32), V((n_dp, 1, 128), f32), V((n_dp, 1, 128), f32), V((n_mx, tokens, bc), f32),
            D((4 + n_mx,)), D((1,)), D((2,)), D((2,)), D((2,)), D((1,)), D((1,)), D((1,)), D((1,)),
            pltpu.SemaphoreType.REGULAR((7,)),
        ],
        compiler_params=pltpu.CompilerParams(
            collective_id=0, has_side_effects=True, vmem_limit_bytes=64_000_000
        ),
    )(ts, tw, ss, sw, mask.reshape(1, tokens))
    mism, loss, grad = pl.pallas_call(
        deliver,
        out_shape=(
            jax.ShapeDtypeStruct((1, tokens), f32),
            jax.ShapeDtypeStruct((1, 1), f32),
            jax.ShapeDtypeStruct((tokens, cols), f32),
        ),
        in_specs=[vm, vm],
        out_specs=(hbm, hbm, hbm),
        scratch_shapes=[V((1, tokens), f32), V((1, 1), f32), D((3,))],
        compiler_params=pltpu.CompilerParams(vmem_limit_bytes=16 * 1024 * 1024),
    )(*[pltpu.with_memory_space_constraint(x, pltpu.VMEM) for x in held])
    return mism.reshape(tokens), loss.reshape(()), grad


def solution(mesh):
    sizes = (mesh.shape["dp"], mesh.shape["mx"], mesh.shape["my"])
    placed = (P("dp", None), P(None, ("mx", "my")), P("dp", "mx"), P("mx", "my"), P("dp"))
    return jax.shard_map(
        functools.partial(shards, sizes), mesh=mesh, in_specs=placed,
        out_specs=(P("dp"), P(), P("dp", "my")), check_vma=False,
    )
```

```python
import functools

import jax
import jax.numpy as jnp
from jax import lax
from jax.experimental import pallas as pl
from jax.experimental.pallas import tpu as pltpu
from jax.sharding import PartitionSpec as P

SOFTENING_HEAT = 2.0
CORES = 2
RING_Y = 8
MESH = pl.DeviceIdType.MESH


def kernel(
    sizes,
    ts_hbm, tw_hbm, ss_hbm, sw_hbm, mask_hbm,
    small_ref, grad_ref,
    ts, tw, ss, sw, mask_v,
    d_send, d_recv, own, z_send, z_recv, g_send,
    st_all, los_all, cnt_all, g_all,
    ld_sem, dd_ssem, dd_rsem, zz_rsem, ag_rsem, rl_sem, st_sem, dp_sem, cn_sem, token,
):
    n_dp, n_mx, n_my = sizes
    group = n_mx * n_my
    dp, mx, my = lax.axis_index("dp"), lax.axis_index("mx"), lax.axis_index("my")
    zz, cc = lax.div(mx, CORES), lax.rem(mx, CORES)
    oz, oc = 1 - zz, 1 - cc
    me = mx * n_my + my
    partner = {"mx": zz * CORES + oc}
    far = oz * CORES + cc
    tokens, bc = own.shape[1:]

    def remote(src, dst, ssem, rsem, dev):
        return pltpu.make_async_remote_copy(
            src_ref=src, dst_ref=dst, send_sem=ssem, recv_sem=rsem, device_id=dev, device_id_type=MESH
        )

    line = [
        {"mx": lax.rem(mx + i, n_mx), "my": lax.rem(my + j, n_my)}
        for i in (2, 3, 1, 0) for j in range(n_my) if (i, j) != (0, 0)
    ]
    ring_x = n_dp // RING_Y
    px, py = lax.div(dp, RING_Y), lax.rem(dp, RING_Y)

    def plane(i, j):
        return {"dp": lax.rem(px + i, ring_x) * RING_Y + lax.rem(py + j, RING_Y)}

    near = [plane(1, 0), plane(ring_x - 1, 0), plane(0, 1), plane(0, RING_Y - 1)]

    def tell(sem, devices):
        for device in devices:
            pl.semaphore_signal(sem, inc=1, device_id=device, device_id_type=MESH)

    ring_z = n_mx // CORES * n_my
    z = zz * n_my + my

    def along(k, core):
        to = lax.rem(z + k, ring_z)
        return {"mx": lax.div(to, n_my) * CORES + core, "my": lax.rem(to, n_my)}

    below, above = lax.div(z + ring_z - 1, ring_z), 1 - lax.div(z + 1, ring_z)
    upper_low = zz * (1 - lax.div(my, 2))

    def head(k):
        to = lax.rem(z + k, ring_z)
        return along(k, 1 - (1 - zz) * lax.div(to, n_my) * (1 - lax.div(lax.rem(to, n_my), 2)))

    upper_high = zz * lax.div(my, 2)
    low_last = (1 - zz) * lax.div(my, n_my - 1)
    mute = jnp.logical_and(cc == 0, upper_high == 1)
    steps = (4, 3, 5, 2, 6)
    plane_heads = [dict(device, mx=zz * CORES + 1) for device in near]
    beside = below + above
    extra = upper_low * (n_my - 1 + my)
    barrier = pltpu.get_barrier_semaphore()
    blocks = [oz * CORES + oc, far, zz * CORES + oc, mx]
    student = [pltpu.make_async_copy(ss_hbm, ss, ld_sem.at[0])]
    for k, block in enumerate(blocks):
        cols = pl.ds(pl.multiple_of(block * bc, bc), bc)
        student.append(pltpu.make_async_copy(sw_hbm.at[:, cols], sw.at[k], ld_sem.at[1 + k]))
    teacher = [
        pltpu.make_async_copy(ts_hbm, ts, ld_sem.at[1 + n_mx]),
        pltpu.make_async_copy(tw_hbm, tw, ld_sem.at[2 + n_mx]),
    ]
    mask_load = pltpu.make_async_copy(mask_hbm, mask_v, ld_sem.at[3 + n_mx])
    for c in student[:2]:
        c.start()
    for k in steps:
        @pl.when(jnp.logical_not(jnp.logical_and(mute, lax.rem(z + k, ring_z) == n_my - 1)))
        def _():
            tell(barrier, [head(k)])

    tell(barrier, plane_heads + [along(ring_z - 1, 1 - below), along(1, 1 - above)])

    @pl.when(cc == 1)
    def _():
        tell(barrier, [partner])

    for c in student[2:]:
        c.start()

    def dot(k):
        student[1 + k].wait()
        return jnp.dot(ss[...], sw[k], preferred_element_type=jnp.float32)

    d_copies = [
        remote(d_send.at[k], d_recv.at[k], dd_ssem.at[0], dd_rsem.at[k], partner) for k in range(2)
    ]
    here = mx == my
    s_near = remote(z_send.at[0], z_recv.at[0], ld_sem.at[0], zz_rsem.at[0], {"mx": my, "my": mx})
    s_far = remote(z_send.at[1], z_recv.at[1], ld_sem.at[1], zz_rsem.at[1], {"mx": my, "my": far})

    student[0].wait()
    d_send[0] = dot(0)
    for c in teacher:
        c.start()
    mask_load.start()

    @pl.when(cc == 0)
    def _():
        pl.semaphore_wait(barrier, 1 + CORES * (beside + extra))
        tell(token.at[3], [partner])

        @pl.when(below == 1)
        def _():
            tell(token.at[4], [along(ring_z - 1, core) for core in range(CORES)])

        @pl.when(above == 1)
        def _():
            tell(token.at[4], [along(1, core) for core in range(CORES)])

    @pl.when(cc == 1)
    def _():
        pl.semaphore_wait(token.at[3], 1)

    d_copies[0].start()
    own[0] = dot(1)
    d_send[1] = dot(2)
    d_copies[1].start()
    own[1] = dot(3)
    d_copies[0].wait_recv()
    z_send[1] = own[0] + d_recv[0]

    def finish_near():
        d_copies[1].wait_recv()

        @pl.when(here)
        def _():
            z_recv[0] = own[1] + d_recv[1]

        @pl.when(jnp.logical_not(here))
        def _():
            z_send[0] = own[1] + d_recv[1]

    away_by = lax.rem(lax.div(my, CORES) * n_my + mx + ring_z - z, ring_z)
    short = jnp.logical_or(away_by <= 2, away_by >= ring_z - 2)
    early = jnp.logical_and(zz == 0, short)
    soon = jnp.logical_or(early, upper_low == 1)

    @pl.when(upper_low == 1)
    def _():
        s_far.start()

    @pl.when(soon)
    def _():
        finish_near()

    @pl.when(early)
    def _():
        pl.semaphore_wait(token.at[4], beside)

    @pl.when(z == 1)
    def _():
        tell(token.at[5], [along(ring_z - 1, cc)])

    @pl.when(z == 0)
    def _():
        pl.semaphore_wait(token.at[5], 1)

    @pl.when(jnp.logical_and(zz == 0, my < 2))
    def _():
        s_far.start()

    @pl.when(jnp.logical_and(soon, jnp.logical_not(here)))
    def _():
        s_near.start()

    @pl.when(cc == 1)
    def _():
        pl.semaphore_wait(barrier, CORES * (len(steps) + len(near) + 2 - beside - extra - low_last))
        tell(token.at[3], [partner])

    @pl.when(cc == 0)
    def _():
        pl.semaphore_wait(token.at[3], 1)

    @pl.when(my >= 2)
    def _():
        s_far.start()

    @pl.when(jnp.logical_not(soon))
    def _():
        finish_near()

    @pl.when(jnp.logical_and(jnp.logical_not(soon), jnp.logical_not(here)))
    def _():
        s_near.start()

    tell(token.at[0], near)

    @pl.when(mute)
    def _():
        for core in range(CORES):
            tell(token.at[6], [{"mx": core, "my": n_my - 1}])

    for c in teacher:
        c.wait()
    t_blk = jnp.dot(ts[...], tw[...], preferred_element_type=jnp.float32) * (1.0 / SOFTENING_HEAT)
    mt = jnp.max(t_blk, axis=1, keepdims=True)
    td = t_blk - mt
    et = jnp.exp(td)
    st = jnp.sum(et, axis=1, keepdims=True)
    log_st = jnp.log(st)
    tt = jnp.sum(et * td, axis=1, keepdims=True)

    @pl.when(jnp.logical_not(early))
    def _():
        pl.semaphore_wait(token.at[4], beside)

    pl.semaphore_wait(token.at[0], len(near))
    tell(token.at[1], [plane(0, 2), plane(0, RING_Y - 2)])

    @pl.when(jnp.logical_not(here))
    def _():
        s_near.wait_recv()

    s_far.wait_recv()
    s_blk = (z_recv[0] + z_recv[1]) * (1.0 / SOFTENING_HEAT)
    ms = jnp.max(s_blk, axis=1, keepdims=True)
    sd = s_blk - ms
    log_ss = jnp.log(jnp.sum(jnp.exp(sd), axis=1, keepdims=True))
    kl = (tt - jnp.sum(et * sd, axis=1, keepdims=True)) / st - log_st + log_ss
    lane = lax.broadcasted_iota(jnp.int32, (tokens, 128), 1)
    upper = jnp.where(lane == 0, mt + log_st, kl)
    lower = jnp.broadcast_to(ms + log_ss, (tokens, 128))
    st_all[me] = jnp.concatenate([upper, lower], axis=0).T[:2, :]
    @pl.when(low_last == 1)
    def _():
        pl.semaphore_wait(token.at[6], 2)

    for device in line:
        remote(st_all.at[me], st_all.at[me], ld_sem.at[5], st_sem.at[0], device).start()
    others = st_all.at[pl.ds(0, group - 1)]
    stats = remote(others, others, ld_sem.at[5], st_sem.at[0], partner)

    pl.semaphore_wait(token.at[1], 2)
    tell(token.at[2], [plane(i, 0) for i in range(1, ring_x)])
    mask_load.wait()
    mask = mask_v[...].astype(jnp.float32)
    cnt_all[dp] = jnp.broadcast_to(jnp.sum(mask, axis=1, keepdims=True), cnt_all.shape[1:])
    pl.semaphore_wait(token.at[2], ring_x - 1)
    away = [(i, j) for i in range(ring_x) for j in range(RING_Y) if (i, j) != (0, 0)]
    away.sort(key=lambda p: -min(p[0], ring_x - p[0]) - min(p[1], RING_Y - p[1]))

    def spread(buf, ssem, rsem):
        for i, j in away:
            remote(buf.at[dp], buf.at[dp], ssem, rsem, plane(i, j)).start()
        others = buf.at[pl.ds(0, n_dp - 1)]
        return remote(others, others, ssem, rsem, partner)

    counts = spread(cnt_all, ld_sem.at[7], cn_sem.at[0])
    stats.wait_recv()
    both = st_all[:, 0, :]
    kls = st_all[:, 1, :][:, :tokens]
    top = jnp.max(both, axis=0, keepdims=True)
    lse = top + jnp.log(jnp.sum(jnp.exp(both - top), axis=0, keepdims=True))
    rel = both - lse
    rel_t, rel_s = rel[:, :tokens], rel[:, tokens:2 * tokens]
    mism = (SOFTENING_HEAT * SOFTENING_HEAT) * jnp.sum(
        jnp.exp(rel_t) * (kls + (rel_t - rel_s)), axis=0, keepdims=True
    )
    los_all[dp] = jnp.broadcast_to(jnp.sum(mask * mism, axis=1, keepdims=True), los_all.shape[1:])
    losses = spread(los_all, ld_sem.at[6], dp_sem.at[0])
    small_ref[0:1, :tokens] = mism

    mult = mask * (SOFTENING_HEAT * n_mx * n_my * bc * n_dp * tokens)
    mult = jnp.concatenate([mult, mult], axis=1)
    row = lax.broadcasted_iota(jnp.int32, (128, 128), 0)
    back = jnp.where(row == 0, lse, mult).T
    lt, ls, mu = back[:tokens, 0:1], back[tokens:2 * tokens, 0:1], back[:tokens, 1:2]
    g_send[...] = (jnp.exp(s_blk - ls) - jnp.exp(t_blk - lt)) * mu

    my_far = (1 - lax.div(my, CORES)) * CORES + lax.rem(my, CORES)
    g_near = remote(g_send, g_all.at[my], ld_sem.at[2], ag_rsem.at[0], {"mx": my, "my": mx})
    g_far = remote(g_send, g_all.at[my], ld_sem.at[3], ag_rsem.at[1], {"mx": my_far, "my": mx})

    @pl.when(jnp.logical_not(here))
    def _():
        g_near.start()

    g_far.start()

    @pl.when(here)
    def _():
        g_all[mx] = g_send[...]

    relays = [
        remote(g_all.at[slot], g_all.at[slot], ld_sem.at[4], rl_sem.at[0], partner) for slot in (mx, far)
    ]

    @pl.when(jnp.logical_not(here))
    def _():
        g_near.wait_recv()

    relays[0].start()
    g_far.wait_recv()
    relays[1].start()
    pair = g_all.at[pl.ds(0, 2)]
    relayed = remote(pair, pair, ld_sem.at[4], rl_sem.at[0], partner)
    relayed.wait_recv()
    counts.wait_recv()
    count = jnp.sum(cnt_all[:, 0, :], axis=0, keepdims=True)
    grad_ref[...] = g_all[...] * (1.0 / count[:, 0:1]).reshape(1, 1, 1)
    losses.wait_recv()
    small_ref[1:2, :] = jnp.sum(los_all[:, 0, :], axis=0, keepdims=True) / count

    @pl.when(jnp.logical_not(here))
    def _():
        s_near.wait_send()
        g_near.wait_send()

    halves = remote(d_send, d_recv, dd_ssem.at[0], dd_rsem.at[0], partner)
    for c in [counts, losses, stats, s_far, g_far, halves, relayed]:
        c.wait_send()


def deliver(small_ref, grad_ref, mism_out, loss_out, grad_out, mism_v, loss_v, sem):
    bc = grad_ref.shape[2]
    half = grad_ref.shape[1] // 2
    for j in range(grad_ref.shape[0]):
        for r in (0, half):
            rows = pl.ds(r, half)
            pltpu.make_async_copy(
                grad_ref.at[j, rows], grad_out.at[rows, j * bc:(j + 1) * bc], sem.at[0]
            ).start()
    mism_v[...] = small_ref[0:1, :mism_v.shape[1]]
    loss_v[...] = small_ref[1:2, 0:1]
    copies = [pltpu.make_async_copy(mism_v, mism_out, sem.at[1]), pltpu.make_async_copy(loss_v, loss_out, sem.at[2])]
    for c in copies:
        c.start()
    pltpu.make_async_copy(grad_out, grad_out, sem.at[0]).wait()
    for c in copies:
        c.wait()


def shards(sizes, ts, tw, ss, sw, mask):
    n_dp, n_mx, n_my = sizes
    tokens, bc = ts.shape[0], tw.shape[1]
    cols = sw.shape[1]
    group = n_mx * n_my
    f32 = jnp.float32
    V, D = pltpu.VMEM, pltpu.SemaphoreType.DMA
    hbm = pl.BlockSpec(memory_space=pltpu.HBM)
    vm = pl.BlockSpec(memory_space=pltpu.VMEM)
    held = pl.pallas_call(
        functools.partial(kernel, sizes),
        out_shape=(V((8, 128), f32), V((n_mx, tokens, bc), f32)),
        in_specs=[hbm, hbm, hbm, hbm, hbm],
        out_specs=(vm, vm),
        scratch_shapes=[
            V(ts.shape, ts.dtype), V(tw.shape, tw.dtype), V(ss.shape, ss.dtype),
            V((n_mx, sw.shape[0], bc), sw.dtype), V((1, tokens), mask.dtype),
            V((2, tokens, bc), f32), V((2, tokens, bc), f32), V((2, tokens, bc), f32),
            V((2, tokens, bc), f32), V((2, tokens, bc), f32), V((tokens, bc), f32),
            V((group, 2, 128), f32), V((n_dp, 1, 128), f32), V((n_dp, 1, 128), f32), V((n_mx, tokens, bc), f32),
            D((4 + n_mx,)), D((1,)), D((2,)), D((2,)), D((2,)), D((1,)), D((1,)), D((1,)), D((1,)),
            pltpu.SemaphoreType.REGULAR((7,)),
        ],
        compiler_params=pltpu.CompilerParams(
            collective_id=0, has_side_effects=True, vmem_limit_bytes=64_000_000
        ),
    )(ts, tw, ss, sw, mask.reshape(1, tokens))
    mism, loss, grad = pl.pallas_call(
        deliver,
        out_shape=(
            jax.ShapeDtypeStruct((1, tokens), f32),
            jax.ShapeDtypeStruct((1, 1), f32),
            jax.ShapeDtypeStruct((tokens, cols), f32),
        ),
        in_specs=[vm, vm],
        out_specs=(hbm, hbm, hbm),
        scratch_shapes=[V((1, tokens), f32), V((1, 1), f32), D((3,))],
        compiler_params=pltpu.CompilerParams(vmem_limit_bytes=16 * 1024 * 1024),
    )(*[pltpu.with_memory_space_constraint(x, pltpu.VMEM) for x in held])
    return mism.reshape(tokens), loss.reshape(()), grad


def solution(mesh):
    sizes = (mesh.shape["dp"], mesh.shape["mx"], mesh.shape["my"])
    placed = (P("dp", None), P(None, ("mx", "my")), P("dp", "mx"), P("mx", "my"), P("dp"))
    return jax.shard_map(
        functools.partial(shards, sizes), mesh=mesh, in_specs=placed,
        out_specs=(P("dp"), P(), P("dp", "my")), check_vma=False,
    )
```
